32 devices in a mesh: section: 8 (over y, x, core), ctx: 4 (over z).
Axes of the slice: x: 2, y: 2, z: 4, core: 2. Of those that a mesh axis runs over, the one named last changes fastest.
Arguments:
- section_inputs: bfloat16 [8, 448, 2048], P('section', 'ctx'), may hold values from -3 to 3
- saved_inputs: bfloat16 [8, 448, 2048], P('section', 'ctx'), may hold values from -3 to 3
- output_grads: bfloat16 [8, 448, 2048], P('section', 'ctx'), may hold values from -6 to 6
- token_positions: int32 [448], P('ctx'), may hold values from 0 to 447, each once
- norm_gain: float32 [8, 2048], P('section'), may hold values from 0.7 to 6
- query_weight: bfloat16 [8, 2048, 2048], P('section', 'ctx'), may hold values from -0.13258252 to 0.13258252
- keyval_weight: bfloat16 [8, 2048, 1024], P('section', 'ctx'), may hold values from -0.13258252 to 0.13258252
- output_weight: bfloat16 [8, 2048, 2048], P('section'), may hold values from -0.125 to 0.125
Outputs:
- next_inputs: bfloat16 [8, 448, 2048], P('section', 'ctx')
- input_grads: bfloat16 [8, 448, 2048], P('section', 'ctx')
The draws below stay inside these ranges and needn't reach their ends.
Inputs may be any that keep to these rules, and one draw needn't show every extreme that they name: `token_positions`: each position of the sequence once.
All inputs are finite; a program needn't handle non-finite values.
Results may differ from the reference program's by a relative error of at most 0.04.
The reference program's roundings to bfloat16 on the way (of `normed`, `rounded` and `mixed`) count: a program that leaves them out, or rounds other values in their place, can miss the bound.
Values may be sent and summed in bfloat16 or wider, within the bound.
A program may use at most 192 MiB of HBM per device.

```python
import jax
import jax.numpy as jnp
from jax import lax

D = 2048
HEADS = 16
KV_HEADS = 4
HEAD_DIM = 128
SECTIONS = 8
SEQ = 448


def paired_weights(key):
    query_key = jax.random.fold_in(key, 11)
    keyval_key = jax.random.fold_in(key, 12)
    query_matrix = jax.random.truncated_normal(query_key, -4.0, 4.0, (SECTIONS, D, HEADS * HEAD_DIM), jnp.float32) * D ** (-0.5)
    keyval_matrix = jax.random.truncated_normal(keyval_key, -4.0, 4.0, (SECTIONS, D, 2 * KV_HEADS * HEAD_DIM), jnp.float32) * D ** (-0.5)
    return (query_matrix, keyval_matrix)


def draw_query_weight(key, part):
    return paired_weights(key)[0].astype(jnp.bfloat16)


def draw_keyval_weight(key, part):
    return paired_weights(key)[1].astype(jnp.bfloat16)


def draw_norm_gain(key, part):
    gain_key = jax.random.fold_in(key, 21)
    return 1.0 + 0.1 * jax.random.truncated_normal(gain_key, -3.0, 3.0, (SECTIONS, D), jnp.float32)


def block_levels(key, dims, shards, low, top_value):
    level, own = 1.0, jax.random.fold_in(key, 6)
    for axis_at, shards_of in shards:
        steps = jnp.exp(jax.random.uniform(jax.random.fold_in(own, axis_at), (shards_of,), jnp.float32, low / len(shards), top_value / len(shards)))
        level = level * jnp.repeat(steps, dims[axis_at] // shards_of).reshape([-1 if axis == axis_at else 1 for axis in range(len(dims))])
    return level


def normal_values(key, shape, spread, bound, cuts=(), kind=jnp.bfloat16):
    array = spread * jax.random.normal(key, shape, jnp.float32)
    if cuts:
        array = array * block_levels(key, shape, cuts, -0.22, 0.18)
    return jnp.clip(array, -bound, bound).astype(kind)


def setup_inputs(seed: int = 0) -> dict:
    keys = jax.random.split(jax.random.key(seed), 9)
    section_inputs = normal_values(keys[0], (SECTIONS, SEQ, D), 0.5, 3.0, ((0, 8), (1, 4)))
    saved_inputs = normal_values(keys[1], (SECTIONS, SEQ, D), 0.5, 3.0, ((0, 8), (1, 4)))
    output_grads = normal_values(keys[2], (SECTIONS, SEQ, D), 1.0, 6.0, ((0, 8), (1, 4)))
    token_positions = jax.random.permutation(keys[3], SEQ).astype(jnp.int32)
    norm_gain = draw_norm_gain(jax.random.fold_in(keys[8], 71), 0)
    query_weight = draw_query_weight(jax.random.fold_in(keys[8], 71), 0)
    keyval_weight = draw_keyval_weight(jax.random.fold_in(keys[8], 71), 0)
    output_weight = normal_values(keys[7], (SECTIONS, HEADS * HEAD_DIM, D), (HEADS * HEAD_DIM) ** -0.5, 0.125, ((0, 8),))
    return {"section_inputs": section_inputs, "saved_inputs": saved_inputs, "output_grads": output_grads, "token_positions": token_positions, "norm_gain": norm_gain, "query_weight": query_weight, "keyval_weight": keyval_weight, "output_weight": output_weight}


norm_eps = 1e-05
rope_base = 500000.0

def rotate(matrix, positions):
    half_dim = matrix.shape[-1] // 2
    frequency = rope_base ** (-2.0 * jnp.arange(half_dim, dtype=jnp.float32) / matrix.shape[-1])
    angles = positions.astype(jnp.float32)[:, None] * frequency[None, :]
    cos_table = jnp.cos(angles)[:, None, :]
    sin_table = jnp.sin(angles)[:, None, :]
    leading = matrix[..., :half_dim]
    trailing = matrix[..., half_dim:]
    return jnp.concatenate([leading * cos_table - trailing * sin_table, trailing * cos_table + leading * sin_table], axis=-1)

def project(tokens, gain, query_matrix, keyval_matrix, positions):
    widened = tokens.astype(jnp.float32)
    inverse = lax.rsqrt(lax.optimization_barrier(jnp.mean(widened * widened, axis=-1, keepdims=True)) + norm_eps)
    normed = (widened * inverse * gain[None, :]).astype(jnp.bfloat16)
    row_count = tokens.shape[0]
    query_full = jnp.dot(normed, query_matrix, preferred_element_type=jnp.float32)
    keyval_full = jnp.dot(normed, keyval_matrix, preferred_element_type=jnp.float32)
    queries = rotate(query_full.reshape(row_count, -1, HEAD_DIM), positions).astype(jnp.bfloat16)
    paired = keyval_full.reshape(row_count, 2, -1, HEAD_DIM)
    key_rows = rotate(paired[:, 0], positions).astype(jnp.bfloat16)
    value_rows = paired[:, 1].astype(jnp.bfloat16)
    return (queries, key_rows, value_rows)

def attend(queries, key_wide, value_wide, query_pos, key_pos):
    row_count = queries.shape[0]
    group_size = queries.shape[1] // key_wide.shape[1]
    grouped = queries.astype(jnp.float32).reshape(row_count, key_wide.shape[1], group_size, queries.shape[2])
    scores = jnp.einsum('rkgd,skd->kgrs', grouped, key_wide) * queries.shape[2] ** (-0.5)
    visible = (key_pos[None, :] <= query_pos[:, None])[None, None]
    masked = jnp.where(visible, scores, -1e+30)
    row_max = lax.stop_gradient(lax.optimization_barrier(jnp.max(masked, axis=-1, keepdims=True)))
    numerators = jnp.where(visible, jnp.exp(masked - row_max), 0.0)
    totals = lax.optimization_barrier(jnp.sum(numerators, axis=-1))
    rounded = lax.optimization_barrier(numerators.astype(jnp.bfloat16)).astype(jnp.float32)
    summed = jnp.einsum('kgrs,skd->rkgd', rounded, value_wide)
    averaged = summed / jnp.transpose(totals, (2, 0, 1))[..., None]
    return averaged.reshape(row_count, -1).astype(jnp.bfloat16)

def finish(tokens, mixed, output_matrix):
    return (tokens.astype(jnp.float32) + jnp.dot(mixed, output_matrix, preferred_element_type=jnp.float32)).astype(jnp.bfloat16)

def section_layer(tokens, gain, query_matrix, keyval_matrix, output_matrix, positions):
    queries, key_rows, value_rows = project(tokens, gain, query_matrix, keyval_matrix, positions)
    mixed = attend(queries, key_rows.astype(jnp.float32), value_rows.astype(jnp.float32), positions, positions)
    return finish(tokens, mixed, output_matrix)

def reference(section_inputs, saved_inputs, output_grads, token_positions, norm_gain, query_weight, keyval_weight, output_weight):

    def one_section(packed):
        forward_tokens, saved_tokens, upstream, gain, query_matrix, keyval_matrix, output_matrix = packed

        def layer(tokens):
            return section_layer(tokens, gain, query_matrix, keyval_matrix, output_matrix, token_positions)
        produced = layer(forward_tokens)
        unused, back_layer = jax.vjp(layer, saved_tokens)
        token_grads, = back_layer(upstream)
        return (produced, token_grads)
    results, gradients = lax.map(one_section, (section_inputs, saved_inputs, output_grads, norm_gain, query_weight, keyval_weight, output_weight))
    return (jnp.roll(results, 1, axis=0), jnp.roll(gradients, -1, axis=0))
```

```python
import functools

import jax
import jax.numpy as jnp
import numpy as np
from jax import lax
from jax.experimental import pallas as pl
from jax.experimental.pallas import tpu as pltpu
from jax.sharding import PartitionSpec as P

HEAD_DIM = 128


norm_eps = 1e-05
rope_base = 500000.0


def from_behind(block, axis, distance):
    devices = range(lax.axis_size(axis))
    route = [((i - distance) % len(devices), i) for i in devices]
    return lax.ppermute(block, axis, route)


def rotate(matrix, positions):
    half_dim = matrix.shape[-1] // 2
    frequency = rope_base ** (-2.0 * jnp.arange(half_dim, dtype=jnp.float32) / matrix.shape[-1])
    angles = positions.astype(jnp.float32)[:, None] * frequency[None, :]
    cos_table = jnp.cos(angles)[:, None, :]
    sin_table = jnp.sin(angles)[:, None, :]
    leading = matrix[..., :half_dim]
    trailing = matrix[..., half_dim:]
    return jnp.concatenate(
        [leading * cos_table - trailing * sin_table, trailing * cos_table + leading * sin_table],
        axis=-1,
    )


def project(tokens, gain, query_matrix, keyval_matrix, positions):
    widened = tokens.astype(jnp.float32)
    inverse = lax.rsqrt(jnp.mean(widened * widened, axis=-1, keepdims=True) + norm_eps)
    normed = (widened * inverse * gain[None, :]).astype(jnp.bfloat16)
    row_count = tokens.shape[0]
    query_full = jnp.dot(normed, query_matrix, preferred_element_type=jnp.float32)
    keyval_full = jnp.dot(normed, keyval_matrix, preferred_element_type=jnp.float32)
    queries = rotate(query_full.reshape(row_count, -1, HEAD_DIM), positions).astype(jnp.bfloat16)
    paired = keyval_full.reshape(row_count, 2, -1, HEAD_DIM)
    key_rows = rotate(paired[:, 0], positions).astype(jnp.bfloat16)
    value_rows = paired[:, 1].astype(jnp.bfloat16)
    return (queries, key_rows, value_rows)


def attend(queries, key_wide, value_wide, query_pos, key_pos, narrow):
    row_count = queries.shape[0]
    kv_count = key_wide.shape[1]
    head_size = queries.shape[2]
    group_size = queries.shape[1] // kv_count
    grouped = jnp.moveaxis(queries.reshape(row_count, kv_count, group_size, head_size), 1, 0)
    key_heads = jnp.moveaxis(key_wide, 1, 0)
    value_heads = jnp.moveaxis(value_wide, 1, 0)
    visible = (key_pos[None, :] <= query_pos[:, None])[None]

    def one_head(block):
        query_block, key_block, value_block = block
        scores = jnp.einsum(
            "rgd,sd->grs", query_block, key_block, preferred_element_type=jnp.float32
        ) * head_size ** (-0.5)
        masked = jnp.where(visible, scores, -1e30)
        row_max = lax.stop_gradient(jnp.max(masked, axis=-1, keepdims=True))
        numerators = jnp.where(visible, jnp.exp(masked - row_max), 0.0)
        totals = jnp.sum(numerators, axis=-1)
        if narrow:
            rounded = numerators.astype(jnp.bfloat16)
        else:
            rounded = lax.optimization_barrier(numerators.astype(jnp.bfloat16)).astype(jnp.float32)
        summed = jnp.einsum("grs,sd->rgd", rounded, value_block, preferred_element_type=jnp.float32)
        return summed / jnp.transpose(totals, (1, 0))[..., None]

    averaged = lax.map(one_head, (grouped, key_heads, value_heads))
    return jnp.moveaxis(averaged, 0, 1).reshape(row_count, -1).astype(jnp.bfloat16)


def finish(tokens, mixed, output_matrix):
    return (
        tokens.astype(jnp.float32)
        + jnp.dot(mixed, output_matrix, preferred_element_type=jnp.float32)
    ).astype(jnp.bfloat16)


def shards(
    section_inputs,
    saved_inputs,
    output_grads,
    token_positions,
    norm_gain,
    query_weight,
    keyval_weight,
    output_weight,
):
    key_positions = lax.all_gather(token_positions, "ctx", axis=0, tiled=True)
    full_query, full_keyval = (
        lax.all_gather(query_weight[0], "ctx", axis=0, tiled=True),
        lax.all_gather(keyval_weight[0], "ctx", axis=0, tiled=True),
    )
    full_output = output_weight[0]
    gain = norm_gain[0]
    forward_tokens = section_inputs[0]
    saved_tokens = saved_inputs[0]
    upstream = output_grads[0]

    def projector(tokens):
        return project(tokens, gain, full_query, full_keyval, token_positions)

    def attention_wide(queries, key_wide, value_wide):
        return attend(queries, key_wide, value_wide, token_positions, key_positions, False)

    def finishing(tokens, mixed):
        return finish(tokens, mixed, full_output)

    forward_queries, forward_keys, forward_values = projector(forward_tokens)
    (backward_queries, backward_keys, backward_values), back_project = jax.vjp(
        projector, saved_tokens
    )
    forward_keyset, forward_valueset = (
        lax.all_gather(forward_keys, "ctx", axis=0, tiled=True),
        lax.all_gather(forward_values, "ctx", axis=0, tiled=True),
    )
    mixed = attend(
        forward_queries, forward_keyset, forward_valueset, token_positions, key_positions, True
    )
    produced = finishing(forward_tokens, mixed)
    sent_on = from_behind(produced[None], "section", 1)
    backward_keyset, backward_valueset = (
        lax.all_gather(backward_keys, "ctx", axis=0, tiled=True),
        lax.all_gather(backward_values, "ctx", axis=0, tiled=True),
    )
    mixed, back_attend = jax.vjp(
        attention_wide,
        backward_queries.astype(jnp.float32),
        backward_keyset.astype(jnp.float32),
        backward_valueset.astype(jnp.float32),
    )
    produced, back_finish = jax.vjp(finishing, saved_tokens, mixed)
    residual_grad, mixed_grad = back_finish(upstream)
    query_grad, key_partial, value_partial = back_attend(mixed_grad)
    key_grads = lax.psum_scatter(
        key_partial.astype(jnp.bfloat16), "ctx", scatter_dimension=0, tiled=True
    )
    value_grads = lax.psum_scatter(
        value_partial.astype(jnp.bfloat16), "ctx", scatter_dimension=0, tiled=True
    )
    (project_grad,) = back_project((query_grad.astype(jnp.bfloat16), key_grads, value_grads))
    sent_back = from_behind((residual_grad + project_grad)[None], "section", -1)
    return (sent_on, sent_back)


MESH = pl.DeviceIdType.MESH
VMEM = pl.BlockSpec(memory_space=pltpu.VMEM)
ANY = pl.BlockSpec(memory_space=pl.ANY)
WIDE = jnp.float32
SLIM = jnp.bfloat16


def remote(src, dst, send, recv, device):
    return pltpu.make_async_remote_copy(
        src_ref=src, dst_ref=dst, send_sem=send, recv_sem=recv, device_id=device, device_id_type=MESH
    )


def layer_kernel(
    n, sections, tokens, saved, up, gain, wo_hbm, wq, wkv, pos, waves, ahead, back,
    nx, mine, mgl, mg, wo, wh, posg, bias, cos, sin, keys, values, dkey, dval, mixed, mixed_in, dqkv,
    part, from_mate, from_z, dn, produced, grads,
    nsend, nrecv, wsend, wrecv, msend, mrecv, psend, precv, asend, arecv, bsend, brecv, zsend, zrecv,
    osend, orecv, csend, crecv, own,
):
    section = lax.axis_index("section")
    me = lax.axis_index("ctx")
    half = n // 2
    core = lax.rem(section, 2)
    base = section - core
    mate = base + 1 - core
    side = me // half
    served = base + side
    lead = core == side
    partner = 2 * side * half + half - 1 - me
    edge = half - 1 + side
    at_edge = me == edge
    group_at = lax.rem(me, half) * 2 + core
    near, far = half - side, (n - 1) * (1 - side)
    depth, _ = wq.shape
    rows, width = tokens.shape
    gq = mg.shape[2]
    group = gq // HEAD_DIM
    kv_half = wkv.shape[1] // 2
    total_rows = n * rows
    scale = HEAD_DIM ** (-0.5)
    following, preceding = lax.rem(section + 1, sections), lax.rem(section + sections - 1, sections)
    pieces = group + 2

    barrier = pltpu.get_barrier_semaphore()
    for k in range(1, n):
        for other in (section, mate):
            pl.semaphore_signal(barrier, inc=1, device_id=(other, lax.rem(me + k, n)), device_id_type=MESH)
    for other in (mate, following, preceding):
        pl.semaphore_signal(barrier, inc=1, device_id=(other, me), device_id_type=MESH)

    wo_copy = pltpu.make_async_copy(wo_hbm, wo, own.at[0])
    wo_copy.start()

    def normed(block):
        widened = block[...].astype(WIDE)
        inverse = lax.rsqrt(jnp.mean(widened * widened, axis=-1, keepdims=True) + norm_eps)
        return (widened * inverse * gain[...]).astype(SLIM)

    for batch, block in enumerate((tokens, saved)):
        mine[batch] = normed(block)

    @pl.when(lead)
    def _():
        for batch in (0, 1):
            nx[batch, me] = mine[batch]

    posg[me] = pos[...]
    pl.semaphore_wait(barrier, 2 * n + 1)

    def seat(owner_core, j):
        return (base + j % 2, owner_core * half + j // 2)

    def token_copy(batch, lane, src, block, device):
        return remote(src, nx.at[batch, block], nsend.at[batch, lane, block], nrecv.at[batch, block], device)

    def to_mate(batch, block):
        return token_copy(batch, 0, nx.at[batch, block], block, (mate, me))

    def to_partner(batch, block):
        return token_copy(batch, 1, nx.at[batch, block], block, (section, partner))

    def to_edge(batch):
        return token_copy(batch, 0, mine.at[batch], me, (section, half - 1 + core))

    def piece_source(j, piece):
        if piece < group:
            return wq.at[:, pl.ds(j * gq + piece * HEAD_DIM, HEAD_DIM)], piece * HEAD_DIM
        value = piece - group
        return wkv.at[:, pl.ds(value * kv_half + j * HEAD_DIM, HEAD_DIM)], piece * HEAD_DIM

    def weight_copy(j, piece):
        src, to = piece_source(j, piece)
        return remote(
            src, wh.at[me, :, pl.ds(to, HEAD_DIM)], wsend.at[j, piece], wrecv.at[me, piece], seat(core, j)
        )

    def weight_here(j, piece):
        src, to = piece_source(j, piece)
        return pltpu.make_async_copy(src, wh.at[me, :, pl.ds(to, HEAD_DIM)], wrecv.at[me, piece])

    def weight_arrived(block, piece):
        dst = wh.at[block, :, pl.ds(piece * HEAD_DIM, HEAD_DIM)]
        remote(dst, dst, wsend.at[0, 0], wrecv.at[block, piece], (section, me)).wait_recv()

    def here(j):
        return jnp.logical_and(lead, group_at == j)

    def send_weights(piece):
        for j in range(n):
            pl.when(here(j))(lambda: weight_here(j, piece).start())
            pl.when(jnp.logical_not(here(j)))(lambda: weight_copy(j, piece).start())

    def grad_copy(j):
        return remote(mgl.at[j], mg.at[me], msend.at[j], mrecv.at[me], seat(core, j))

    def place_copy(k):
        return remote(pos, posg.at[me], psend.at[k], precv.at[me], (section, lax.rem(me + k, n)))

    @pl.when(lead)
    def _():
        for batch in (0, 1):
            to_partner(batch, me).start()
        for batch in (0, 1):
            to_mate(batch, me).start()

    @pl.when(jnp.logical_not(lead))
    def _():
        for batch in (0, 1):
            to_edge(batch).start()

    for k in range(1, n):
        place_copy(k).start()
    send_weights(group)
    send_weights(group + 1)

    wo_copy.wait()
    for j in range(n):
        mgl[j] = lax.dot_general(
            up[...], wo[pl.ds(j * gq, gq), :], (((1,), (1,)), ((), ())), preferred_element_type=WIDE
        ).astype(SLIM)
    for j in range(n):
        @pl.when(here(j))
        def _():
            mg[me] = mgl[j]

        pl.when(jnp.logical_not(here(j)))(lambda: grad_copy(j).start())

    @pl.when(jnp.logical_not(lead))
    def _():
        for piece in range(group):
            send_weights(piece)

    def token_arrived(batch, block):
        dst = nx.at[batch, block]
        remote(dst, dst, nsend.at[0, 0, 0], nrecv.at[batch, block], (section, me)).wait_recv()

    @pl.when(lead)
    def _():
        for batch in (0, 1):
            for block, outer in ((partner, False), (near, True), (far, True)):
                token_arrived(batch, block)
                if outer:
                    pl.when(at_edge)(lambda: to_partner(batch, block).start())
                to_mate(batch, block).start()
        for piece in range(group):
            send_weights(piece)

    for k in range(1, n):
        source = lax.rem(me + k, n)
        remote(pos, posg.at[source], psend.at[0], precv.at[source], (section, me)).wait_recv()
    columns = []
    for j in range(n):
        column = jnp.transpose(jnp.broadcast_to(posg[j].astype(WIDE), (HEAD_DIM, rows)))
        angles = column * waves[0:1, :]
        at = pl.ds(j * rows, rows)
        cos[at, :] = jnp.cos(angles)
        sin[at, :] = jnp.sin(angles) * waves[1:2, :]
        columns.append(column)
    column = jnp.concatenate(columns, axis=0)
    bias[...] = jnp.where(jnp.transpose(column)[0:1, :] <= column[:, 0:1], 0.0, -1e30)

    @pl.when(jnp.logical_not(lead))
    def _():
        for batch in (0, 1):
            for block in range(n):
                token_arrived(batch, block)

    def turn(block, sign):
        return block * cos[...] + sign * (pltpu.roll(block, HEAD_DIM // 2, 1) * sin[...])

    def dot(a, b, dims):
        return lax.dot_general(a, b, (dims, ((), ())), preferred_element_type=WIDE)

    def projected(batch, at):
        result = None
        for j in range(n):
            term = dot(
                nx[batch, :, :, pl.ds(j * depth, depth)].reshape(total_rows, depth), wh[j, :, at], ((1,), (0,))
            )
            result = term if result is None else result + term
        return result

    for piece in (group, group + 1):
        for j in range(n):
            weight_arrived(j, piece)
    for batch in (0, 1):
        both = projected(batch, pl.ds(gq, 2 * HEAD_DIM))
        keys[batch] = turn(both[:, :HEAD_DIM], 1.0).astype(SLIM)
        values[batch] = both[:, HEAD_DIM:].astype(SLIM)

    def weigh(queries, key_block):
        masked = dot(queries, key_block, ((1,), (1,))) * scale + bias[...]
        numerators = jnp.exp(masked - jnp.max(masked, axis=-1, keepdims=True))
        return numerators, jnp.sum(numerators, axis=-1, keepdims=True)

    def mixed_copy(block, h):
        return remote(
            mixed.at[block, h], mixed_in.at[group_at, h], asend.at[block, h], arecv.at[group_at, h], (served, block)
        )

    def elsewhere(block):
        return jnp.logical_not(jnp.logical_and(lead, me == block))

    dkey[...] = jnp.zeros_like(dkey)
    dval[...] = jnp.zeros_like(dval)

    for h in range(group):
        at = pl.ds(h * HEAD_DIM, HEAD_DIM)
        for j in range(n):
            weight_arrived(j, h)
        queries = turn(projected(0, at), 1.0).astype(SLIM)
        numerators, totals = weigh(queries, keys[0])
        result = dot(numerators.astype(SLIM), values[0], ((1,), (0,))) / totals
        mixed[:, h] = result.astype(SLIM).reshape(n, rows, HEAD_DIM)

        for block in range(n):
            pl.when(elsewhere(block))(lambda: mixed_copy(block, h).start())

        @pl.when(lead)
        def _():
            mixed_in[group_at, h] = mixed[me, h]

        if h == 0:
            for block in range(n):
                pl.when(elsewhere(block))(
                    lambda: remote(
                        mg.at[block], mg.at[block], msend.at[0], mrecv.at[block], (section, me)
                    ).wait_recv()
                )
        queries = turn(projected(1, at), 1.0).astype(SLIM)
        numerators, totals = weigh(queries, keys[1])
        rounded = numerators.astype(SLIM)
        summed = dot(rounded, values[1], ((1,), (0,)))
        summed_grad = mg[:, :, at].reshape(total_rows, HEAD_DIM).astype(WIDE) / totals
        totals_grad = -jnp.sum(summed_grad * (summed / totals), axis=-1, keepdims=True)
        narrow_grad = summed_grad.astype(SLIM)
        numer_grad = dot(narrow_grad, values[1], ((1,), (1,))) + totals_grad
        score_grad = (numerators * numer_grad * scale).astype(SLIM)
        query_grad = dot(score_grad, keys[1], ((1,), (0,))).astype(SLIM)
        dqkv[:, at] = turn(query_grad.astype(WIDE), -1.0).astype(SLIM)
        dkey[...] += dot(score_grad, queries, ((0,), (0,)))
        dval[...] += dot(rounded, narrow_grad, ((0,), (0,)))

    dqkv[:, pl.ds(gq, HEAD_DIM)] = turn(dkey[...].astype(SLIM).astype(WIDE), -1.0).astype(SLIM)
    dqkv[:, pl.ds(gq + HEAD_DIM, HEAD_DIM)] = dval[...].astype(SLIM)

    def partial_grad(block):
        block_rows = dqkv[pl.ds(pl.multiple_of(block * rows, 16), rows), :]
        for j in range(n):
            part[block, :, pl.ds(j * depth, depth)] = dot(block_rows, wh[j], ((1,), (1,))).astype(SLIM)

    def mate_sum(block):
        return remote(part.at[block], from_mate.at[block], bsend.at[block], brecv.at[block], (mate, me))

    def partner_sum(block):
        return remote(part.at[block], from_z.at[block], zsend.at[block], zrecv.at[block], (section, partner))

    def owner_sum(block):
        return remote(part.at[block], dn, osend.at[block], orecv.at[0], (section, block))

    def add_mate(block):
        mate_sum(block).wait_recv()
        part[block] = (part[block].astype(WIDE) + from_mate[block].astype(WIDE)).astype(SLIM)

    def add_partner(block):
        partner_sum(block).wait_recv()
        return (part[block].astype(WIDE) + from_z[block].astype(WIDE)).astype(SLIM)

    for block in (near, far, partner, me):
        partial_grad(block)
        pl.when(jnp.logical_not(lead))(lambda: mate_sum(block).start())

        @pl.when(lead)
        def _():
            add_mate(block)

        if block is partner:
            pl.when(lead)(lambda: partner_sum(block).start())
        elif block is not me:
            inner = jnp.logical_and(lead, jnp.logical_not(at_edge))
            pl.when(inner)(lambda: partner_sum(block).start())

    @pl.when(jnp.logical_and(lead, at_edge))
    def _():
        for block in (near, far):
            part[block] = add_partner(block)
            owner_sum(block).start()

    total = tokens[...].astype(WIDE)
    for j in range(n):
        def arrived():
            for h in range(group):
                dst = mixed_in.at[j, h]
                remote(dst, dst, asend.at[0, 0], arecv.at[j, h], (section, me)).wait_recv()

        pl.when(jnp.logical_not(here(j)))(arrived)
        for h in range(group):
            total += jnp.dot(
                mixed_in[j, h], wo[pl.ds(j * gq + h * HEAD_DIM, HEAD_DIM), :], preferred_element_type=WIDE
            )
    produced[...] = total.astype(SLIM)
    ahead_copy = remote(produced, ahead, csend.at[0], crecv.at[0], (following, me))
    ahead_copy.start()

    @pl.when(lead)
    def _():
        dn[...] = add_partner(me)

    @pl.when(jnp.logical_not(lead))
    def _():
        owner_sum(me).wait_recv()

    widened = saved[...].astype(WIDE)
    inverse = lax.rsqrt(jnp.mean(widened * widened, axis=-1, keepdims=True) + norm_eps)
    scaled = dn[...].astype(WIDE) * gain[...]
    inner_mean = jnp.mean(scaled * widened, axis=-1, keepdims=True)
    project_grad = inverse * scaled - widened * (inverse * inverse * inverse * inner_mean)
    grads[...] = up[...] + project_grad.astype(SLIM)
    back_copy = remote(grads, back, csend.at[1], crecv.at[1], (preceding, me))
    back_copy.start()

    @pl.when(lead)
    def _():
        for batch in (0, 1):
            for block in range(n):
                to_mate(batch, block).wait_send()
            to_partner(batch, me).wait_send()
            for block in (near, far):
                pl.when(at_edge)(lambda: to_partner(batch, block).wait_send())

    @pl.when(jnp.logical_not(lead))
    def _():
        for batch in (0, 1):
            to_edge(batch).wait_send()

    for k in range(1, n):
        place_copy(k).wait_send()
    for j in range(n):
        @pl.when(jnp.logical_not(here(j)))
        def _():
            for piece in range(pieces):
                weight_copy(j, piece).wait_send()
            grad_copy(j).wait_send()

        @pl.when(elsewhere(j))
        def _():
            for h in range(group):
                mixed_copy(j, h).wait_send()

    for block in range(n):
        pl.when(jnp.logical_not(lead))(lambda: mate_sum(block).wait_send())

    @pl.when(lead)
    def _():
        partner_sum(partner).wait_send()
        for block in (near, far):
            pl.when(at_edge)(lambda: owner_sum(block).wait_send())
            pl.when(jnp.logical_not(at_edge))(lambda: partner_sum(block).wait_send())

    ahead_copy.wait()
    back_copy.wait()


def hand_kernel(first, second, first_out, second_out):
    first_out[...] = first[...]
    second_out[...] = second[...]


def by_pairs(n, sections):
    def step(
        section_inputs, saved_inputs, output_grads, token_positions, norm_gain,
        query_weight, keyval_weight, output_weight,
    ):
        _, rows, width = section_inputs.shape
        _, depth, query_width = query_weight.shape
        gq = query_width // n
        group = gq // HEAD_DIM
        wide = gq + keyval_weight.shape[2] // n

        half_dim = HEAD_DIM // 2
        frequency = rope_base ** (-2.0 * np.arange(half_dim) / HEAD_DIM)
        signs = np.ones(half_dim)
        waves = jnp.asarray(
            np.stack([np.concatenate([frequency, frequency]), np.concatenate([-signs, signs])]), WIDE
        )

        def shaped(shape, kind=SLIM):
            return jax.ShapeDtypeStruct(shape, kind)

        def held(*shape, kind=SLIM):
            return pltpu.VMEM(shape, kind)

        pair = (shaped((rows, width)), shaped((rows, width)))
        dma = pltpu.SemaphoreType.DMA
        ahead, back = pl.pallas_call(
            functools.partial(layer_kernel, n, sections),
            out_shape=pair,
            in_specs=[VMEM, VMEM, VMEM, VMEM, ANY, ANY, ANY, VMEM, VMEM],
            out_specs=(VMEM,) * 2,
            scratch_shapes=[
                held(2, n, rows, width), held(2, rows, width),
                held(n, rows, gq), held(n, rows, gq), held(query_width, width), held(n, depth, wide),
                held(n, 1, rows, kind=jnp.int32), held(n * rows, n * rows, kind=WIDE),
                held(n * rows, HEAD_DIM, kind=WIDE), held(n * rows, HEAD_DIM, kind=WIDE),
                held(2, n * rows, HEAD_DIM), held(2, n * rows, HEAD_DIM),
                held(n * rows, HEAD_DIM, kind=WIDE), held(n * rows, HEAD_DIM, kind=WIDE),
                held(n, group, rows, HEAD_DIM), held(n, group, rows, HEAD_DIM), held(n * rows, wide),
                held(n, rows, width), held(n, rows, width), held(n, rows, width), held(rows, width),
                held(rows, width), held(rows, width),
                dma((2, 2, n)), dma((2, n)), dma((n, group + 2)), dma((n, group + 2)),
                *[dma((n,))] * 4, *[dma((n, group))] * 2, *[dma((n,))] * 5, dma((1,)),
                *[dma((2,))] * 2, dma((1,)),
            ],
            compiler_params=pltpu.CompilerParams(
                collective_id=0, has_side_effects=True, vmem_limit_bytes=60 * 2**20
            ),
            name="layer",
        )(
            section_inputs[0], saved_inputs[0], output_grads[0], norm_gain, output_weight[0],
            query_weight[0], keyval_weight[0], token_positions[None], waves,
        )
        ahead, back = pl.pallas_call(
            hand_kernel, out_shape=pair, in_specs=[VMEM] * 2, out_specs=(VMEM,) * 2, name="hand"
        )(ahead, back)
        return (ahead[None], back[None])

    return step


def solution(mesh):
    placed = (
        P("section", "ctx", None),
        P("section", "ctx", None),
        P("section", "ctx", None),
        P("ctx"),
        P("section", None),
        P("section", "ctx", None),
        P("section", "ctx", None),
        P("section", None, None),
    )
    n, sections = mesh.shape["ctx"], mesh.shape["section"]

    def chosen(*blocks):
        kv_heads = blocks[6].shape[2] // (2 * HEAD_DIM)
        if n == 4 and sections > 2 and sections % 2 == 0 and kv_heads == n:
            return by_pairs(n, sections)(*blocks)
        return shards(*blocks)

    return jax.shard_map(
        chosen,
        mesh=mesh,
        in_specs=placed,
        out_specs=(P("section", "ctx", None), P("section", "ctx", None)),
        check_vma=False,
    )
```

```python
import functools

import jax
import jax.numpy as jnp
import numpy as np
from jax import lax
from jax.experimental import pallas as pl
from jax.experimental.pallas import tpu as pltpu
from jax.sharding import PartitionSpec as P

HEAD_DIM = 128


norm_eps = 1e-05
rope_base = 500000.0


def from_behind(block, axis, distance):
    devices = range(lax.axis_size(axis))
    route = [((i - distance) % len(devices), i) for i in devices]
    return lax.ppermute(block, axis, route)


def rotate(matrix, positions):
    half_dim = matrix.shape[-1] // 2
    frequency = rope_base ** (-2.0 * jnp.arange(half_dim, dtype=jnp.float32) / matrix.shape[-1])
    angles = positions.astype(jnp.float32)[:, None] * frequency[None, :]
    cos_table = jnp.cos(angles)[:, None, :]
    sin_table = jnp.sin(angles)[:, None, :]
    leading = matrix[..., :half_dim]
    trailing = matrix[..., half_dim:]
    return jnp.concatenate(
        [leading * cos_table - trailing * sin_table, trailing * cos_table + leading * sin_table],
        axis=-1,
    )


def project(tokens, gain, query_matrix, keyval_matrix, positions):
    widened = tokens.astype(jnp.float32)
    inverse = lax.rsqrt(jnp.mean(widened * widened, axis=-1, keepdims=True) + norm_eps)
    normed = (widened * inverse * gain[None, :]).astype(jnp.bfloat16)
    row_count = tokens.shape[0]
    query_full = jnp.dot(normed, query_matrix, preferred_element_type=jnp.float32)
    keyval_full = jnp.dot(normed, keyval_matrix, preferred_element_type=jnp.float32)
    queries = rotate(query_full.reshape(row_count, -1, HEAD_DIM), positions).astype(jnp.bfloat16)
    paired = keyval_full.reshape(row_count, 2, -1, HEAD_DIM)
    key_rows = rotate(paired[:, 0], positions).astype(jnp.bfloat16)
    value_rows = paired[:, 1].astype(jnp.bfloat16)
    return (queries, key_rows, value_rows)


def attend(queries, key_wide, value_wide, query_pos, key_pos, narrow):
    row_count = queries.shape[0]
    kv_count = key_wide.shape[1]
    head_size = queries.shape[2]
    group_size = queries.shape[1] // kv_count
    grouped = jnp.moveaxis(queries.reshape(row_count, kv_count, group_size, head_size), 1, 0)
    key_heads = jnp.moveaxis(key_wide, 1, 0)
    value_heads = jnp.moveaxis(value_wide, 1, 0)
    visible = (key_pos[None, :] <= query_pos[:, None])[None]

    def one_head(block):
        query_block, key_block, value_block = block
        scores = jnp.einsum(
            "rgd,sd->grs", query_block, key_block, preferred_element_type=jnp.float32
        ) * head_size ** (-0.5)
        masked = jnp.where(visible, scores, -1e30)
        row_max = lax.stop_gradient(jnp.max(masked, axis=-1, keepdims=True))
        numerators = jnp.where(visible, jnp.exp(masked - row_max), 0.0)
        totals = jnp.sum(numerators, axis=-1)
        if narrow:
            rounded = numerators.astype(jnp.bfloat16)
        else:
            rounded = lax.optimization_barrier(numerators.astype(jnp.bfloat16)).astype(jnp.float32)
        summed = jnp.einsum("grs,sd->rgd", rounded, value_block, preferred_element_type=jnp.float32)
        return summed / jnp.transpose(totals, (1, 0))[..., None]

    averaged = lax.map(one_head, (grouped, key_heads, value_heads))
    return jnp.moveaxis(averaged, 0, 1).reshape(row_count, -1).astype(jnp.bfloat16)


def finish(tokens, mixed, output_matrix):
    return (
        tokens.astype(jnp.float32)
        + jnp.dot(mixed, output_matrix, preferred_element_type=jnp.float32)
    ).astype(jnp.bfloat16)


def shards(
    section_inputs,
    saved_inputs,
    output_grads,
    token_positions,
    norm_gain,
    query_weight,
    keyval_weight,
    output_weight,
):
    key_positions = lax.all_gather(token_positions, "ctx", axis=0, tiled=True)
    full_query, full_keyval = (
        lax.all_gather(query_weight[0], "ctx", axis=0, tiled=True),
        lax.all_gather(keyval_weight[0], "ctx", axis=0, tiled=True),
    )
    full_output = output_weight[0]
    gain = norm_gain[0]
    forward_tokens = section_inputs[0]
    saved_tokens = saved_inputs[0]
    upstream = output_grads[0]

    def projector(tokens):
        return project(tokens, gain, full_query, full_keyval, token_positions)

    def attention_wide(queries, key_wide, value_wide):
        return attend(queries, key_wide, value_wide, token_positions, key_positions, False)

    def finishing(tokens, mixed):
        return finish(tokens, mixed, full_output)

    forward_queries, forward_keys, forward_values = projector(forward_tokens)
    (backward_queries, backward_keys, backward_values), back_project = jax.vjp(
        projector, saved_tokens
    )
    forward_keyset, forward_valueset = (
        lax.all_gather(forward_keys, "ctx", axis=0, tiled=True),
        lax.all_gather(forward_values, "ctx", axis=0, tiled=True),
    )
    mixed = attend(
        forward_queries, forward_keyset, forward_valueset, token_positions, key_positions, True
    )
    produced = finishing(forward_tokens, mixed)
    sent_on = from_behind(produced[None], "section", 1)
    backward_keyset, backward_valueset = (
        lax.all_gather(backward_keys, "ctx", axis=0, tiled=True),
        lax.all_gather(backward_values, "ctx", axis=0, tiled=True),
    )
    mixed, back_attend = jax.vjp(
        attention_wide,
        backward_queries.astype(jnp.float32),
        backward_keyset.astype(jnp.float32),
        backward_valueset.astype(jnp.float32),
    )
    produced, back_finish = jax.vjp(finishing, saved_tokens, mixed)
    residual_grad, mixed_grad = back_finish(upstream)
    query_grad, key_partial, value_partial = back_attend(mixed_grad)
    key_grads = lax.psum_scatter(
        key_partial.astype(jnp.bfloat16), "ctx", scatter_dimension=0, tiled=True
    )
    value_grads = lax.psum_scatter(
        value_partial.astype(jnp.bfloat16), "ctx", scatter_dimension=0, tiled=True
    )
    (project_grad,) = back_project((query_grad.astype(jnp.bfloat16), key_grads, value_grads))
    sent_back = from_behind((residual_grad + project_grad)[None], "section", -1)
    return (sent_on, sent_back)


MESH = pl.DeviceIdType.MESH
VMEM = pl.BlockSpec(memory_space=pltpu.VMEM)
ANY = pl.BlockSpec(memory_space=pl.ANY)
WIDE = jnp.float32
SLIM = jnp.bfloat16


def remote(src, dst, send, recv, device):
    return pltpu.make_async_remote_copy(
        src_ref=src, dst_ref=dst, send_sem=send, recv_sem=recv, device_id=device, device_id_type=MESH
    )


def row_chunks(rows):
    tiles = rows // 16
    sizes = [size * 16 for size in ((tiles - 1) - (tiles - 1) // 2, (tiles - 1) // 2, 1) if size]
    return [(sum(sizes[:i]), size) for i, size in enumerate(sizes)]


def layer_kernel(
    n, sections, tokens_hbm, saved_hbm, up_hbm, gain_hbm, wo_hbm, wq, wkv, pos_hbm, waves_hbm, ahead, back,
    tokens, saved, up, gain, pos, waves, nx, mine, mgl, mg, wo, wh, posg, bias, cos, sin, keys, values, dkey, dval, mixed, mixed_in, dqkv,
    part, from_mate, from_z, dn, produced, grads,
    nsend, nrecv, wsend, wrecv, msend, mrecv, psend, precv, asend, arecv, bsend, brecv, zsend, zrecv,
    osend, orecv, csend, crecv, own,
):
    section = lax.axis_index("section")
    me = lax.axis_index("ctx")
    half = n // 2
    core = lax.rem(section, 2)
    base = section - core
    mate = base + 1 - core
    side = me // half
    served = base + side
    lead = core == side
    partner = 2 * side * half + half - 1 - me
    edge = half - 1 + side
    at_edge = me == edge
    group_at = lax.rem(me, half) * 2 + core
    near, far = half - side, (n - 1) * (1 - side)
    depth, _ = wq.shape
    rows, width = tokens.shape
    gq = mg.shape[2]
    group = gq // HEAD_DIM
    kv_half = wkv.shape[1] // 2
    total_rows = n * rows
    scale = HEAD_DIM ** (-0.5)
    following, preceding = lax.rem(section + 1, sections), lax.rem(section + sections - 1, sections)
    pieces = group + 2

    barrier = pltpu.get_barrier_semaphore()
    for k in range(1, n):
        for other in (section, mate):
            pl.semaphore_signal(barrier, inc=1, device_id=(other, lax.rem(me + k, n)), device_id_type=MESH)
    for other in (mate, following, preceding):
        pl.semaphore_signal(barrier, inc=1, device_id=(other, me), device_id_type=MESH)

    loads = [
        pltpu.make_async_copy(src, dst, own.at[i])
        for i, (src, dst) in enumerate(
            (
                (gain_hbm, gain), (tokens_hbm, tokens), (saved_hbm, saved), (pos_hbm, pos), (up_hbm, up),
                (waves_hbm, waves), (wo_hbm, wo),
            )
        )
    ]
    for load in loads:
        load.start()

    def normed(block):
        widened = block[...].astype(WIDE)
        inverse = lax.rsqrt(jnp.mean(widened * widened, axis=-1, keepdims=True) + norm_eps)
        return (widened * inverse * gain[...]).astype(SLIM)

    for load in loads[:4]:
        load.wait()
    for batch, block in enumerate((tokens, saved)):
        mine[batch] = normed(block)

    @pl.when(lead)
    def _():
        for batch in (0, 1):
            nx[batch, me] = mine[batch]

    posg[me] = pos[...]
    pl.semaphore_wait(barrier, 2 * n + 1)

    def seat(owner_core, j):
        return (base + lax.rem(j, 2), owner_core * half + j // 2)

    def token_copy(batch, lane, src, block, device):
        return remote(src, nx.at[batch, block], nsend.at[batch, lane, block], nrecv.at[batch, block], device)

    def to_mate(batch, block):
        return token_copy(batch, 0, nx.at[batch, block], block, (mate, me))

    def to_partner(batch, block):
        return token_copy(batch, 1, nx.at[batch, block], block, (section, partner))

    def to_edge(batch):
        return token_copy(batch, 0, mine.at[batch], me, (section, half - 1 + core))

    def piece_source(j, piece):
        if piece < group:
            start = j * gq + piece * HEAD_DIM
            return wq.at[:, pl.ds(pl.multiple_of(start, HEAD_DIM), HEAD_DIM)], piece * HEAD_DIM
        start = (piece - group) * kv_half + j * HEAD_DIM
        return wkv.at[:, pl.ds(pl.multiple_of(start, HEAD_DIM), HEAD_DIM)], piece * HEAD_DIM

    def weight_copy(j, piece):
        src, to = piece_source(j, piece)
        return remote(
            src, wh.at[me, :, pl.ds(to, HEAD_DIM)], wsend.at[j, piece], wrecv.at[me, piece], seat(core, j)
        )

    def weight_here(j, piece):
        src, to = piece_source(j, piece)
        return pltpu.make_async_copy(src, wh.at[me, :, pl.ds(to, HEAD_DIM)], wrecv.at[me, piece])

    def weight_arrived(block, piece):
        dst = wh.at[block, :, pl.ds(piece * HEAD_DIM, HEAD_DIM)]
        remote(dst, dst, wsend.at[0, 0], wrecv.at[block, piece], (section, me)).wait_recv()

    def here(j):
        return jnp.logical_and(lead, group_at == j)

    def send_weights(piece):
        for i in range(n):
            j = lax.rem(i + core * half, n)
            pl.when(here(j))(lambda: weight_here(j, piece).start())
            pl.when(jnp.logical_not(here(j)))(lambda: weight_copy(j, piece).start())

    def grad_copy(j):
        return remote(mgl.at[j], mg.at[me], msend.at[j], mrecv.at[me], seat(core, j))

    def place_copy(k):
        return remote(pos, posg.at[me], psend.at[k], precv.at[me], (section, lax.rem(me + k, n)))

    @pl.when(lead)
    def _():
        for batch in (0, 1):
            to_partner(batch, me).start()
        for batch in (0, 1):
            to_mate(batch, me).start()

    @pl.when(jnp.logical_not(lead))
    def _():
        for batch in (0, 1):
            to_edge(batch).start()

    for k in range(1, n):
        place_copy(k).start()
    send_weights(group)
    send_weights(group + 1)

    for load in loads[4:]:
        load.wait()
    for j in range(n):
        mgl[j] = lax.dot_general(
            up[...], wo[pl.ds(j * gq, gq), :], (((1,), (1,)), ((), ())), preferred_element_type=WIDE
        ).astype(SLIM)
    for j in range(n):
        @pl.when(here(j))
        def _():
            mg[me] = mgl[j]

        pl.when(jnp.logical_not(here(j)))(lambda: grad_copy(j).start())

    @pl.when(jnp.logical_not(lead))
    def _():
        for piece in range(group):
            send_weights(piece)

    def token_arrived(batch, block):
        dst = nx.at[batch, block]
        remote(dst, dst, nsend.at[0, 0, 0], nrecv.at[batch, block], (section, me)).wait_recv()

    @pl.when(lead)
    def _():
        for batch in (0, 1):
            for block, outer in ((partner, False), (near, True), (far, True)):
                token_arrived(batch, block)
                if outer:
                    pl.when(at_edge)(lambda: to_partner(batch, block).start())
                to_mate(batch, block).start()
        for piece in range(group):
            send_weights(piece)

    for k in range(1, n):
        source = lax.rem(me + k, n)
        remote(pos, posg.at[source], psend.at[0], precv.at[source], (section, me)).wait_recv()
    columns = []
    for j in range(n):
        column = jnp.transpose(jnp.broadcast_to(posg[j].astype(WIDE), (HEAD_DIM, rows)))
        angles = column * waves[0:1, :]
        at = pl.ds(j * rows, rows)
        cos[at, :] = jnp.cos(angles)
        sin[at, :] = jnp.sin(angles) * waves[1:2, :]
        columns.append(column)
    column = jnp.concatenate(columns, axis=0)
    bias[...] = jnp.where(jnp.transpose(column)[0:1, :] <= column[:, 0:1], 0.0, -1e30)

    @pl.when(jnp.logical_not(lead))
    def _():
        for batch in (0, 1):
            for block in range(n):
                token_arrived(batch, block)

    def turn(block, sign):
        return block * cos[...] + sign * (pltpu.roll(block, HEAD_DIM // 2, 1) * sin[...])

    def dot(a, b, dims):
        return lax.dot_general(a, b, (dims, ((), ())), preferred_element_type=WIDE)

    def projected(batch, at):
        result = None
        for j in range(n):
            term = dot(
                nx[batch, :, :, pl.ds(j * depth, depth)].reshape(total_rows, depth), wh[j, :, at], ((1,), (0,))
            )
            result = term if result is None else result + term
        return result

    for piece in (group, group + 1):
        for j in range(n):
            weight_arrived(j, piece)
    for batch in (0, 1):
        both = projected(batch, pl.ds(gq, 2 * HEAD_DIM))
        keys[batch] = turn(both[:, :HEAD_DIM], 1.0).astype(SLIM)
        values[batch] = both[:, HEAD_DIM:].astype(SLIM)

    def weigh(queries, key_block):
        masked = dot(queries, key_block, ((1,), (1,))) * scale + bias[...]
        numerators = jnp.exp(masked - jnp.max(masked, axis=-1, keepdims=True))
        return numerators, jnp.sum(numerators, axis=-1, keepdims=True)

    last = group - 1
    spans = ((0, last * HEAD_DIM), (last * HEAD_DIM, HEAD_DIM))

    def mixed_copy(block, i):
        at = pl.ds(*spans[i])
        return remote(
            mixed.at[block, :, at], mixed_in.at[group_at, :, at],
            asend.at[block, i], arecv.at[group_at, i], (served, block),
        )

    def elsewhere(block):
        return jnp.logical_not(jnp.logical_and(lead, me == block))

    def send_mixed(i, *blocks):
        for block in blocks:
            pl.when(elsewhere(block))(lambda: mixed_copy(block, i).start())

    def keep_mixed(i):
        @pl.when(lead)
        def _():
            at = pl.ds(*spans[i])
            mixed_in[group_at, :, at] = mixed[me, :, at]

    def forward_head(h):
        at = pl.ds(h * HEAD_DIM, HEAD_DIM)
        queries = turn(projected(0, at), 1.0).astype(SLIM)
        numerators, totals = weigh(queries, keys[0])
        result = dot(numerators.astype(SLIM), values[0], ((1,), (0,))) / totals
        mixed[:, :, at] = result.astype(SLIM).reshape(n, rows, HEAD_DIM)

    def backward_head(h):
        at = pl.ds(h * HEAD_DIM, HEAD_DIM)
        queries = turn(projected(1, at), 1.0).astype(SLIM)
        numerators, totals = weigh(queries, keys[1])
        rounded = numerators.astype(SLIM)
        summed = dot(rounded, values[1], ((1,), (0,)))
        summed_grad = mg[:, :, at].reshape(total_rows, HEAD_DIM).astype(WIDE) / totals
        totals_grad = -jnp.sum(summed_grad * (summed / totals), axis=-1, keepdims=True)
        narrow_grad = summed_grad.astype(SLIM)
        numer_grad = dot(narrow_grad, values[1], ((1,), (1,))) + totals_grad
        score_grad = (numerators * numer_grad * scale).astype(SLIM)
        query_grad = dot(score_grad, keys[1], ((1,), (0,))).astype(SLIM)
        dqkv[:, at] = turn(query_grad.astype(WIDE), -1.0).astype(SLIM)
        dkey[...] += dot(score_grad, queries, ((0,), (0,)))
        dval[...] += dot(rounded, narrow_grad, ((0,), (0,)))

    dkey[...] = jnp.zeros_like(dkey)
    dval[...] = jnp.zeros_like(dval)

    for h in range(group):
        for j in range(n):
            weight_arrived(j, h)
        if h == last:
            send_mixed(0, far, near)
        if h == 0:
            for block in range(n):
                pl.when(elsewhere(block))(
                    lambda: remote(
                        mg.at[block], mg.at[block], msend.at[0], mrecv.at[block], (section, me)
                    ).wait_recv()
                )
        backward_head(h)
        if h < last:
            forward_head(h)
        if h == last - 1:
            send_mixed(0, partner, me)
            keep_mixed(0)

    dqkv[:, pl.ds(gq, HEAD_DIM)] = turn(dkey[...].astype(SLIM).astype(WIDE), -1.0).astype(SLIM)
    dqkv[:, pl.ds(gq + HEAD_DIM, HEAD_DIM)] = dval[...].astype(SLIM)

    def partial_grads(first):
        block_rows = dqkv[pl.ds(pl.multiple_of(first * rows, 16), half * rows), :]
        for j in range(n):
            part[pl.ds(first, half), :, pl.ds(j * depth, depth)] = (
                dot(block_rows, wh[j], ((1,), (1,))).astype(SLIM).reshape(half, rows, depth)
            )

    chunks = row_chunks(rows)

    def mate_sum(block, c):
        at = pl.ds(*chunks[c])
        return remote(
            part.at[block, at], from_mate.at[block, at], bsend.at[block, c], brecv.at[block, c], (mate, me)
        )

    def partner_sum(block, c):
        at = pl.ds(*chunks[c])
        return remote(
            part.at[block, at], from_z.at[block, at], zsend.at[block, c], zrecv.at[block, c], (section, partner)
        )

    def owner_sum(block, c):
        at = pl.ds(*chunks[c])
        return remote(part.at[block, at], dn.at[at], osend.at[block, c], orecv.at[c], (section, block))

    def each_chunk(*blocks):
        return [(block, c) for block in blocks for c in range(len(chunks))]

    def summed_part(block, c, *others):
        at = pl.ds(*chunks[c])
        value = part[block, at].astype(WIDE)
        for other in others:
            value += other[block, at].astype(WIDE)
        return value.astype(SLIM)

    trailing = jnp.logical_not(lead)
    at_lead_edge = jnp.logical_and(lead, at_edge)
    at_lead_inner = jnp.logical_and(lead, jnp.logical_not(at_edge))

    partial_grads((1 - side) * half)

    @pl.when(trailing)
    def _():
        for block, c in each_chunk(near, far):
            mate_sum(block, c).start()

    partial_grads(side * half)

    @pl.when(trailing)
    def _():
        for block, c in each_chunk(partner, me):
            mate_sum(block, c).start()

    def pass_on(block, c):
        mate_sum(block, c).wait_recv()
        part[block, pl.ds(*chunks[c])] = summed_part(block, c, from_mate)
        partner_sum(block, c).start()

    @pl.when(at_lead_inner)
    def _():
        for block, c in each_chunk(near):
            pass_on(block, c)

    forward_head(last)
    send_mixed(1, far, near, partner, me)
    keep_mixed(1)

    @pl.when(at_lead_inner)
    def _():
        for block, c in each_chunk(far, partner):
            pass_on(block, c)

    @pl.when(at_lead_edge)
    def _():
        for block, c in each_chunk(partner):
            pass_on(block, c)


    def finish_block(block):
        for c in range(len(chunks)):
            mate_sum(block, c).wait_recv()
            partner_sum(block, c).wait_recv()
            part[block, pl.ds(*chunks[c])] = summed_part(block, c, from_mate, from_z)
            owner_sum(block, c).start()

    pl.when(at_lead_edge)(lambda: finish_block(near))

    def back_copy(c):
        at = pl.ds(*chunks[c])
        return remote(grads.at[at], back.at[at], csend.at[c], crecv.at[c], (preceding, me))

    def give_back():
        for c, chunk in enumerate(chunks):
            at = pl.ds(*chunk)

            @pl.when(lead)
            def _():
                mate_sum(me, c).wait_recv()
                partner_sum(me, c).wait_recv()
                dn[at] = summed_part(me, c, from_mate, from_z)

            pl.when(trailing)(lambda: owner_sum(me, c).wait_recv())
            widened = saved[at].astype(WIDE)
            inverse = lax.rsqrt(jnp.mean(widened * widened, axis=-1, keepdims=True) + norm_eps)
            scaled = dn[at].astype(WIDE) * gain[...]
            inner_mean = jnp.mean(scaled * widened, axis=-1, keepdims=True)
            project_grad = inverse * scaled - widened * (inverse * inverse * inverse * inner_mean)
            grads[at] = up[at] + project_grad.astype(SLIM)
            back_copy(c).start()

    early = jnp.logical_and(at_lead_inner, core == 0)
    pl.when(early)(give_back)

    total = tokens[...].astype(WIDE)
    for j in range(n):
        def arrived():
            for i, span in enumerate(spans):
                dst = mixed_in.at[j, :, pl.ds(*span)]
                remote(dst, dst, asend.at[0, 0], arecv.at[j, i], (section, me)).wait_recv()

        pl.when(jnp.logical_not(here(j)))(arrived)
        total += jnp.dot(mixed_in[j], wo[pl.ds(j * gq, gq), :], preferred_element_type=WIDE)
    produced[...] = total.astype(SLIM)
    ahead_copy = remote(produced, ahead, csend.at[len(chunks)], crecv.at[len(chunks)], (following, me))
    ahead_copy.start()
    pl.when(at_lead_edge)(lambda: finish_block(far))

    pl.when(jnp.logical_not(early))(give_back)

    @pl.when(lead)
    def _():
        for batch in (0, 1):
            for block in range(n):
                to_mate(batch, block).wait_send()
            to_partner(batch, me).wait_send()
            for block in (near, far):
                pl.when(at_edge)(lambda: to_partner(batch, block).wait_send())

    @pl.when(jnp.logical_not(lead))
    def _():
        for batch in (0, 1):
            to_edge(batch).wait_send()

    for k in range(1, n):
        place_copy(k).wait_send()
    for j in range(n):
        @pl.when(jnp.logical_not(here(j)))
        def _():
            for piece in range(pieces):
                weight_copy(j, piece).wait_send()
            grad_copy(j).wait_send()

        @pl.when(elsewhere(j))
        def _():
            for i in range(len(spans)):
                mixed_copy(j, i).wait_send()

    @pl.when(trailing)
    def _():
        for block, c in each_chunk(*range(n)):
            mate_sum(block, c).wait_send()

    @pl.when(lead)
    def _():
        for _, c in each_chunk(partner):
            partner_sum(partner, c).wait_send()
        for block, c in each_chunk(near, far):
            pl.when(at_edge)(lambda: owner_sum(block, c).wait_send())
            pl.when(jnp.logical_not(at_edge))(lambda: partner_sum(block, c).wait_send())

    ahead_copy.wait()
    for c in range(len(chunks)):
        back_copy(c).wait()


def hand_kernel(first, second, first_out, second_out, block, sems):
    takes = [pltpu.make_async_copy(ref, block.at[i], sems.at[i]) for i, ref in enumerate((first, second))]
    gives = [
        pltpu.make_async_copy(block.at[i], ref, sems.at[i + 2]) for i, ref in enumerate((first_out, second_out))
    ]
    for take in takes:
        take.start()
    for take, give in zip(takes, gives):
        take.wait()
        give.start()
    for give in gives:
        give.wait()


def by_pairs(n, sections):
    def step(
        section_inputs, saved_inputs, output_grads, token_positions, norm_gain,
        query_weight, keyval_weight, output_weight,
    ):
        _, rows, width = section_inputs.shape
        _, depth, query_width = query_weight.shape
        gq = query_width // n
        group = gq // HEAD_DIM
        wide = gq + keyval_weight.shape[2] // n

        chunks = len(row_chunks(rows))

        half_dim = HEAD_DIM // 2
        frequency = rope_base ** (-2.0 * np.arange(half_dim) / HEAD_DIM)
        signs = np.ones(half_dim)
        waves = jnp.asarray(
            np.stack([np.concatenate([frequency, frequency]), np.concatenate([-signs, signs])]), WIDE
        )

        def shaped(shape, kind=SLIM):
            return jax.ShapeDtypeStruct(shape, kind)

        def held(*shape, kind=SLIM):
            return pltpu.VMEM(shape, kind)

        pair = (shaped((rows, width)), shaped((rows, width)))
        dma = pltpu.SemaphoreType.DMA
        ahead, back = pl.pallas_call(
            functools.partial(layer_kernel, n, sections),
            out_shape=pair,
            in_specs=[ANY] * 9,
            out_specs=(VMEM,) * 2,
            scratch_shapes=[
                *[held(rows, width)] * 3, held(1, width, kind=WIDE), held(1, rows, kind=jnp.int32),
                held(2, HEAD_DIM, kind=WIDE), held(2, n, rows, width), held(2, rows, width),
                held(n, rows, gq), held(n, rows, gq), held(query_width, width), held(n, depth, wide),
                held(n, 1, rows, kind=jnp.int32), held(n * rows, n * rows, kind=WIDE),
                held(n * rows, HEAD_DIM, kind=WIDE), held(n * rows, HEAD_DIM, kind=WIDE),
                held(2, n * rows, HEAD_DIM), held(2, n * rows, HEAD_DIM),
                held(n * rows, HEAD_DIM, kind=WIDE), held(n * rows, HEAD_DIM, kind=WIDE),
                held(n, rows, gq), held(n, rows, gq), held(n * rows, wide),
                held(n, rows, width), held(n, rows, width), held(n, rows, width), held(rows, width),
                held(rows, width), held(rows, width),
                dma((2, 2, n)), dma((2, n)), dma((n, group + 2)), dma((n, group + 2)),
                *[dma((n,))] * 4, *[dma((n, 2))] * 2, *[dma((n, chunks))] * 5, dma((chunks,)),
                *[dma((chunks + 1,))] * 2, dma((7,)),
            ],
            compiler_params=pltpu.CompilerParams(
                collective_id=0, has_side_effects=True, vmem_limit_bytes=60 * 2**20
            ),
            name="layer",
        )(
            section_inputs[0], saved_inputs[0], output_grads[0], norm_gain, output_weight[0],
            query_weight[0], keyval_weight[0], token_positions[None], waves,
        )
        ahead, back = pl.pallas_call(
            hand_kernel, out_shape=pair, in_specs=[ANY] * 2, out_specs=(ANY,) * 2,
            scratch_shapes=[held(2, rows, width), dma((4,))], name="hand",
        )(ahead, back)
        return (ahead[None], back[None])

    return step


def solution(mesh):
    placed = (
        P("section", "ctx", None),
        P("section", "ctx", None),
        P("section", "ctx", None),
        P("ctx"),
        P("section", None),
        P("section", "ctx", None),
        P("section", "ctx", None),
        P("section", None, None),
    )
    n, sections = mesh.shape["ctx"], mesh.shape["section"]

    def chosen(*blocks):
        kv_heads = blocks[6].shape[2] // (2 * HEAD_DIM)
        rows, query_heads = blocks[0].shape[1], blocks[5].shape[2] // HEAD_DIM
        paired = n == 4 and sections > 2 and sections % 2 == 0
        if paired and kv_heads == n and query_heads > n and rows % 16 == 0:
            return by_pairs(n, sections)(*blocks)
        return shards(*blocks)

    return jax.shard_map(
        chosen,
        mesh=mesh,
        in_specs=placed,
        out_specs=(P("section", "ctx", None), P("section", "ctx", None)),
        check_vma=False,
    )
```

```python
import functools

import jax
import jax.numpy as jnp
import numpy as np
from jax import lax
from jax.experimental import pallas as pl
from jax.experimental.pallas import tpu as pltpu
from jax.sharding import PartitionSpec as P

HEAD_DIM = 128


norm_eps = 1e-05
rope_base = 500000.0


def from_behind(block, axis, distance):
    devices = range(lax.axis_size(axis))
    route = [((i - distance) % len(devices), i) for i in devices]
    return lax.ppermute(block, axis, route)


def rotate(matrix, positions):
    half_dim = matrix.shape[-1] // 2
    frequency = rope_base ** (-2.0 * jnp.arange(half_dim, dtype=jnp.float32) / matrix.shape[-1])
    angles = positions.astype(jnp.float32)[:, None] * frequency[None, :]
    cos_table = jnp.cos(angles)[:, None, :]
    sin_table = jnp.sin(angles)[:, None, :]
    leading = matrix[..., :half_dim]
    trailing = matrix[..., half_dim:]
    return jnp.concatenate(
        [leading * cos_table - trailing * sin_table, trailing * cos_table + leading * sin_table],
        axis=-1,
    )


def project(tokens, gain, query_matrix, keyval_matrix, positions):
    widened = tokens.astype(jnp.float32)
    inverse = lax.rsqrt(jnp.mean(widened * widened, axis=-1, keepdims=True) + norm_eps)
    normed = (widened * inverse * gain[None, :]).astype(jnp.bfloat16)
    row_count = tokens.shape[0]
    query_full = jnp.dot(normed, query_matrix, preferred_element_type=jnp.float32)
    keyval_full = jnp.dot(normed, keyval_matrix, preferred_element_type=jnp.float32)
    queries = rotate(query_full.reshape(row_count, -1, HEAD_DIM), positions).astype(jnp.bfloat16)
    paired = keyval_full.reshape(row_count, 2, -1, HEAD_DIM)
    key_rows = rotate(paired[:, 0], positions).astype(jnp.bfloat16)
    value_rows = paired[:, 1].astype(jnp.bfloat16)
    return (queries, key_rows, value_rows)


def attend(queries, key_wide, value_wide, query_pos, key_pos, narrow):
    row_count = queries.shape[0]
    kv_count = key_wide.shape[1]
    head_size = queries.shape[2]
    group_size = queries.shape[1] // kv_count
    grouped = jnp.moveaxis(queries.reshape(row_count, kv_count, group_size, head_size), 1, 0)
    key_heads = jnp.moveaxis(key_wide, 1, 0)
    value_heads = jnp.moveaxis(value_wide, 1, 0)
    visible = (key_pos[None, :] <= query_pos[:, None])[None]

    def one_head(block):
        query_block, key_block, value_block = block
        scores = jnp.einsum(
            "rgd,sd->grs", query_block, key_block, preferred_element_type=jnp.float32
        ) * head_size ** (-0.5)
        masked = jnp.where(visible, scores, -1e30)
        row_max = lax.stop_gradient(jnp.max(masked, axis=-1, keepdims=True))
        numerators = jnp.where(visible, jnp.exp(masked - row_max), 0.0)
        totals = jnp.sum(numerators, axis=-1)
        if narrow:
            rounded = numerators.astype(jnp.bfloat16)
        else:
            rounded = lax.optimization_barrier(numerators.astype(jnp.bfloat16)).astype(jnp.float32)
        summed = jnp.einsum("grs,sd->rgd", rounded, value_block, preferred_element_type=jnp.float32)
        return summed / jnp.transpose(totals, (1, 0))[..., None]

    averaged = lax.map(one_head, (grouped, key_heads, value_heads))
    return jnp.moveaxis(averaged, 0, 1).reshape(row_count, -1).astype(jnp.bfloat16)


def finish(tokens, mixed, output_matrix):
    return (
        tokens.astype(jnp.float32)
        + jnp.dot(mixed, output_matrix, preferred_element_type=jnp.float32)
    ).astype(jnp.bfloat16)


def shards(
    section_inputs,
    saved_inputs,
    output_grads,
    token_positions,
    norm_gain,
    query_weight,
    keyval_weight,
    output_weight,
):
    key_positions = lax.all_gather(token_positions, "ctx", axis=0, tiled=True)
    full_query, full_keyval = (
        lax.all_gather(query_weight[0], "ctx", axis=0, tiled=True),
        lax.all_gather(keyval_weight[0], "ctx", axis=0, tiled=True),
    )
    full_output = output_weight[0]
    gain = norm_gain[0]
    forward_tokens = section_inputs[0]
    saved_tokens = saved_inputs[0]
    upstream = output_grads[0]

    def projector(tokens):
        return project(tokens, gain, full_query, full_keyval, token_positions)

    def attention_wide(queries, key_wide, value_wide):
        return attend(queries, key_wide, value_wide, token_positions, key_positions, False)

    def finishing(tokens, mixed):
        return finish(tokens, mixed, full_output)

    forward_queries, forward_keys, forward_values = projector(forward_tokens)
    (backward_queries, backward_keys, backward_values), back_project = jax.vjp(
        projector, saved_tokens
    )
    forward_keyset, forward_valueset = (
        lax.all_gather(forward_keys, "ctx", axis=0, tiled=True),
        lax.all_gather(forward_values, "ctx", axis=0, tiled=True),
    )
    mixed = attend(
        forward_queries, forward_keyset, forward_valueset, token_positions, key_positions, True
    )
    produced = finishing(forward_tokens, mixed)
    sent_on = from_behind(produced[None], "section", 1)
    backward_keyset, backward_valueset = (
        lax.all_gather(backward_keys, "ctx", axis=0, tiled=True),
        lax.all_gather(backward_values, "ctx", axis=0, tiled=True),
    )
    mixed, back_attend = jax.vjp(
        attention_wide,
        backward_queries.astype(jnp.float32),
        backward_keyset.astype(jnp.float32),
        backward_valueset.astype(jnp.float32),
    )
    produced, back_finish = jax.vjp(finishing, saved_tokens, mixed)
    residual_grad, mixed_grad = back_finish(upstream)
    query_grad, key_partial, value_partial = back_attend(mixed_grad)
    key_grads = lax.psum_scatter(
        key_partial.astype(jnp.bfloat16), "ctx", scatter_dimension=0, tiled=True
    )
    value_grads = lax.psum_scatter(
        value_partial.astype(jnp.bfloat16), "ctx", scatter_dimension=0, tiled=True
    )
    (project_grad,) = back_project((query_grad.astype(jnp.bfloat16), key_grads, value_grads))
    sent_back = from_behind((residual_grad + project_grad)[None], "section", -1)
    return (sent_on, sent_back)


MESH = pl.DeviceIdType.MESH
VMEM = pl.BlockSpec(memory_space=pltpu.VMEM)
ANY = pl.BlockSpec(memory_space=pl.ANY)
WIDE = jnp.float32
SLIM = jnp.bfloat16


def remote(src, dst, send, recv, device):
    return pltpu.make_async_remote_copy(
        src_ref=src, dst_ref=dst, send_sem=send, recv_sem=recv, device_id=device, device_id_type=MESH
    )


HBM = pl.BlockSpec(memory_space=pltpu.HBM)


def row_chunks(rows):
    tiles = rows // 16
    sizes = [size * 16 for size in ((tiles - 1) - (tiles - 1) // 2, (tiles - 1) // 2, 1) if size]
    return [(sum(sizes[:i]), size) for i, size in enumerate(sizes)]


def layer_kernel(
    n, sections, tokens_hbm, saved_hbm, up_hbm, gain_hbm, wo_hbm, wq, wkv, pos_hbm, waves_hbm, ahead, back,
    tokens, saved, up, gain, pos, waves, nx, mine, mgl, mg, wo, wh, posg, bias, cos, sin, keys, values, dkey, dval, mixed, mixed_in, dqkv,
    part, from_mate, from_z, dn, produced, grads,
    nsend, nrecv, wsend, wrecv, msend, mrecv, psend, precv, asend, arecv, bsend, brecv, zsend, zrecv,
    osend, orecv, csend, crecv, own,
):
    section = lax.axis_index("section")
    me = lax.axis_index("ctx")
    half = n // 2
    core = lax.rem(section, 2)
    base = section - core
    mate = base + 1 - core
    side = me // half
    served = base + side
    lead = core == side
    partner = 2 * side * half + half - 1 - me
    edge = half - 1 + side
    at_edge = me == edge
    group_at = lax.rem(me, half) * 2 + core
    near, far = half - side, (n - 1) * (1 - side)
    depth, _ = wq.shape
    rows, width = tokens.shape
    gq = mg.shape[2]
    group = gq // HEAD_DIM
    kv_half = wkv.shape[1] // 2
    total_rows = n * rows
    scale = HEAD_DIM ** (-0.5)
    following, preceding = lax.rem(section + 1, sections), lax.rem(section + sections - 1, sections)
    pieces = group + 2

    barrier = pltpu.get_barrier_semaphore()
    for k in range(1, n):
        for other in (section, mate):
            pl.semaphore_signal(barrier, inc=1, device_id=(other, lax.rem(me + k, n)), device_id_type=MESH)
    for other in (mate, following, preceding):
        pl.semaphore_signal(barrier, inc=1, device_id=(other, me), device_id_type=MESH)

    loads = [
        pltpu.make_async_copy(src, dst, own.at[i])
        for i, (src, dst) in enumerate(
            (
                (gain_hbm, gain), (tokens_hbm, tokens), (saved_hbm, saved), (pos_hbm, pos), (up_hbm, up),
                (waves_hbm, waves), (wo_hbm, wo),
            )
        )
    ]
    for load in loads:
        load.start()

    def normed(block):
        widened = block[...].astype(WIDE)
        inverse = lax.rsqrt(jnp.mean(widened * widened, axis=-1, keepdims=True) + norm_eps)
        return (widened * inverse * gain[...]).astype(SLIM)

    for load in loads[:4]:
        load.wait()
    for batch, block in enumerate((tokens, saved)):
        mine[batch] = normed(block)

    @pl.when(lead)
    def _():
        for batch in (0, 1):
            nx[batch, me] = mine[batch]

    posg[me] = pos[...]
    pl.semaphore_wait(barrier, 2 * n + 1)

    def seat(owner_core, j):
        return (base + lax.rem(j, 2), owner_core * half + j // 2)

    def token_copy(batch, lane, src, block, device):
        return remote(src, nx.at[batch, block], nsend.at[batch, lane, block], nrecv.at[batch, block], device)

    def to_mate(batch, block):
        return token_copy(batch, 0, nx.at[batch, block], block, (mate, me))

    def to_partner(batch, block):
        return token_copy(batch, 1, nx.at[batch, block], block, (section, partner))

    def to_edge(batch):
        return token_copy(batch, 0, mine.at[batch], me, (section, half - 1 + core))

    def piece_source(j, piece):
        if piece < group:
            start = j * gq + piece * HEAD_DIM
            return wq.at[:, pl.ds(pl.multiple_of(start, HEAD_DIM), HEAD_DIM)], piece * HEAD_DIM
        start = (piece - group) * kv_half + j * HEAD_DIM
        return wkv.at[:, pl.ds(pl.multiple_of(start, HEAD_DIM), HEAD_DIM)], piece * HEAD_DIM

    def weight_copy(j, piece):
        src, to = piece_source(j, piece)
        return remote(
            src, wh.at[me, :, pl.ds(to, HEAD_DIM)], wsend.at[j, piece], wrecv.at[me, piece], seat(core, j)
        )

    def weight_here(j, piece):
        src, to = piece_source(j, piece)
        return pltpu.make_async_copy(src, wh.at[me, :, pl.ds(to, HEAD_DIM)], wrecv.at[me, piece])

    def weight_arrived(block, piece):
        dst = wh.at[block, :, pl.ds(piece * HEAD_DIM, HEAD_DIM)]
        remote(dst, dst, wsend.at[0, 0], wrecv.at[block, piece], (section, me)).wait_recv()

    def here(j):
        return jnp.logical_and(lead, group_at == j)

    def send_weights(piece):
        for i in range(n):
            j = lax.rem(i + core * half, n)
            pl.when(here(j))(lambda: weight_here(j, piece).start())
            pl.when(jnp.logical_not(here(j)))(lambda: weight_copy(j, piece).start())

    def grad_copy(j):
        return remote(mgl.at[j], mg.at[me], msend.at[j], mrecv.at[me], seat(core, j))

    def place_copy(k):
        return remote(pos, posg.at[me], psend.at[k], precv.at[me], (section, lax.rem(me + k, n)))

    @pl.when(lead)
    def _():
        for batch in (0, 1):
            to_partner(batch, me).start()
        for batch in (0, 1):
            to_mate(batch, me).start()

    @pl.when(jnp.logical_not(lead))
    def _():
        for batch in (0, 1):
            to_edge(batch).start()

    for k in range(1, n):
        place_copy(k).start()
    send_weights(group)
    send_weights(group + 1)

    for load in loads[4:]:
        load.wait()
    for j in range(n):
        mgl[j] = lax.dot_general(
            up[...], wo[pl.ds(j * gq, gq), :], (((1,), (1,)), ((), ())), preferred_element_type=WIDE
        ).astype(SLIM)
    for j in range(n):
        @pl.when(here(j))
        def _():
            mg[me] = mgl[j]

        pl.when(jnp.logical_not(here(j)))(lambda: grad_copy(j).start())

    @pl.when(jnp.logical_not(lead))
    def _():
        for piece in range(group):
            send_weights(piece)

    def token_arrived(batch, block):
        dst = nx.at[batch, block]
        remote(dst, dst, nsend.at[0, 0, 0], nrecv.at[batch, block], (section, me)).wait_recv()

    @pl.when(lead)
    def _():
        for batch in (0, 1):
            for block, outer in ((partner, False), (near, True), (far, True)):
                token_arrived(batch, block)
                if outer:
                    pl.when(at_edge)(lambda: to_partner(batch, block).start())
                to_mate(batch, block).start()
        for piece in range(group):
            send_weights(piece)

    for k in range(1, n):
        source = lax.rem(me + k, n)
        remote(pos, posg.at[source], psend.at[0], precv.at[source], (section, me)).wait_recv()
    columns = []
    for j in range(n):
        column = jnp.transpose(jnp.broadcast_to(posg[j].astype(WIDE), (HEAD_DIM, rows)))
        angles = column * waves[0:1, :]
        at = pl.ds(j * rows, rows)
        cos[at, :] = jnp.cos(angles)
        sin[at, :] = jnp.sin(angles) * waves[1:2, :]
        columns.append(column)
    column = jnp.concatenate(columns, axis=0)
    bias[...] = jnp.where(jnp.transpose(column)[0:1, :] <= column[:, 0:1], 0.0, -1e30)

    @pl.when(jnp.logical_not(lead))
    def _():
        for batch in (0, 1):
            for block in range(n):
                token_arrived(batch, block)

    def turn(block, sign):
        return block * cos[...] + sign * (pltpu.roll(block, HEAD_DIM // 2, 1) * sin[...])

    def dot(a, b, dims):
        return lax.dot_general(a, b, (dims, ((), ())), preferred_element_type=WIDE)

    def projected(batch, at):
        result = None
        for j in range(n):
            term = dot(
                nx[batch, :, :, pl.ds(j * depth, depth)].reshape(total_rows, depth), wh[j, :, at], ((1,), (0,))
            )
            result = term if result is None else result + term
        return result

    for piece in (group, group + 1):
        for j in range(n):
            weight_arrived(j, piece)
    for batch in (0, 1):
        both = projected(batch, pl.ds(gq, 2 * HEAD_DIM))
        keys[batch] = turn(both[:, :HEAD_DIM], 1.0).astype(SLIM)
        values[batch] = both[:, HEAD_DIM:].astype(SLIM)

    def weigh(queries, key_block):
        masked = dot(queries, key_block, ((1,), (1,))) * scale + bias[...]
        numerators = jnp.exp(masked - jnp.max(masked, axis=-1, keepdims=True))
        return numerators, jnp.sum(numerators, axis=-1, keepdims=True)

    last = group - 1
    spans = ((0, last * HEAD_DIM), (last * HEAD_DIM, HEAD_DIM))

    def mixed_copy(block, i):
        at = pl.ds(*spans[i])
        return remote(
            mixed.at[block, :, at], mixed_in.at[group_at, :, at],
            asend.at[block, i], arecv.at[group_at, i], (served, block),
        )

    def elsewhere(block):
        return jnp.logical_not(jnp.logical_and(lead, me == block))

    def send_mixed(i, *blocks):
        for block in blocks:
            pl.when(elsewhere(block))(lambda: mixed_copy(block, i).start())

    def keep_mixed(i):
        @pl.when(lead)
        def _():
            at = pl.ds(*spans[i])
            mixed_in[group_at, :, at] = mixed[me, :, at]

    def forward_head(h):
        at = pl.ds(h * HEAD_DIM, HEAD_DIM)
        queries = turn(projected(0, at), 1.0).astype(SLIM)
        numerators, totals = weigh(queries, keys[0])
        result = dot(numerators.astype(SLIM), values[0], ((1,), (0,))) / totals
        mixed[:, :, at] = result.astype(SLIM).reshape(n, rows, HEAD_DIM)

    def backward_head(h):
        at = pl.ds(h * HEAD_DIM, HEAD_DIM)
        queries = turn(projected(1, at), 1.0).astype(SLIM)
        numerators, totals = weigh(queries, keys[1])
        rounded = numerators.astype(SLIM)
        summed = dot(rounded, values[1], ((1,), (0,)))
        summed_grad = mg[:, :, at].reshape(total_rows, HEAD_DIM).astype(WIDE) / totals
        totals_grad = -jnp.sum(summed_grad * (summed / totals), axis=-1, keepdims=True)
        narrow_grad = summed_grad.astype(SLIM)
        numer_grad = dot(narrow_grad, values[1], ((1,), (1,))) + totals_grad
        score_grad = (numerators * numer_grad * scale).astype(SLIM)
        query_grad = dot(score_grad, keys[1], ((1,), (0,))).astype(SLIM)
        dqkv[:, at] = turn(query_grad.astype(WIDE), -1.0).astype(SLIM)
        dkey[...] += dot(score_grad, queries, ((0,), (0,)))
        dval[...] += dot(rounded, narrow_grad, ((0,), (0,)))

    dkey[...] = jnp.zeros_like(dkey)
    dval[...] = jnp.zeros_like(dval)

    for h in range(group):
        for j in range(n):
            weight_arrived(j, h)
        if h == 0:
            for block in range(n):
                pl.when(elsewhere(block))(
                    lambda: remote(
                        mg.at[block], mg.at[block], msend.at[0], mrecv.at[block], (section, me)
                    ).wait_recv()
                )
        backward_head(h)
        if h < last:
            forward_head(h)
        if h == last - 1:
            send_mixed(0, partner, me)
            keep_mixed(0)

    dqkv[:, pl.ds(gq, HEAD_DIM)] = turn(dkey[...].astype(SLIM).astype(WIDE), -1.0).astype(SLIM)
    dqkv[:, pl.ds(gq + HEAD_DIM, HEAD_DIM)] = dval[...].astype(SLIM)
    send_mixed(0, far, near)

    def partial_grads(first):
        block_rows = dqkv[pl.ds(pl.multiple_of(first * rows, 16), half * rows), :]
        for j in range(n):
            part[pl.ds(first, half), :, pl.ds(j * depth, depth)] = (
                dot(block_rows, wh[j], ((1,), (1,))).astype(SLIM).reshape(half, rows, depth)
            )

    chunks = row_chunks(rows)

    def mate_sum(block, c):
        at = pl.ds(*chunks[c])
        return remote(
            part.at[block, at], from_mate.at[block, at], bsend.at[block, c], brecv.at[block, c], (mate, me)
        )

    def partner_sum(block, c):
        at = pl.ds(*chunks[c])
        return remote(
            part.at[block, at], from_z.at[block, at], zsend.at[block, c], zrecv.at[block, c], (section, partner)
        )

    def owner_sum(block, c):
        at = pl.ds(*chunks[c])
        return remote(part.at[block, at], dn.at[at], osend.at[block, c], orecv.at[c], (section, block))

    def each_chunk(*blocks):
        return [(block, c) for block in blocks for c in range(len(chunks))]

    def summed_part(block, c, *others):
        at = pl.ds(*chunks[c])
        value = part[block, at].astype(WIDE)
        for other in others:
            value += other[block, at].astype(WIDE)
        return value.astype(SLIM)

    trailing = jnp.logical_not(lead)
    at_lead_edge = jnp.logical_and(lead, at_edge)
    at_lead_inner = jnp.logical_and(lead, jnp.logical_not(at_edge))

    partial_grads((1 - side) * half)

    @pl.when(trailing)
    def _():
        for block, c in each_chunk(near, far):
            mate_sum(block, c).start()

    partial_grads(side * half)

    @pl.when(trailing)
    def _():
        for block, c in each_chunk(partner, me):
            mate_sum(block, c).start()

    def pass_on(block, c):
        mate_sum(block, c).wait_recv()
        part[block, pl.ds(*chunks[c])] = summed_part(block, c, from_mate)
        partner_sum(block, c).start()

    @pl.when(at_lead_inner)
    def _():
        for block, c in each_chunk(near):
            pass_on(block, c)

    forward_head(last)
    send_mixed(1, far, near, partner, me)
    keep_mixed(1)

    @pl.when(at_lead_inner)
    def _():
        for block, c in each_chunk(far, partner):
            pass_on(block, c)

    @pl.when(at_lead_edge)
    def _():
        for block, c in each_chunk(partner):
            pass_on(block, c)


    def finish_block(block):
        for c in range(len(chunks)):
            mate_sum(block, c).wait_recv()
            partner_sum(block, c).wait_recv()
            part[block, pl.ds(*chunks[c])] = summed_part(block, c, from_mate, from_z)
            owner_sum(block, c).start()

    pl.when(at_lead_edge)(lambda: finish_block(near))

    def back_copy(c):
        at = pl.ds(*chunks[c])
        return remote(grads.at[at], back.at[at], csend.at[c], crecv.at[c], (preceding, me))

    def give_back():
        for c, chunk in enumerate(chunks):
            at = pl.ds(*chunk)

            @pl.when(lead)
            def _():
                mate_sum(me, c).wait_recv()
                partner_sum(me, c).wait_recv()
                dn[at] = summed_part(me, c, from_mate, from_z)

            pl.when(trailing)(lambda: owner_sum(me, c).wait_recv())
            widened = saved[at].astype(WIDE)
            inverse = lax.rsqrt(jnp.mean(widened * widened, axis=-1, keepdims=True) + norm_eps)
            scaled = dn[at].astype(WIDE) * gain[...]
            inner_mean = jnp.mean(scaled * widened, axis=-1, keepdims=True)
            project_grad = inverse * scaled - widened * (inverse * inverse * inverse * inner_mean)
            grads[at] = up[at] + project_grad.astype(SLIM)
            back_copy(c).start()

    early = jnp.logical_and(at_lead_inner, core == 0)
    pl.when(early)(give_back)

    total = tokens[...].astype(WIDE)
    for j in range(n):
        def arrived():
            for i, span in enumerate(spans):
                dst = mixed_in.at[j, :, pl.ds(*span)]
                remote(dst, dst, asend.at[0, 0], arecv.at[j, i], (section, me)).wait_recv()

        pl.when(jnp.logical_not(here(j)))(arrived)
        total += jnp.dot(mixed_in[j], wo[pl.ds(j * gq, gq), :], preferred_element_type=WIDE)
    produced[...] = total.astype(SLIM)
    ahead_copy = remote(produced, ahead, csend.at[len(chunks)], crecv.at[len(chunks)], (following, me))
    ahead_copy.start()
    pl.when(at_lead_edge)(lambda: finish_block(far))

    pl.when(jnp.logical_not(early))(give_back)

    @pl.when(lead)
    def _():
        for batch in (0, 1):
            for block in range(n):
                to_mate(batch, block).wait_send()
            to_partner(batch, me).wait_send()
            for block in (near, far):
                pl.when(at_edge)(lambda: to_partner(batch, block).wait_send())

    @pl.when(jnp.logical_not(lead))
    def _():
        for batch in (0, 1):
            to_edge(batch).wait_send()

    for k in range(1, n):
        place_copy(k).wait_send()
    for j in range(n):
        @pl.when(jnp.logical_not(here(j)))
        def _():
            for piece in range(pieces):
                weight_copy(j, piece).wait_send()
            grad_copy(j).wait_send()

        @pl.when(elsewhere(j))
        def _():
            for i in range(len(spans)):
                mixed_copy(j, i).wait_send()

    @pl.when(trailing)
    def _():
        for block, c in each_chunk(*range(n)):
            mate_sum(block, c).wait_send()

    @pl.when(lead)
    def _():
        for _, c in each_chunk(partner):
            partner_sum(partner, c).wait_send()
        for block, c in each_chunk(near, far):
            pl.when(at_edge)(lambda: owner_sum(block, c).wait_send())
            pl.when(jnp.logical_not(at_edge))(lambda: partner_sum(block, c).wait_send())

    ahead_copy.wait_send()
    for c in range(len(chunks)):
        back_copy(c).wait_send()
    ahead_copy.wait_recv()
    for c in range(len(chunks)):
        back_copy(c).wait_recv()


def by_pairs(n, sections):
    def step(
        section_inputs, saved_inputs, output_grads, token_positions, norm_gain,
        query_weight, keyval_weight, output_weight,
    ):
        _, rows, width = section_inputs.shape
        _, depth, query_width = query_weight.shape
        gq = query_width // n
        group = gq // HEAD_DIM
        wide = gq + keyval_weight.shape[2] // n

        chunks = len(row_chunks(rows))

        half_dim = HEAD_DIM // 2
        frequency = rope_base ** (-2.0 * np.arange(half_dim) / HEAD_DIM)
        signs = np.ones(half_dim)
        waves = jnp.asarray(
            np.stack([np.concatenate([frequency, frequency]), np.concatenate([-signs, signs])]), WIDE
        )

        def shaped(shape, kind=SLIM):
            return jax.ShapeDtypeStruct(shape, kind)

        def held(*shape, kind=SLIM):
            return pltpu.VMEM(shape, kind)

        pair = (shaped((rows, width)), shaped((rows, width)))
        dma = pltpu.SemaphoreType.DMA
        ahead, back = pl.pallas_call(
            functools.partial(layer_kernel, n, sections),
            out_shape=(pltpu.VMEM((rows, width), SLIM),) * 2,
            in_specs=[HBM] * 9,
            out_specs=(VMEM,) * 2,
            scratch_shapes=[
                *[held(rows, width)] * 3, held(1, width, kind=WIDE), held(1, rows, kind=jnp.int32),
                held(2, HEAD_DIM, kind=WIDE), held(2, n, rows, width), held(2, rows, width),
                held(n, rows, gq), held(n, rows, gq), held(query_width, width), held(n, depth, wide),
                held(n, 1, rows, kind=jnp.int32), held(n * rows, n * rows, kind=WIDE),
                held(n * rows, HEAD_DIM, kind=WIDE), held(n * rows, HEAD_DIM, kind=WIDE),
                held(2, n * rows, HEAD_DIM), held(2, n * rows, HEAD_DIM),
                held(n * rows, HEAD_DIM, kind=WIDE), held(n * rows, HEAD_DIM, kind=WIDE),
                held(n, rows, gq), held(n, rows, gq), held(n * rows, wide),
                held(n, rows, width), held(n, rows, width), held(n, rows, width), held(rows, width),
                held(rows, width), held(rows, width),
                dma((2, 2, n)), dma((2, n)), dma((n, group + 2)), dma((n, group + 2)),
                *[dma((n,))] * 4, *[dma((n, 2))] * 2, *[dma((n, chunks))] * 5, dma((chunks,)),
                *[dma((chunks + 1,))] * 2, dma((7,)),
            ],
            compiler_params=pltpu.CompilerParams(
                collective_id=0, has_side_effects=True, vmem_limit_bytes=67043328 - 4 * rows * width - 2**16
            ),
            name="layer",
        )(
            section_inputs[0], saved_inputs[0], output_grads[0], norm_gain, output_weight[0],
            query_weight[0], keyval_weight[0], token_positions[None], waves,
        )
        return (ahead[None], back[None])

    return step


def solution(mesh):
    placed = (
        P("section", "ctx", None),
        P("section", "ctx", None),
        P("section", "ctx", None),
        P("ctx"),
        P("section", None),
        P("section", "ctx", None),
        P("section", "ctx", None),
        P("section", None, None),
    )
    n, sections = mesh.shape["ctx"], mesh.shape["section"]

    def chosen(*blocks):
        kv_heads = blocks[6].shape[2] // (2 * HEAD_DIM)
        rows, query_heads = blocks[0].shape[1], blocks[5].shape[2] // HEAD_DIM
        paired = n == 4 and sections > 2 and sections % 2 == 0
        if paired and kv_heads == n and query_heads > n and rows % 16 == 0:
            return by_pairs(n, sections)(*blocks)
        return shards(*blocks)

    return jax.shard_map(
        chosen,
        mesh=mesh,
        in_specs=placed,
        out_specs=(P("section", "ctx", None), P("section", "ctx", None)),
        check_vma=False,
    )
```

```python
import functools

import jax
import jax.numpy as jnp
import numpy as np
from jax import lax
from jax.experimental import pallas as pl
from jax.experimental.pallas import tpu as pltpu
from jax.sharding import PartitionSpec as P

HEAD_DIM = 128


norm_eps = 1e-05
rope_base = 500000.0


def from_behind(block, axis, distance):
    devices = range(lax.axis_size(axis))
    route = [((i - distance) % len(devices), i) for i in devices]
    return lax.ppermute(block, axis, route)


def rotate(matrix, positions):
    half_dim = matrix.shape[-1] // 2
    frequency = rope_base ** (-2.0 * jnp.arange(half_dim, dtype=jnp.float32) / matrix.shape[-1])
    angles = positions.astype(jnp.float32)[:, None] * frequency[None, :]
    cos_table = jnp.cos(angles)[:, None, :]
    sin_table = jnp.sin(angles)[:, None, :]
    leading = matrix[..., :half_dim]
    trailing = matrix[..., half_dim:]
    return jnp.concatenate(
        [leading * cos_table - trailing * sin_table, trailing * cos_table + leading * sin_table],
        axis=-1,
    )


def project(tokens, gain, query_matrix, keyval_matrix, positions):
    widened = tokens.astype(jnp.float32)
    inverse = lax.rsqrt(jnp.mean(widened * widened, axis=-1, keepdims=True) + norm_eps)
    normed = (widened * inverse * gain[None, :]).astype(jnp.bfloat16)
    row_count = tokens.shape[0]
    query_full = jnp.dot(normed, query_matrix, preferred_element_type=jnp.float32)
    keyval_full = jnp.dot(normed, keyval_matrix, preferred_element_type=jnp.float32)
    queries = rotate(query_full.reshape(row_count, -1, HEAD_DIM), positions).astype(jnp.bfloat16)
    paired = keyval_full.reshape(row_count, 2, -1, HEAD_DIM)
    key_rows = rotate(paired[:, 0], positions).astype(jnp.bfloat16)
    value_rows = paired[:, 1].astype(jnp.bfloat16)
    return (queries, key_rows, value_rows)


def attend(queries, key_wide, value_wide, query_pos, key_pos, narrow):
    row_count = queries.shape[0]
    kv_count = key_wide.shape[1]
    head_size = queries.shape[2]
    group_size = queries.shape[1] // kv_count
    grouped = jnp.moveaxis(queries.reshape(row_count, kv_count, group_size, head_size), 1, 0)
    key_heads = jnp.moveaxis(key_wide, 1, 0)
    value_heads = jnp.moveaxis(value_wide, 1, 0)
    visible = (key_pos[None, :] <= query_pos[:, None])[None]

    def one_head(block):
        query_block, key_block, value_block = block
        scores = jnp.einsum(
            "rgd,sd->grs", query_block, key_block, preferred_element_type=jnp.float32
        ) * head_size ** (-0.5)
        masked = jnp.where(visible, scores, -1e30)
        row_max = lax.stop_gradient(jnp.max(masked, axis=-1, keepdims=True))
        numerators = jnp.where(visible, jnp.exp(masked - row_max), 0.0)
        totals = jnp.sum(numerators, axis=-1)
        if narrow:
            rounded = numerators.astype(jnp.bfloat16)
        else:
            rounded = lax.optimization_barrier(numerators.astype(jnp.bfloat16)).astype(jnp.float32)
        summed = jnp.einsum("grs,sd->rgd", rounded, value_block, preferred_element_type=jnp.float32)
        return summed / jnp.transpose(totals, (1, 0))[..., None]

    averaged = lax.map(one_head, (grouped, key_heads, value_heads))
    return jnp.moveaxis(averaged, 0, 1).reshape(row_count, -1).astype(jnp.bfloat16)


def finish(tokens, mixed, output_matrix):
    return (
        tokens.astype(jnp.float32)
        + jnp.dot(mixed, output_matrix, preferred_element_type=jnp.float32)
    ).astype(jnp.bfloat16)


def shards(
    section_inputs,
    saved_inputs,
    output_grads,
    token_positions,
    norm_gain,
    query_weight,
    keyval_weight,
    output_weight,
):
    key_positions = lax.all_gather(token_positions, "ctx", axis=0, tiled=True)
    full_query, full_keyval = (
        lax.all_gather(query_weight[0], "ctx", axis=0, tiled=True),
        lax.all_gather(keyval_weight[0], "ctx", axis=0, tiled=True),
    )
    full_output = output_weight[0]
    gain = norm_gain[0]
    forward_tokens = section_inputs[0]
    saved_tokens = saved_inputs[0]
    upstream = output_grads[0]

    def projector(tokens):
        return project(tokens, gain, full_query, full_keyval, token_positions)

    def attention_wide(queries, key_wide, value_wide):
        return attend(queries, key_wide, value_wide, token_positions, key_positions, False)

    def finishing(tokens, mixed):
        return finish(tokens, mixed, full_output)

    forward_queries, forward_keys, forward_values = projector(forward_tokens)
    (backward_queries, backward_keys, backward_values), back_project = jax.vjp(
        projector, saved_tokens
    )
    forward_keyset, forward_valueset = (
        lax.all_gather(forward_keys, "ctx", axis=0, tiled=True),
        lax.all_gather(forward_values, "ctx", axis=0, tiled=True),
    )
    mixed = attend(
        forward_queries, forward_keyset, forward_valueset, token_positions, key_positions, True
    )
    produced = finishing(forward_tokens, mixed)
    sent_on = from_behind(produced[None], "section", 1)
    backward_keyset, backward_valueset = (
        lax.all_gather(backward_keys, "ctx", axis=0, tiled=True),
        lax.all_gather(backward_values, "ctx", axis=0, tiled=True),
    )
    mixed, back_attend = jax.vjp(
        attention_wide,
        backward_queries.astype(jnp.float32),
        backward_keyset.astype(jnp.float32),
        backward_valueset.astype(jnp.float32),
    )
    produced, back_finish = jax.vjp(finishing, saved_tokens, mixed)
    residual_grad, mixed_grad = back_finish(upstream)
    query_grad, key_partial, value_partial = back_attend(mixed_grad)
    key_grads = lax.psum_scatter(
        key_partial.astype(jnp.bfloat16), "ctx", scatter_dimension=0, tiled=True
    )
    value_grads = lax.psum_scatter(
        value_partial.astype(jnp.bfloat16), "ctx", scatter_dimension=0, tiled=True
    )
    (project_grad,) = back_project((query_grad.astype(jnp.bfloat16), key_grads, value_grads))
    sent_back = from_behind((residual_grad + project_grad)[None], "section", -1)
    return (sent_on, sent_back)


MESH = pl.DeviceIdType.MESH
VMEM = pl.BlockSpec(memory_space=pltpu.VMEM)
ANY = pl.BlockSpec(memory_space=pl.ANY)
WIDE = jnp.float32
SLIM = jnp.bfloat16


def remote(src, dst, send, recv, device):
    return pltpu.make_async_remote_copy(
        src_ref=src, dst_ref=dst, send_sem=send, recv_sem=recv, device_id=device, device_id_type=MESH
    )


HBM = pl.BlockSpec(memory_space=pltpu.HBM)


def row_chunks(rows):
    tiles = rows // 16
    singles = min(tiles, 3)
    rest = tiles - singles
    sizes = [size * 16 for size in (rest - rest // 2, rest // 2, *[1] * singles) if size]
    return [(sum(sizes[:i]), size) for i, size in enumerate(sizes)]


def layer_kernel(
    n, sections, tokens_hbm, saved_hbm, up_hbm, gain_hbm, wo_hbm, wq, wkv, pos_hbm, waves_hbm, ahead, back,
    tokens, saved, up, gain, pos, waves, nx, mine, mgl, mg, wo, wh, posg, bias, cos, sin, keys, values, dkey, dval, mixed, mixed_in, dqkv,
    part, from_mate, from_z, dn, produced, grads,
    nsend, nrecv, wsend, wrecv, msend, mrecv, psend, precv, asend, arecv, bsend, brecv, zsend, zrecv,
    osend, orecv, csend, crecv, own,
):
    section = lax.axis_index("section")
    me = lax.axis_index("ctx")
    half = n // 2
    core = lax.rem(section, 2)
    base = section - core
    mate = base + 1 - core
    side = me // half
    served = base + side
    lead = core == side
    partner = 2 * side * half + half - 1 - me
    edge = half - 1 + side
    at_edge = me == edge
    group_at = lax.rem(me, half) * 2 + core
    near, far = half - side, (n - 1) * (1 - side)
    depth, _ = wq.shape
    rows, width = tokens.shape
    gq = mg.shape[2]
    group = gq // HEAD_DIM
    kv_half = wkv.shape[1] // 2
    total_rows = n * rows
    scale = HEAD_DIM ** (-0.5)
    following, preceding = lax.rem(section + 1, sections), lax.rem(section + sections - 1, sections)

    barrier = pltpu.get_barrier_semaphore()
    for k in range(1, n):
        for other in (section, mate):
            pl.semaphore_signal(barrier, inc=1, device_id=(other, lax.rem(me + k, n)), device_id_type=MESH)
    for other in (mate, following, preceding):
        pl.semaphore_signal(barrier, inc=1, device_id=(other, me), device_id_type=MESH)

    loads = [
        pltpu.make_async_copy(src, dst, own.at[i])
        for i, (src, dst) in enumerate(
            (
                (gain_hbm, gain), (tokens_hbm, tokens), (saved_hbm, saved), (pos_hbm, pos), (up_hbm, up),
                (waves_hbm, waves), (wo_hbm, wo),
            )
        )
    ]
    for load in loads:
        load.start()

    def normed(block):
        widened = block[...].astype(WIDE)
        inverse = lax.rsqrt(jnp.mean(widened * widened, axis=-1, keepdims=True) + norm_eps)
        return (widened * inverse * gain[...]).astype(SLIM)

    for load in loads[:4]:
        load.wait()
    for batch, block in enumerate((tokens, saved)):
        mine[batch] = normed(block)

    @pl.when(lead)
    def _():
        for batch in (0, 1):
            nx[batch, me] = mine[batch]

    posg[me] = pos[...]
    pl.semaphore_wait(barrier, 2 * n + 1)

    def seat(owner_core, j):
        return (base + lax.rem(j, 2), owner_core * half + j // 2)

    def token_copy(batch, lane, src, block, device):
        return remote(src, nx.at[batch, block], nsend.at[batch, lane], nrecv.at[batch, block], device)

    def to_mate(batch, block):
        return token_copy(batch, 0, nx.at[batch, block], block, (mate, me))

    def to_partner(batch, block):
        return token_copy(batch, 1, nx.at[batch, block], block, (section, partner))

    def to_edge(batch):
        return token_copy(batch, 0, mine.at[batch], me, (section, half - 1 + core))

    def piece_source(j, piece):
        if piece < group:
            start = j * gq + piece * HEAD_DIM
            return wq.at[:, pl.ds(pl.multiple_of(start, HEAD_DIM), HEAD_DIM)], piece * HEAD_DIM
        start = (piece - group) * kv_half + j * HEAD_DIM
        return wkv.at[:, pl.ds(pl.multiple_of(start, HEAD_DIM), HEAD_DIM)], piece * HEAD_DIM

    def weight_copy(j, piece):
        src, to = piece_source(j, piece)
        return remote(
            src, wh.at[me, :, pl.ds(to, HEAD_DIM)], wsend.at[j], wrecv.at[min(piece, group)], seat(core, j)
        )

    def weight_here(j, piece):
        src, to = piece_source(j, piece)
        return pltpu.make_async_copy(src, wh.at[me, :, pl.ds(to, HEAD_DIM)], wrecv.at[min(piece, group)])

    def taken(dst, recv):
        remote(dst, dst, osend.at[0], recv, (section, me)).wait_recv()

    def given(src, send):
        remote(src, src, send, orecv.at[0], (section, me)).wait_send()

    def weight_arrived(piece):
        size = HEAD_DIM if piece < group else 2 * HEAD_DIM
        taken(wh.at[:, :, pl.ds(piece * HEAD_DIM, size)], wrecv.at[piece])

    def here(j):
        return jnp.logical_and(lead, group_at == j)

    def send_weights(piece):
        for i in range(n):
            j = lax.rem(i + core * half, n)
            pl.when(here(j))(lambda: weight_here(j, piece).start())
            pl.when(jnp.logical_not(here(j)))(lambda: weight_copy(j, piece).start())

    def grad_copy(j):
        return remote(mgl.at[j], mg.at[me], msend.at[0], mrecv.at[0], seat(core, j))

    def place_copy(k):
        return remote(pos, posg.at[me], psend.at[0], precv.at[0], (section, lax.rem(me + k, n)))

    @pl.when(lead)
    def _():
        for batch in (0, 1):
            to_partner(batch, me).start()
        for batch in (0, 1):
            to_mate(batch, me).start()

    @pl.when(jnp.logical_not(lead))
    def _():
        for batch in (0, 1):
            to_edge(batch).start()

    for k in range(1, n):
        place_copy(k).start()
    send_weights(group)
    send_weights(group + 1)

    for load in loads[4:]:
        load.wait()
    for j in range(n):
        mgl[j] = lax.dot_general(
            up[...], wo[pl.ds(j * gq, gq), :], (((1,), (1,)), ((), ())), preferred_element_type=WIDE
        ).astype(SLIM)
    for j in range(n):
        @pl.when(here(j))
        def _():
            mg[me] = mgl[j]

        pl.when(jnp.logical_not(here(j)))(lambda: grad_copy(j).start())

    @pl.when(jnp.logical_not(lead))
    def _():
        for piece in range(group):
            send_weights(piece)

    def token_arrived(batch, block):
        dst = nx.at[batch, block]
        remote(dst, dst, nsend.at[0, 0], nrecv.at[batch, block], (section, me)).wait_recv()

    @pl.when(lead)
    def _():
        for batch in (0, 1):
            for block, outer in ((partner, False), (near, True), (far, True)):
                token_arrived(batch, block)
                if outer:
                    pl.when(at_edge)(lambda: to_partner(batch, block).start())
                to_mate(batch, block).start()
        for piece in range(group):
            send_weights(piece)

    taken(posg.at[pl.ds(0, n - 1)], precv.at[0])
    columns = []
    for j in range(n):
        column = jnp.transpose(jnp.broadcast_to(posg[j].astype(WIDE), (HEAD_DIM, rows)))
        angles = column * waves[0:1, :]
        at = pl.ds(j * rows, rows)
        cos[at, :] = jnp.cos(angles)
        sin[at, :] = jnp.sin(angles) * waves[1:2, :]
        columns.append(column)
    column = jnp.concatenate(columns, axis=0)
    bias[...] = jnp.where(jnp.transpose(column)[0:1, :] <= column[:, 0:1], 0.0, -1e30)

    @pl.when(jnp.logical_not(lead))
    def _():
        for batch in (0, 1):
            for block in range(n):
                token_arrived(batch, block)

    def turn(block, sign):
        return block * cos[...] + sign * (pltpu.roll(block, HEAD_DIM // 2, 1) * sin[...])

    def dot(a, b, dims):
        return lax.dot_general(a, b, (dims, ((), ())), preferred_element_type=WIDE)

    def projected(batch, at):
        result = None
        for j in range(n):
            term = dot(
                nx[batch, :, :, pl.ds(j * depth, depth)].reshape(total_rows, depth), wh[j, :, at], ((1,), (0,))
            )
            result = term if result is None else result + term
        return result

    weight_arrived(group)
    for batch in (0, 1):
        both = projected(batch, pl.ds(gq, 2 * HEAD_DIM))
        keys[batch] = turn(both[:, :HEAD_DIM], 1.0).astype(SLIM)
        values[batch] = both[:, HEAD_DIM:].astype(SLIM)

    def weigh(queries, key_block):
        masked = dot(queries, key_block, ((1,), (1,))) * scale + bias[...]
        numerators = jnp.exp(masked - jnp.max(masked, axis=-1, keepdims=True))
        return numerators, jnp.sum(numerators, axis=-1, keepdims=True)

    last = group - 1
    spans = ((0, last * HEAD_DIM), (last * HEAD_DIM, HEAD_DIM))

    def mixed_copy(block, i):
        at = pl.ds(*spans[i])
        return remote(
            mixed.at[block, :, at], mixed_in.at[group_at, :, at],
            asend.at[i], arecv.at[i], (served, block),
        )

    def elsewhere(block):
        return jnp.logical_not(jnp.logical_and(lead, me == block))

    def send_mixed(i, *blocks):
        for block in blocks:
            pl.when(elsewhere(block))(lambda: mixed_copy(block, i).start())

    def keep_mixed(i):
        @pl.when(lead)
        def _():
            at = pl.ds(*spans[i])
            mixed_in[group_at, :, at] = mixed[me, :, at]

    def forward_head(h):
        at = pl.ds(h * HEAD_DIM, HEAD_DIM)
        queries = turn(projected(0, at), 1.0).astype(SLIM)
        numerators, totals = weigh(queries, keys[0])
        result = dot(numerators.astype(SLIM), values[0], ((1,), (0,))) / totals
        mixed[:, :, at] = result.astype(SLIM).reshape(n, rows, HEAD_DIM)

    def backward_head(h):
        at = pl.ds(h * HEAD_DIM, HEAD_DIM)
        queries = turn(projected(1, at), 1.0).astype(SLIM)
        numerators, totals = weigh(queries, keys[1])
        rounded = numerators.astype(SLIM)
        summed = dot(rounded, values[1], ((1,), (0,)))
        summed_grad = mg[:, :, at].reshape(total_rows, HEAD_DIM).astype(WIDE) / totals
        totals_grad = -jnp.sum(summed_grad * (summed / totals), axis=-1, keepdims=True)
        narrow_grad = summed_grad.astype(SLIM)
        numer_grad = dot(narrow_grad, values[1], ((1,), (1,))) + totals_grad
        score_grad = (numerators * numer_grad * scale).astype(SLIM)
        query_grad = dot(score_grad, keys[1], ((1,), (0,))).astype(SLIM)
        dqkv[:, at] = turn(query_grad.astype(WIDE), -1.0).astype(SLIM)
        dkey[...] += dot(score_grad, queries, ((0,), (0,)))
        dval[...] += dot(rounded, narrow_grad, ((0,), (0,)))

    dkey[...] = jnp.zeros_like(dkey)
    dval[...] = jnp.zeros_like(dval)

    for h in range(group):
        weight_arrived(h)
        if h == 0:
            pl.when(lead)(lambda: taken(mg.at[pl.ds(0, n - 1)], mrecv.at[0]))
            pl.when(jnp.logical_not(lead))(lambda: taken(mg, mrecv.at[0]))
        backward_head(h)
        if h < last:
            forward_head(h)
        if h == last - 1:
            send_mixed(0, partner, me)
            keep_mixed(0)

    dqkv[:, pl.ds(gq, HEAD_DIM)] = turn(dkey[...].astype(SLIM).astype(WIDE), -1.0).astype(SLIM)
    dqkv[:, pl.ds(gq + HEAD_DIM, HEAD_DIM)] = dval[...].astype(SLIM)
    send_mixed(0, far, near)

    def partial_grads(first):
        block_rows = dqkv[pl.ds(pl.multiple_of(first * rows, 16), half * rows), :]
        for j in range(n):
            part[pl.ds(first, half), :, pl.ds(j * depth, depth)] = (
                dot(block_rows, wh[j], ((1,), (1,))).astype(SLIM).reshape(half, rows, depth)
            )

    chunks = row_chunks(rows)

    def mate_sum(slot, block):
        return remote(part.at[block], from_mate.at[block], bsend.at[0], brecv.at[slot], (mate, me))

    def mate_sum_taken(slot, block):
        taken(from_mate.at[block], brecv.at[slot])

    def partner_sum(slot, block, c):
        at = pl.ds(*chunks[c])
        return remote(
            part.at[block, at], from_z.at[block, at], zsend.at[0], zrecv.at[slot, c], (section, partner)
        )

    def owner_sum(block, c):
        at = pl.ds(*chunks[c])
        return remote(part.at[block, at], dn.at[at], osend.at[0], orecv.at[c], (section, block))

    def summed_part(block, c, *others):
        at = pl.ds(*chunks[c])
        value = part[block, at].astype(WIDE)
        for other in others:
            value += other[block, at].astype(WIDE)
        return value.astype(SLIM)

    trailing = jnp.logical_not(lead)
    at_lead_edge = jnp.logical_and(lead, at_edge)
    at_lead_inner = jnp.logical_and(lead, jnp.logical_not(at_edge))

    partial_grads((1 - side) * half)

    @pl.when(trailing)
    def _():
        mate_sum(0, near).start()
        mate_sum(1, far).start()

    partial_grads(side * half)

    @pl.when(trailing)
    def _():
        mate_sum(2, partner).start()
        mate_sum(3, me).start()

    def pass_on(slot, block):
        mate_sum_taken(slot, block)
        for c in range(len(chunks)):
            part[block, pl.ds(*chunks[c])] = summed_part(block, c, from_mate)
            partner_sum(slot, block, c).start()

    @pl.when(at_lead_inner)
    def _():
        pass_on(0, near)

    forward_head(last)
    send_mixed(1, far, near, partner, me)
    keep_mixed(1)

    @pl.when(at_lead_inner)
    def _():
        pass_on(1, far)
        pass_on(2, partner)

    @pl.when(at_lead_edge)
    def _():
        pass_on(2, partner)


    def finish_block(slot, block):
        mate_sum_taken(slot, block)
        for c in range(len(chunks)):
            partner_sum(slot, block, c).wait_recv()
            part[block, pl.ds(*chunks[c])] = summed_part(block, c, from_mate, from_z)
            owner_sum(block, c).start()

    pl.when(at_lead_edge)(lambda: finish_block(0, near))

    def back_copy(c):
        at = pl.ds(*chunks[c])
        return remote(grads.at[at], back.at[at], csend.at[1], crecv.at[1], (preceding, me))

    def give_back():
        pl.when(lead)(lambda: mate_sum_taken(3, me))
        for c, chunk in enumerate(chunks):
            at = pl.ds(*chunk)

            @pl.when(lead)
            def _():
                partner_sum(2, me, c).wait_recv()
                dn[at] = summed_part(me, c, from_mate, from_z)

            pl.when(trailing)(lambda: owner_sum(me, c).wait_recv())
            widened = saved[at].astype(WIDE)
            inverse = lax.rsqrt(jnp.mean(widened * widened, axis=-1, keepdims=True) + norm_eps)
            scaled = dn[at].astype(WIDE) * gain[...]
            inner_mean = jnp.mean(scaled * widened, axis=-1, keepdims=True)
            project_grad = inverse * scaled - widened * (inverse * inverse * inverse * inner_mean)
            grads[at] = up[at] + project_grad.astype(SLIM)
            back_copy(c).start()

    early = jnp.logical_and(at_lead_inner, core == 0)
    pl.when(early)(give_back)

    total = tokens[...].astype(WIDE)
    for i, span in enumerate(spans):
        at = pl.ds(*span)
        pl.when(lead)(lambda: taken(mixed_in.at[pl.ds(0, n - 1), :, at], arecv.at[i]))
        pl.when(trailing)(lambda: taken(mixed_in.at[:, :, at], arecv.at[i]))
    for j in range(n):
        total += jnp.dot(mixed_in[j], wo[pl.ds(j * gq, gq), :], preferred_element_type=WIDE)
    produced[...] = total.astype(SLIM)
    ahead_copy = remote(produced, ahead, csend.at[0], crecv.at[0], (following, me))
    ahead_copy.start()
    pl.when(at_lead_edge)(lambda: finish_block(1, far))

    pl.when(jnp.logical_not(early))(give_back)

    @pl.when(lead)
    def _():
        for batch in (0, 1):
            given(nx.at[batch], nsend.at[batch, 0])
        given(mgl.at[pl.ds(0, n - 1)], msend.at[0])
        for i, span in enumerate(spans):
            given(mixed.at[pl.ds(0, n - 1), :, pl.ds(*span)], asend.at[i])

    @pl.when(at_lead_edge)
    def _():
        for batch in (0, 1):
            given(nx.at[batch, pl.ds(0, half + 1)], nsend.at[batch, 1])
        given(part.at[0], zsend.at[0])
        given(part.at[pl.ds(0, half)], osend.at[0])

    @pl.when(at_lead_inner)
    def _():
        for batch in (0, 1):
            given(nx.at[batch, 0], nsend.at[batch, 1])
        given(part.at[pl.ds(0, half + 1)], zsend.at[0])

    @pl.when(trailing)
    def _():
        for batch in (0, 1):
            given(mine.at[batch], nsend.at[batch, 0])
        given(mgl, msend.at[0])
        for i, span in enumerate(spans):
            given(mixed.at[:, :, pl.ds(*span)], asend.at[i])
        given(part, bsend.at[0])

    given(posg.at[pl.ds(0, n - 1)], psend.at[0])
    for j in range(n):
        pl.when(jnp.logical_not(here(j)))(lambda: given(wh.at[0], wsend.at[j]))

    ahead_copy.wait_send()
    given(grads, csend.at[1])
    ahead_copy.wait_recv()
    taken(back, crecv.at[1])


def by_pairs(n, sections):
    def step(
        section_inputs, saved_inputs, output_grads, token_positions, norm_gain,
        query_weight, keyval_weight, output_weight,
    ):
        _, rows, width = section_inputs.shape
        _, depth, query_width = query_weight.shape
        gq = query_width // n
        group = gq // HEAD_DIM
        wide = gq + keyval_weight.shape[2] // n

        chunks = len(row_chunks(rows))

        half_dim = HEAD_DIM // 2
        frequency = rope_base ** (-2.0 * np.arange(half_dim) / HEAD_DIM)
        signs = np.ones(half_dim)
        waves = jnp.asarray(
            np.stack([np.concatenate([frequency, frequency]), np.concatenate([-signs, signs])]), WIDE
        )

        def shaped(shape, kind=SLIM):
            return jax.ShapeDtypeStruct(shape, kind)

        def held(*shape, kind=SLIM):
            return pltpu.VMEM(shape, kind)

        pair = (shaped((rows, width)), shaped((rows, width)))
        dma = pltpu.SemaphoreType.DMA
        ahead, back = pl.pallas_call(
            functools.partial(layer_kernel, n, sections),
            out_shape=(pltpu.VMEM((rows, width), SLIM),) * 2,
            in_specs=[HBM] * 9,
            out_specs=(VMEM,) * 2,
            scratch_shapes=[
                *[held(rows, width)] * 3, held(1, width, kind=WIDE), held(1, rows, kind=jnp.int32),
                held(2, HEAD_DIM, kind=WIDE), held(2, n, rows, width), held(2, rows, width),
                held(n, rows, gq), held(n, rows, gq), held(query_width, width), held(n, depth, wide),
                held(n, 1, rows, kind=jnp.int32), held(n * rows, n * rows, kind=WIDE),
                held(n * rows, HEAD_DIM, kind=WIDE), held(n * rows, HEAD_DIM, kind=WIDE),
                held(2, n * rows, HEAD_DIM), held(2, n * rows, HEAD_DIM),
                held(n * rows, HEAD_DIM, kind=WIDE), held(n * rows, HEAD_DIM, kind=WIDE),
                held(n, rows, gq), held(n, rows, gq), held(n * rows, wide),
                held(n, rows, width), held(n, rows, width), held(n, rows, width), held(rows, width),
                held(rows, width), held(rows, width),
                dma((2, 2)), dma((2, n)), dma((n,)), dma((group + 1,)), *[dma((1,))] * 4, *[dma((2,))] * 2,
                dma((1,)), dma((n,)), dma((1,)), dma((3, chunks)), dma((1,)), dma((chunks,)),
                *[dma((2,))] * 2, dma((7,)),
            ],
            compiler_params=pltpu.CompilerParams(
                collective_id=0, has_side_effects=True, vmem_limit_bytes=67043328 - 4 * rows * width - 2**16
            ),
            name="layer",
        )(
            section_inputs[0], saved_inputs[0], output_grads[0], norm_gain, output_weight[0],
            query_weight[0], keyval_weight[0], token_positions[None], waves,
        )
        return (ahead[None], back[None])

    return step


def solution(mesh):
    placed = (
        P("section", "ctx", None),
        P("section", "ctx", None),
        P("section", "ctx", None),
        P("ctx"),
        P("section", None),
        P("section", "ctx", None),
        P("section", "ctx", None),
        P("section", None, None),
    )
    n, sections = mesh.shape["ctx"], mesh.shape["section"]

    def chosen(*blocks):
        kv_heads = blocks[6].shape[2] // (2 * HEAD_DIM)
        rows, query_heads = blocks[0].shape[1], blocks[5].shape[2] // HEAD_DIM
        paired = n == 4 and sections > 2 and sections % 2 == 0
        if paired and kv_heads == n and query_heads > n and rows % 16 == 0:
            return by_pairs(n, sections)(*blocks)
        return shards(*blocks)

    return jax.shard_map(
        chosen,
        mesh=mesh,
        in_specs=placed,
        out_specs=(P("section", "ctx", None), P("section", "ctx", None)),
        check_vma=False,
    )
```

```python
import functools

import jax
import jax.numpy as jnp
import numpy as np
from jax import lax
from jax.experimental import pallas as pl
from jax.experimental.pallas import tpu as pltpu
from jax.sharding import PartitionSpec as P

HEAD_DIM = 128


norm_eps = 1e-05
rope_base = 500000.0


def from_behind(block, axis, distance):
    devices = range(lax.axis_size(axis))
    route = [((i - distance) % len(devices), i) for i in devices]
    return lax.ppermute(block, axis, route)


def rotate(matrix, positions):
    half_dim = matrix.shape[-1] // 2
    frequency = rope_base ** (-2.0 * jnp.arange(half_dim, dtype=jnp.float32) / matrix.shape[-1])
    angles = positions.astype(jnp.float32)[:, None] * frequency[None, :]
    cos_table = jnp.cos(angles)[:, None, :]
    sin_table = jnp.sin(angles)[:, None, :]
    leading = matrix[..., :half_dim]
    trailing = matrix[..., half_dim:]
    return jnp.concatenate(
        [leading * cos_table - trailing * sin_table, trailing * cos_table + leading * sin_table],
        axis=-1,
    )


def project(tokens, gain, query_matrix, keyval_matrix, positions):
    widened = tokens.astype(jnp.float32)
    inverse = lax.rsqrt(jnp.mean(widened * widened, axis=-1, keepdims=True) + norm_eps)
    normed = (widened * inverse * gain[None, :]).astype(jnp.bfloat16)
    row_count = tokens.shape[0]
    query_full = jnp.dot(normed, query_matrix, preferred_element_type=jnp.float32)
    keyval_full = jnp.dot(normed, keyval_matrix, preferred_element_type=jnp.float32)
    queries = rotate(query_full.reshape(row_count, -1, HEAD_DIM), positions).astype(jnp.bfloat16)
    paired = keyval_full.reshape(row_count, 2, -1, HEAD_DIM)
    key_rows = rotate(paired[:, 0], positions).astype(jnp.bfloat16)
    value_rows = paired[:, 1].astype(jnp.bfloat16)
    return (queries, key_rows, value_rows)


def attend(queries, key_wide, value_wide, query_pos, key_pos, narrow):
    row_count = queries.shape[0]
    kv_count = key_wide.shape[1]
    head_size = queries.shape[2]
    group_size = queries.shape[1] // kv_count
    grouped = jnp.moveaxis(queries.reshape(row_count, kv_count, group_size, head_size), 1, 0)
    key_heads = jnp.moveaxis(key_wide, 1, 0)
    value_heads = jnp.moveaxis(value_wide, 1, 0)
    visible = (key_pos[None, :] <= query_pos[:, None])[None]

    def one_head(block):
        query_block, key_block, value_block = block
        scores = jnp.einsum(
            "rgd,sd->grs", query_block, key_block, preferred_element_type=jnp.float32
        ) * head_size ** (-0.5)
        masked = jnp.where(visible, scores, -1e30)
        row_max = lax.stop_gradient(jnp.max(masked, axis=-1, keepdims=True))
        numerators = jnp.where(visible, jnp.exp(masked - row_max), 0.0)
        totals = jnp.sum(numerators, axis=-1)
        if narrow:
            rounded = numerators.astype(jnp.bfloat16)
        else:
            rounded = lax.optimization_barrier(numerators.astype(jnp.bfloat16)).astype(jnp.float32)
        summed = jnp.einsum("grs,sd->rgd", rounded, value_block, preferred_element_type=jnp.float32)
        return summed / jnp.transpose(totals, (1, 0))[..., None]

    averaged = lax.map(one_head, (grouped, key_heads, value_heads))
    return jnp.moveaxis(averaged, 0, 1).reshape(row_count, -1).astype(jnp.bfloat16)


def finish(tokens, mixed, output_matrix):
    return (
        tokens.astype(jnp.float32)
        + jnp.dot(mixed, output_matrix, preferred_element_type=jnp.float32)
    ).astype(jnp.bfloat16)


def shards(
    section_inputs,
    saved_inputs,
    output_grads,
    token_positions,
    norm_gain,
    query_weight,
    keyval_weight,
    output_weight,
):
    key_positions = lax.all_gather(token_positions, "ctx", axis=0, tiled=True)
    full_query, full_keyval = (
        lax.all_gather(query_weight[0], "ctx", axis=0, tiled=True),
        lax.all_gather(keyval_weight[0], "ctx", axis=0, tiled=True),
    )
    full_output = output_weight[0]
    gain = norm_gain[0]
    forward_tokens = section_inputs[0]
    saved_tokens = saved_inputs[0]
    upstream = output_grads[0]

    def projector(tokens):
        return project(tokens, gain, full_query, full_keyval, token_positions)

    def attention_wide(queries, key_wide, value_wide):
        return attend(queries, key_wide, value_wide, token_positions, key_positions, False)

    def finishing(tokens, mixed):
        return finish(tokens, mixed, full_output)

    forward_queries, forward_keys, forward_values = projector(forward_tokens)
    (backward_queries, backward_keys, backward_values), back_project = jax.vjp(
        projector, saved_tokens
    )
    forward_keyset, forward_valueset = (
        lax.all_gather(forward_keys, "ctx", axis=0, tiled=True),
        lax.all_gather(forward_values, "ctx", axis=0, tiled=True),
    )
    mixed = attend(
        forward_queries, forward_keyset, forward_valueset, token_positions, key_positions, True
    )
    produced = finishing(forward_tokens, mixed)
    sent_on = from_behind(produced[None], "section", 1)
    backward_keyset, backward_valueset = (
        lax.all_gather(backward_keys, "ctx", axis=0, tiled=True),
        lax.all_gather(backward_values, "ctx", axis=0, tiled=True),
    )
    mixed, back_attend = jax.vjp(
        attention_wide,
        backward_queries.astype(jnp.float32),
        backward_keyset.astype(jnp.float32),
        backward_valueset.astype(jnp.float32),
    )
    produced, back_finish = jax.vjp(finishing, saved_tokens, mixed)
    residual_grad, mixed_grad = back_finish(upstream)
    query_grad, key_partial, value_partial = back_attend(mixed_grad)
    key_grads = lax.psum_scatter(
        key_partial.astype(jnp.bfloat16), "ctx", scatter_dimension=0, tiled=True
    )
    value_grads = lax.psum_scatter(
        value_partial.astype(jnp.bfloat16), "ctx", scatter_dimension=0, tiled=True
    )
    (project_grad,) = back_project((query_grad.astype(jnp.bfloat16), key_grads, value_grads))
    sent_back = from_behind((residual_grad + project_grad)[None], "section", -1)
    return (sent_on, sent_back)


MESH = pl.DeviceIdType.MESH
VMEM = pl.BlockSpec(memory_space=pltpu.VMEM)
ANY = pl.BlockSpec(memory_space=pl.ANY)
WIDE = jnp.float32
SLIM = jnp.bfloat16


def remote(src, dst, send, recv, device):
    return pltpu.make_async_remote_copy(
        src_ref=src, dst_ref=dst, send_sem=send, recv_sem=recv, device_id=device, device_id_type=MESH
    )


HBM = pl.BlockSpec(memory_space=pltpu.HBM)


def row_chunks(rows):
    tiles = rows // 16
    singles = min(tiles, 3)
    rest = tiles - singles
    sizes = [size * 16 for size in (rest - rest // 2, rest // 2, *[1] * singles) if size]
    return [(sum(sizes[:i]), size) for i, size in enumerate(sizes)]


def layer_kernel(
    n, sections, tokens_hbm, saved_hbm, up_hbm, gain_hbm, wo_hbm, wq, wkv, pos_hbm, waves_hbm, ahead, back,
    tokens, saved, up, gain, pos, waves, nx, mine, mgl, mg, wo, wh, posg, bias, cos, sin, keys, values, dkey, dval, mixed, mixed_in, dqkv,
    part, from_mate, from_z, dn, produced, grads,
    nsend, nrecv, wsend, wrecv, msend, mrecv, psend, precv, asend, arecv, bsend, brecv, zsend, zrecv,
    osend, orecv, csend, crecv, own,
):
    section = lax.axis_index("section")
    me = lax.axis_index("ctx")
    half = n // 2
    core = lax.rem(section, 2)
    base = section - core
    mate = base + 1 - core
    side = me // half
    served = base + side
    lead = core == side
    partner = 2 * side * half + half - 1 - me
    edge = half - 1 + side
    at_edge = me == edge
    group_at = lax.rem(me, half) * 2 + core
    near, far = half - side, (n - 1) * (1 - side)
    depth, _ = wq.shape
    rows, width = tokens.shape
    gq = mg.shape[2]
    group = gq // HEAD_DIM
    kv_half = wkv.shape[1] // 2
    total_rows = n * rows
    scale = HEAD_DIM ** (-0.5)
    following, preceding = lax.rem(section + 1, sections), lax.rem(section + sections - 1, sections)

    barrier = pltpu.get_barrier_semaphore()
    for k in range(1, n):
        for other in (section, mate):
            pl.semaphore_signal(barrier, inc=1, device_id=(other, lax.rem(me + k, n)), device_id_type=MESH)
    for other in (mate, following, preceding):
        pl.semaphore_signal(barrier, inc=1, device_id=(other, me), device_id_type=MESH)

    loads = [
        pltpu.make_async_copy(src, dst, own.at[i])
        for i, (src, dst) in enumerate(
            (
                (gain_hbm, gain), (tokens_hbm, tokens), (saved_hbm, saved), (pos_hbm, pos), (up_hbm, up),
                (waves_hbm, waves), (wo_hbm, wo),
            )
        )
    ]
    for load in loads:
        load.start()

    def normed(block):
        widened = block[...].astype(WIDE)
        inverse = lax.rsqrt(jnp.mean(widened * widened, axis=-1, keepdims=True) + norm_eps)
        return (widened * inverse * gain[...]).astype(SLIM)

    for load in loads[:4]:
        load.wait()
    for batch, block in enumerate((tokens, saved)):
        mine[batch] = normed(block)

    @pl.when(lead)
    def _():
        for batch in (0, 1):
            nx[batch, me] = mine[batch]

    posg[me] = pos[...]
    pl.semaphore_wait(barrier, 2 * n + 1)

    def seat(owner_core, j):
        return (base + lax.rem(j, 2), owner_core * half + j // 2)

    def token_copy(batch, lane, src, block, device):
        return remote(src, nx.at[batch, block], nsend.at[batch, lane], nrecv.at[batch, block], device)

    def to_mate(batch, block):
        return token_copy(batch, 0, nx.at[batch, block], block, (mate, me))

    def to_partner(batch, block):
        return token_copy(batch, 1, nx.at[batch, block], block, (section, partner))

    def to_edge(batch):
        return token_copy(batch, 0, mine.at[batch], me, (section, half - 1 + core))

    def piece_source(j, piece):
        if piece < group:
            start = j * gq + piece * HEAD_DIM
            return wq.at[:, pl.ds(pl.multiple_of(start, HEAD_DIM), HEAD_DIM)], piece * HEAD_DIM
        start = (piece - group) * kv_half + j * HEAD_DIM
        return wkv.at[:, pl.ds(pl.multiple_of(start, HEAD_DIM), HEAD_DIM)], piece * HEAD_DIM

    def piece_slot(piece):
        if piece != group - 1:
            return min(piece, group)
        return jnp.where(me == half - core, group + 1, piece)

    def weight_copy(j, piece):
        src, to = piece_source(j, piece)
        return remote(
            src, wh.at[me, :, pl.ds(to, HEAD_DIM)], wsend.at[j], wrecv.at[piece_slot(piece)], seat(core, j)
        )

    def weight_here(j, piece):
        src, to = piece_source(j, piece)
        return pltpu.make_async_copy(src, wh.at[me, :, pl.ds(to, HEAD_DIM)], wrecv.at[piece_slot(piece)])

    def taken(dst, recv):
        remote(dst, dst, osend.at[0], recv, (section, me)).wait_recv()

    def given(src, send):
        remote(src, src, send, orecv.at[0], (section, me)).wait_send()

    def weight_arrived(piece):
        size = HEAD_DIM if piece < group else 2 * HEAD_DIM
        taken(wh.at[:, :, pl.ds(piece * HEAD_DIM, size)], wrecv.at[piece])

    def here(j):
        return jnp.logical_and(lead, group_at == j)

    def send_weights(piece):
        for i in range(n):
            j = lax.rem(i + core * half, n)
            pl.when(here(j))(lambda: weight_here(j, piece).start())
            pl.when(jnp.logical_not(here(j)))(lambda: weight_copy(j, piece).start())

    def grad_copy(j):
        return remote(mgl.at[j], mg.at[me], msend.at[0], mrecv.at[0], seat(core, j))

    def place_copy(k):
        return remote(pos, posg.at[me], psend.at[0], precv.at[0], (section, lax.rem(me + k, n)))

    @pl.when(lead)
    def _():
        for batch in (0, 1):
            to_partner(batch, me).start()
        for batch in (0, 1):
            to_mate(batch, me).start()

    @pl.when(jnp.logical_not(lead))
    def _():
        for batch in (0, 1):
            to_edge(batch).start()

    for k in range(1, n):
        place_copy(k).start()
    send_weights(group)
    send_weights(group + 1)

    for load in loads[4:]:
        load.wait()
    for j in range(n):
        mgl[j] = lax.dot_general(
            up[...], wo[pl.ds(j * gq, gq), :], (((1,), (1,)), ((), ())), preferred_element_type=WIDE
        ).astype(SLIM)
    for j in range(n):
        @pl.when(here(j))
        def _():
            mg[me] = mgl[j]

        pl.when(jnp.logical_not(here(j)))(lambda: grad_copy(j).start())

    @pl.when(jnp.logical_not(lead))
    def _():
        for piece in range(group):
            send_weights(piece)

    def token_arrived(batch, block):
        dst = nx.at[batch, block]
        remote(dst, dst, nsend.at[0, 0], nrecv.at[batch, block], (section, me)).wait_recv()

    @pl.when(lead)
    def _():
        for batch in (0, 1):
            for block, outer in ((partner, False), (near, True), (far, True)):
                token_arrived(batch, block)
                if outer:
                    pl.when(at_edge)(lambda: to_partner(batch, block).start())
                to_mate(batch, block).start()
        for piece in range(group):
            send_weights(piece)

    taken(posg.at[pl.ds(0, n - 1)], precv.at[0])
    columns = []
    for j in range(n):
        column = jnp.transpose(jnp.broadcast_to(posg[j].astype(WIDE), (HEAD_DIM, rows)))
        angles = column * waves[0:1, :]
        at = pl.ds(j * rows, rows)
        cos[at, :] = jnp.cos(angles)
        sin[at, :] = jnp.sin(angles) * waves[1:2, :]
        columns.append(column)
    column = jnp.concatenate(columns, axis=0)
    bias[...] = jnp.where(jnp.transpose(column)[0:1, :] <= column[:, 0:1], 0.0, -1e30)

    @pl.when(jnp.logical_not(lead))
    def _():
        for batch in (0, 1):
            for block in range(n):
                token_arrived(batch, block)

    def turn(block, sign):
        return block * cos[...] + sign * (pltpu.roll(block, HEAD_DIM // 2, 1) * sin[...])

    def dot(a, b, dims):
        return lax.dot_general(a, b, (dims, ((), ())), preferred_element_type=WIDE)

    def projected(batch, at, sources=range(n)):
        result = None
        for j in sources:
            columns = pl.ds(pl.multiple_of(j * depth, HEAD_DIM), depth)
            term = dot(nx[batch, :, :, columns].reshape(total_rows, depth), wh[j, :, at], ((1,), (0,)))
            result = term if result is None else result + term
        return result

    weight_arrived(group)
    for batch in (0, 1):
        both = projected(batch, pl.ds(gq, 2 * HEAD_DIM))
        keys[batch] = turn(both[:, :HEAD_DIM], 1.0).astype(SLIM)
        values[batch] = both[:, HEAD_DIM:].astype(SLIM)

    def weigh(queries, key_block):
        masked = dot(queries, key_block, ((1,), (1,))) * scale + bias[...]
        numerators = jnp.exp(masked - jnp.max(masked, axis=-1, keepdims=True))
        return numerators, jnp.sum(numerators, axis=-1, keepdims=True)

    last = group - 1
    spans = ((0, last * HEAD_DIM), (last * HEAD_DIM, HEAD_DIM))

    def mixed_copy(block, i):
        at = pl.ds(*spans[i])
        return remote(
            mixed.at[block, :, at], mixed_in.at[group_at, :, at],
            asend.at[i], arecv.at[i], (served, block),
        )

    def elsewhere(block):
        return jnp.logical_not(jnp.logical_and(lead, me == block))

    def send_mixed(i, *blocks):
        for block in blocks:
            pl.when(elsewhere(block))(lambda: mixed_copy(block, i).start())

    def keep_mixed(i):
        @pl.when(lead)
        def _():
            at = pl.ds(*spans[i])
            mixed_in[group_at, :, at] = mixed[me, :, at]

    def forward_head(h):
        at = pl.ds(h * HEAD_DIM, HEAD_DIM)
        queries = turn(projected(0, at), 1.0).astype(SLIM)
        numerators, totals = weigh(queries, keys[0])
        result = dot(numerators.astype(SLIM), values[0], ((1,), (0,))) / totals
        mixed[:, :, at] = result.astype(SLIM).reshape(n, rows, HEAD_DIM)

    def backward_head(h):
        at = pl.ds(h * HEAD_DIM, HEAD_DIM)
        if h < last:
            weight_arrived(h)
            result = projected(1, at)
        else:
            taken(wh.at[pl.ds(0, n - 1), :, at], wrecv.at[h])
            result = projected(1, at, [lax.rem(near + i, n) for i in range(1, n)])
            taken(wh.at[0, :, at], wrecv.at[group + 1])
            result += projected(1, at, [near])
        queries = turn(result, 1.0).astype(SLIM)
        numerators, totals = weigh(queries, keys[1])
        rounded = numerators.astype(SLIM)
        summed = dot(rounded, values[1], ((1,), (0,)))
        summed_grad = mg[:, :, at].reshape(total_rows, HEAD_DIM).astype(WIDE) / totals
        totals_grad = -jnp.sum(summed_grad * (summed / totals), axis=-1, keepdims=True)
        narrow_grad = summed_grad.astype(SLIM)
        numer_grad = dot(narrow_grad, values[1], ((1,), (1,))) + totals_grad
        score_grad = (numerators * numer_grad * scale).astype(SLIM)
        query_grad = dot(score_grad, keys[1], ((1,), (0,))).astype(SLIM)
        dqkv[:, at] = turn(query_grad.astype(WIDE), -1.0).astype(SLIM)
        dkey[...] += dot(score_grad, queries, ((0,), (0,)))
        dval[...] += dot(rounded, narrow_grad, ((0,), (0,)))

    dkey[...] = jnp.zeros_like(dkey)
    dval[...] = jnp.zeros_like(dval)

    for h in range(group):
        if h == 0:
            pl.when(lead)(lambda: taken(mg.at[pl.ds(0, n - 1)], mrecv.at[0]))
            pl.when(jnp.logical_not(lead))(lambda: taken(mg, mrecv.at[0]))
        backward_head(h)
        if h < last:
            forward_head(h)
        if h == last - 1:
            send_mixed(0, partner, me)
            keep_mixed(0)

    dqkv[:, pl.ds(gq, HEAD_DIM)] = turn(dkey[...].astype(SLIM).astype(WIDE), -1.0).astype(SLIM)
    dqkv[:, pl.ds(gq + HEAD_DIM, HEAD_DIM)] = dval[...].astype(SLIM)
    send_mixed(0, far, near)

    def partial_grads(first):
        block_rows = dqkv[pl.ds(pl.multiple_of(first * rows, 16), half * rows), :]
        for j in range(n):
            part[pl.ds(first, half), :, pl.ds(j * depth, depth)] = (
                dot(block_rows, wh[j], ((1,), (1,))).astype(SLIM).reshape(half, rows, depth)
            )

    chunks = row_chunks(rows)

    def mate_sum(slot, block):
        return remote(part.at[block], from_mate.at[block], bsend.at[0], brecv.at[slot], (mate, me))

    def mate_sum_taken(slot, block):
        taken(from_mate.at[block], brecv.at[slot])

    def partner_sum(slot, block, c):
        at = pl.ds(*chunks[c])
        return remote(
            part.at[block, at], from_z.at[block, at], zsend.at[0], zrecv.at[slot, c], (section, partner)
        )

    def owner_sum(block, c):
        at = pl.ds(*chunks[c])
        return remote(part.at[block, at], dn.at[at], osend.at[0], orecv.at[c], (section, block))

    def summed_part(block, c, *others):
        at = pl.ds(*chunks[c])
        value = part[block, at].astype(WIDE)
        for other in others:
            value += other[block, at].astype(WIDE)
        return value.astype(SLIM)

    trailing = jnp.logical_not(lead)
    at_lead_edge = jnp.logical_and(lead, at_edge)
    at_lead_inner = jnp.logical_and(lead, jnp.logical_not(at_edge))

    def send_outer():
        mate_sum(0, near).start()
        mate_sum(1, far).start()

    def send_inner():
        mate_sum(2, partner).start()
        mate_sum(3, me).start()

    own_first = jnp.where(at_edge, side, 1 - side)
    trail_edge = jnp.logical_and(trailing, at_edge)
    trail_inner = jnp.logical_and(trailing, jnp.logical_not(at_edge))
    partial_grads(own_first * half)
    pl.when(trail_edge)(send_inner)
    pl.when(trail_inner)(send_outer)
    partial_grads((1 - own_first) * half)
    pl.when(trail_edge)(send_outer)
    pl.when(trail_inner)(send_inner)

    def pass_on(slot, block):
        mate_sum_taken(slot, block)
        for c in range(len(chunks)):
            part[block, pl.ds(*chunks[c])] = summed_part(block, c, from_mate)
            partner_sum(slot, block, c).start()

    @pl.when(at_lead_inner)
    def _():
        pass_on(0, near)

    forward_head(last)
    send_mixed(1, far, near, partner, me)
    keep_mixed(1)

    @pl.when(at_lead_inner)
    def _():
        pass_on(1, far)
        pass_on(2, partner)

    @pl.when(at_lead_edge)
    def _():
        pass_on(2, partner)


    def finish_block(slot, block):
        mate_sum_taken(slot, block)
        for c in range(len(chunks)):
            partner_sum(slot, block, c).wait_recv()
            part[block, pl.ds(*chunks[c])] = summed_part(block, c, from_mate, from_z)
            owner_sum(block, c).start()

    pl.when(at_lead_edge)(lambda: finish_block(0, near))

    def back_copy(c):
        at = pl.ds(*chunks[c])
        return remote(grads.at[at], back.at[at], csend.at[1], crecv.at[1], (preceding, me))

    def give_back():
        pl.when(lead)(lambda: mate_sum_taken(3, me))
        for c, chunk in enumerate(chunks):
            at = pl.ds(*chunk)

            @pl.when(lead)
            def _():
                partner_sum(2, me, c).wait_recv()
                dn[at] = summed_part(me, c, from_mate, from_z)

            pl.when(trailing)(lambda: owner_sum(me, c).wait_recv())
            widened = saved[at].astype(WIDE)
            inverse = lax.rsqrt(jnp.mean(widened * widened, axis=-1, keepdims=True) + norm_eps)
            scaled = dn[at].astype(WIDE) * gain[...]
            inner_mean = jnp.mean(scaled * widened, axis=-1, keepdims=True)
            project_grad = inverse * scaled - widened * (inverse * inverse * inverse * inner_mean)
            grads[at] = up[at] + project_grad.astype(SLIM)
            back_copy(c).start()

    early = jnp.logical_and(at_lead_inner, core == 0)
    pl.when(early)(give_back)

    total = tokens[...].astype(WIDE)
    for i, (start, size) in enumerate(spans):
        at = pl.ds(start, size)
        pl.when(lead)(lambda: taken(mixed_in.at[pl.ds(0, n - 1), :, at], arecv.at[i]))
        pl.when(trailing)(lambda: taken(mixed_in.at[:, :, at], arecv.at[i]))
        for j in range(n):
            total += jnp.dot(
                mixed_in[j, :, at], wo[pl.ds(j * gq + start, size), :], preferred_element_type=WIDE
            )
    produced[...] = total.astype(SLIM)
    ahead_copy = remote(produced, ahead, csend.at[0], crecv.at[0], (following, me))
    ahead_copy.start()
    pl.when(at_lead_edge)(lambda: finish_block(1, far))

    pl.when(jnp.logical_not(early))(give_back)

    @pl.when(lead)
    def _():
        for batch in (0, 1):
            given(nx.at[batch], nsend.at[batch, 0])
        given(mgl.at[pl.ds(0, n - 1)], msend.at[0])
        for i, span in enumerate(spans):
            given(mixed.at[pl.ds(0, n - 1), :, pl.ds(*span)], asend.at[i])

    @pl.when(at_lead_edge)
    def _():
        for batch in (0, 1):
            given(nx.at[batch, pl.ds(0, half + 1)], nsend.at[batch, 1])
        given(part.at[0], zsend.at[0])
        given(part.at[pl.ds(0, half)], osend.at[0])

    @pl.when(at_lead_inner)
    def _():
        for batch in (0, 1):
            given(nx.at[batch, 0], nsend.at[batch, 1])
        given(part.at[pl.ds(0, half + 1)], zsend.at[0])

    @pl.when(trailing)
    def _():
        for batch in (0, 1):
            given(mine.at[batch], nsend.at[batch, 0])
        given(mgl, msend.at[0])
        for i, span in enumerate(spans):
            given(mixed.at[:, :, pl.ds(*span)], asend.at[i])
        given(part, bsend.at[0])

    given(posg.at[pl.ds(0, n - 1)], psend.at[0])
    for j in range(n):
        pl.when(jnp.logical_not(here(j)))(lambda: given(wh.at[0], wsend.at[j]))

    ahead_copy.wait_send()
    given(grads, csend.at[1])
    ahead_copy.wait_recv()
    taken(back, crecv.at[1])


def hand_kernel(first, second, first_out, second_out, sems):
    gives = [
        pltpu.make_async_copy(src, dst, sems.at[i])
        for i, (src, dst) in enumerate(((first, first_out), (second, second_out)))
    ]
    for give in gives:
        give.start()
    for give in gives:
        give.wait()


def by_pairs(n, sections):
    def step(
        section_inputs, saved_inputs, output_grads, token_positions, norm_gain,
        query_weight, keyval_weight, output_weight,
    ):
        _, rows, width = section_inputs.shape
        _, depth, query_width = query_weight.shape
        gq = query_width // n
        group = gq // HEAD_DIM
        wide = gq + keyval_weight.shape[2] // n

        chunks = len(row_chunks(rows))

        half_dim = HEAD_DIM // 2
        frequency = rope_base ** (-2.0 * np.arange(half_dim) / HEAD_DIM)
        signs = np.ones(half_dim)
        waves = jnp.asarray(
            np.stack([np.concatenate([frequency, frequency]), np.concatenate([-signs, signs])]), WIDE
        )

        def shaped(shape, kind=SLIM):
            return jax.ShapeDtypeStruct(shape, kind)

        def held(*shape, kind=SLIM):
            return pltpu.VMEM(shape, kind)

        pair = (shaped((rows, width)), shaped((rows, width)))
        dma = pltpu.SemaphoreType.DMA
        ahead, back = pl.pallas_call(
            functools.partial(layer_kernel, n, sections),
            out_shape=(pltpu.VMEM((rows, width), SLIM),) * 2,
            in_specs=[HBM] * 9,
            out_specs=(VMEM,) * 2,
            scratch_shapes=[
                *[held(rows, width)] * 3, held(1, width, kind=WIDE), held(1, rows, kind=jnp.int32),
                held(2, HEAD_DIM, kind=WIDE), held(2, n, rows, width), held(2, rows, width),
                held(n, rows, gq), held(n, rows, gq), held(query_width, width), held(n, depth, wide),
                held(n, 1, rows, kind=jnp.int32), held(n * rows, n * rows, kind=WIDE),
                held(n * rows, HEAD_DIM, kind=WIDE), held(n * rows, HEAD_DIM, kind=WIDE),
                held(2, n * rows, HEAD_DIM), held(2, n * rows, HEAD_DIM),
                held(n * rows, HEAD_DIM, kind=WIDE), held(n * rows, HEAD_DIM, kind=WIDE),
                held(n, rows, gq), held(n, rows, gq), held(n * rows, wide),
                held(n, rows, width), held(n, rows, width), held(n, rows, width), held(rows, width),
                held(rows, width), held(rows, width),
                dma((2, 2)), dma((2, n)), dma((n,)), dma((group + 2,)), *[dma((1,))] * 4, *[dma((2,))] * 2,
                dma((1,)), dma((n,)), dma((1,)), dma((3, chunks)), dma((1,)), dma((chunks,)),
                *[dma((2,))] * 2, dma((7,)),
            ],
            compiler_params=pltpu.CompilerParams(
                collective_id=0, has_side_effects=True, vmem_limit_bytes=67043328 - 4 * rows * width - 2**16
            ),
            name="layer",
        )(
            section_inputs[0], saved_inputs[0], output_grads[0], norm_gain, output_weight[0],
            query_weight[0], keyval_weight[0], token_positions[None], waves,
        )
        ahead, back = (pltpu.with_memory_space_constraint(block, pltpu.VMEM) for block in (ahead, back))
        ahead, back = pl.pallas_call(
            hand_kernel, out_shape=pair, in_specs=[VMEM] * 2, out_specs=(HBM,) * 2,
            scratch_shapes=[dma((2,))], name="hand",
        )(ahead, back)
        return (ahead[None], back[None])

    return step


def solution(mesh):
    placed = (
        P("section", "ctx", None),
        P("section", "ctx", None),
        P("section", "ctx", None),
        P("ctx"),
        P("section", None),
        P("section", "ctx", None),
        P("section", "ctx", None),
        P("section", None, None),
    )
    n, sections = mesh.shape["ctx"], mesh.shape["section"]

    def chosen(*blocks):
        kv_heads = blocks[6].shape[2] // (2 * HEAD_DIM)
        rows, query_heads = blocks[0].shape[1], blocks[5].shape[2] // HEAD_DIM
        paired = n == 4 and sections > 2 and sections % 2 == 0
        if paired and kv_heads == n and query_heads > n and rows % 16 == 0:
            return by_pairs(n, sections)(*blocks)
        return shards(*blocks)

    return jax.shard_map(
        chosen,
        mesh=mesh,
        in_specs=placed,
        out_specs=(P("section", "ctx", None), P("section", "ctx", None)),
        check_vma=False,
    )
```

```python
import functools

import jax
import jax.numpy as jnp
import numpy as np
from jax import lax
from jax.experimental import pallas as pl
from jax.experimental.pallas import tpu as pltpu
from jax.sharding import PartitionSpec as P

HEAD_DIM = 128


norm_eps = 1e-05
rope_base = 500000.0


def from_behind(block, axis, distance):
    devices = range(lax.axis_size(axis))
    route = [((i - distance) % len(devices), i) for i in devices]
    return lax.ppermute(block, axis, route)


def rotate(matrix, positions):
    half_dim = matrix.shape[-1] // 2
    frequency = rope_base ** (-2.0 * jnp.arange(half_dim, dtype=jnp.float32) / matrix.shape[-1])
    angles = positions.astype(jnp.float32)[:, None] * frequency[None, :]
    cos_table = jnp.cos(angles)[:, None, :]
    sin_table = jnp.sin(angles)[:, None, :]
    leading = matrix[..., :half_dim]
    trailing = matrix[..., half_dim:]
    return jnp.concatenate(
        [leading * cos_table - trailing * sin_table, trailing * cos_table + leading * sin_table],
        axis=-1,
    )


def project(tokens, gain, query_matrix, keyval_matrix, positions):
    widened = tokens.astype(jnp.float32)
    inverse = lax.rsqrt(jnp.mean(widened * widened, axis=-1, keepdims=True) + norm_eps)
    normed = (widened * inverse * gain[None, :]).astype(jnp.bfloat16)
    row_count = tokens.shape[0]
    query_full = jnp.dot(normed, query_matrix, preferred_element_type=jnp.float32)
    keyval_full = jnp.dot(normed, keyval_matrix, preferred_element_type=jnp.float32)
    queries = rotate(query_full.reshape(row_count, -1, HEAD_DIM), positions).astype(jnp.bfloat16)
    paired = keyval_full.reshape(row_count, 2, -1, HEAD_DIM)
    key_rows = rotate(paired[:, 0], positions).astype(jnp.bfloat16)
    value_rows = paired[:, 1].astype(jnp.bfloat16)
    return (queries, key_rows, value_rows)


def attend(queries, key_wide, value_wide, query_pos, key_pos, narrow):
    row_count = queries.shape[0]
    kv_count = key_wide.shape[1]
    head_size = queries.shape[2]
    group_size = queries.shape[1] // kv_count
    grouped = jnp.moveaxis(queries.reshape(row_count, kv_count, group_size, head_size), 1, 0)
    key_heads = jnp.moveaxis(key_wide, 1, 0)
    value_heads = jnp.moveaxis(value_wide, 1, 0)
    visible = (key_pos[None, :] <= query_pos[:, None])[None]

    def one_head(block):
        query_block, key_block, value_block = block
        scores = jnp.einsum(
            "rgd,sd->grs", query_block, key_block, preferred_element_type=jnp.float32
        ) * head_size ** (-0.5)
        masked = jnp.where(visible, scores, -1e30)
        row_max = lax.stop_gradient(jnp.max(masked, axis=-1, keepdims=True))
        numerators = jnp.where(visible, jnp.exp(masked - row_max), 0.0)
        totals = jnp.sum(numerators, axis=-1)
        if narrow:
            rounded = numerators.astype(jnp.bfloat16)
        else:
            rounded = lax.optimization_barrier(numerators.astype(jnp.bfloat16)).astype(jnp.float32)
        summed = jnp.einsum("grs,sd->rgd", rounded, value_block, preferred_element_type=jnp.float32)
        return summed / jnp.transpose(totals, (1, 0))[..., None]

    averaged = lax.map(one_head, (grouped, key_heads, value_heads))
    return jnp.moveaxis(averaged, 0, 1).reshape(row_count, -1).astype(jnp.bfloat16)


def finish(tokens, mixed, output_matrix):
    return (
        tokens.astype(jnp.float32)
        + jnp.dot(mixed, output_matrix, preferred_element_type=jnp.float32)
    ).astype(jnp.bfloat16)


def shards(
    section_inputs,
    saved_inputs,
    output_grads,
    token_positions,
    norm_gain,
    query_weight,
    keyval_weight,
    output_weight,
):
    key_positions = lax.all_gather(token_positions, "ctx", axis=0, tiled=True)
    full_query, full_keyval = (
        lax.all_gather(query_weight[0], "ctx", axis=0, tiled=True),
        lax.all_gather(keyval_weight[0], "ctx", axis=0, tiled=True),
    )
    full_output = output_weight[0]
    gain = norm_gain[0]
    forward_tokens = section_inputs[0]
    saved_tokens = saved_inputs[0]
    upstream = output_grads[0]

    def projector(tokens):
        return project(tokens, gain, full_query, full_keyval, token_positions)

    def attention_wide(queries, key_wide, value_wide):
        return attend(queries, key_wide, value_wide, token_positions, key_positions, False)

    def finishing(tokens, mixed):
        return finish(tokens, mixed, full_output)

    forward_queries, forward_keys, forward_values = projector(forward_tokens)
    (backward_queries, backward_keys, backward_values), back_project = jax.vjp(
        projector, saved_tokens
    )
    forward_keyset, forward_valueset = (
        lax.all_gather(forward_keys, "ctx", axis=0, tiled=True),
        lax.all_gather(forward_values, "ctx", axis=0, tiled=True),
    )
    mixed = attend(
        forward_queries, forward_keyset, forward_valueset, token_positions, key_positions, True
    )
    produced = finishing(forward_tokens, mixed)
    sent_on = from_behind(produced[None], "section", 1)
    backward_keyset, backward_valueset = (
        lax.all_gather(backward_keys, "ctx", axis=0, tiled=True),
        lax.all_gather(backward_values, "ctx", axis=0, tiled=True),
    )
    mixed, back_attend = jax.vjp(
        attention_wide,
        backward_queries.astype(jnp.float32),
        backward_keyset.astype(jnp.float32),
        backward_valueset.astype(jnp.float32),
    )
    produced, back_finish = jax.vjp(finishing, saved_tokens, mixed)
    residual_grad, mixed_grad = back_finish(upstream)
    query_grad, key_partial, value_partial = back_attend(mixed_grad)
    key_grads = lax.psum_scatter(
        key_partial.astype(jnp.bfloat16), "ctx", scatter_dimension=0, tiled=True
    )
    value_grads = lax.psum_scatter(
        value_partial.astype(jnp.bfloat16), "ctx", scatter_dimension=0, tiled=True
    )
    (project_grad,) = back_project((query_grad.astype(jnp.bfloat16), key_grads, value_grads))
    sent_back = from_behind((residual_grad + project_grad)[None], "section", -1)
    return (sent_on, sent_back)


MESH = pl.DeviceIdType.MESH
VMEM = pl.BlockSpec(memory_space=pltpu.VMEM)
ANY = pl.BlockSpec(memory_space=pl.ANY)
WIDE = jnp.float32
SLIM = jnp.bfloat16


def remote(src, dst, send, recv, device):
    return pltpu.make_async_remote_copy(
        src_ref=src, dst_ref=dst, send_sem=send, recv_sem=recv, device_id=device, device_id_type=MESH
    )


HBM = pl.BlockSpec(memory_space=pltpu.HBM)


def row_chunks(rows):
    return [(start, 16) for start in range(0, rows, 16)]


def layer_kernel(
    n, sections, tokens_hbm, saved_hbm, up_hbm, gain_hbm, wo_hbm, wq, wkv, pos_hbm, waves_hbm, ahead, back,
    tokens, saved, up, gain, pos, waves, nx, mine, mgl, mg, wo, wh, posg, bias, cos, sin, keys, values, dkey, dval, mixed, mixed_in, dqkv,
    part, from_mate, from_z, dn, produced, grads,
    nsend, nrecv, wsend, wrecv, msend, mrecv, psend, precv, asend, arecv, bsend, brecv, zsend, zrecv,
    osend, orecv, csend, crecv, own,
):
    section = lax.axis_index("section")
    me = lax.axis_index("ctx")
    half = n // 2
    core = lax.rem(section, 2)
    base = section - core
    mate = base + 1 - core
    side = me // half
    served = base + side
    lead = core == side
    partner = 2 * side * half + half - 1 - me
    edge = half - 1 + side
    at_edge = me == edge
    group_at = lax.rem(me, half) * 2 + core
    near, far = half - side, (n - 1) * (1 - side)
    depth, _ = wq.shape
    rows, width = tokens.shape
    gq = mg.shape[2]
    group = gq // HEAD_DIM
    kv_half = wkv.shape[1] // 2
    total_rows = n * rows
    scale = HEAD_DIM ** (-0.5)
    following, preceding = lax.rem(section + 1, sections), lax.rem(section + sections - 1, sections)

    barrier = pltpu.get_barrier_semaphore()
    for k in range(1, n):
        for other in (section, mate):
            pl.semaphore_signal(barrier, inc=1, device_id=(other, lax.rem(me + k, n)), device_id_type=MESH)
    for other in (mate, following, preceding):
        pl.semaphore_signal(barrier, inc=1, device_id=(other, me), device_id_type=MESH)

    loads = [
        pltpu.make_async_copy(src, dst, own.at[i])
        for i, (src, dst) in enumerate(
            (
                (gain_hbm, gain), (tokens_hbm, tokens), (saved_hbm, saved), (pos_hbm, pos), (up_hbm, up),
                (waves_hbm, waves), (wo_hbm, wo),
            )
        )
    ]
    for load in loads:
        load.start()

    def normed(block):
        widened = block[...].astype(WIDE)
        inverse = lax.rsqrt(jnp.mean(widened * widened, axis=-1, keepdims=True) + norm_eps)
        return (widened * inverse * gain[...]).astype(SLIM)

    for load in loads[:4]:
        load.wait()
    for batch, block in enumerate((tokens, saved)):
        mine[batch] = normed(block)

    @pl.when(lead)
    def _():
        for batch in (0, 1):
            nx[batch, me] = mine[batch]

    posg[me] = pos[...]
    pl.semaphore_wait(barrier, 2 * n + 1)

    def seat(owner_core, j):
        return (base + lax.rem(j, 2), owner_core * half + j // 2)

    def token_copy(batch, lane, src, block, device):
        return remote(src, nx.at[batch, block], nsend.at[batch, lane], nrecv.at[batch, block], device)

    def to_mate(batch, block):
        return token_copy(batch, 0, nx.at[batch, block], block, (mate, me))

    def to_partner(batch, block):
        return token_copy(batch, 1, nx.at[batch, block], block, (section, partner))

    def to_edge(batch):
        return token_copy(batch, 0, mine.at[batch], me, (section, half - 1 + core))

    def piece_source(j, piece):
        if piece < group:
            start = j * gq + piece * HEAD_DIM
            return wq.at[:, pl.ds(pl.multiple_of(start, HEAD_DIM), HEAD_DIM)], piece * HEAD_DIM
        start = (piece - group) * kv_half + j * HEAD_DIM
        return wkv.at[:, pl.ds(pl.multiple_of(start, HEAD_DIM), HEAD_DIM)], piece * HEAD_DIM

    def piece_slot(piece):
        if piece != group - 1:
            return min(piece, group)
        return jnp.where(me == half - core, group + 1, piece)

    def weight_copy(j, piece):
        src, to = piece_source(j, piece)
        return remote(
            src, wh.at[me, :, pl.ds(to, HEAD_DIM)], wsend.at[j], wrecv.at[piece_slot(piece)], seat(core, j)
        )

    def weight_here(j, piece):
        src, to = piece_source(j, piece)
        return pltpu.make_async_copy(src, wh.at[me, :, pl.ds(to, HEAD_DIM)], wrecv.at[piece_slot(piece)])

    def taken(dst, recv):
        remote(dst, dst, osend.at[0], recv, (section, me)).wait_recv()

    def given(src, send):
        remote(src, src, send, orecv.at[0], (section, me)).wait_send()

    def weight_arrived(piece):
        size = HEAD_DIM if piece < group else 2 * HEAD_DIM
        taken(wh.at[:, :, pl.ds(piece * HEAD_DIM, size)], wrecv.at[piece])

    def here(j):
        return jnp.logical_and(lead, group_at == j)

    def send_weights(piece):
        for i in range(n):
            j = lax.rem(i + core * half, n)
            pl.when(here(j))(lambda: weight_here(j, piece).start())
            pl.when(jnp.logical_not(here(j)))(lambda: weight_copy(j, piece).start())

    def grad_copy(j):
        return remote(mgl.at[j], mg.at[me], msend.at[0], mrecv.at[0], seat(core, j))

    def place_copy(k):
        return remote(pos, posg.at[me], psend.at[0], precv.at[0], (section, lax.rem(me + k, n)))

    @pl.when(lead)
    def _():
        for batch in (0, 1):
            to_partner(batch, me).start()
        for batch in (0, 1):
            to_mate(batch, me).start()

    @pl.when(jnp.logical_not(lead))
    def _():
        for batch in (0, 1):
            to_edge(batch).start()

    for k in range(1, n):
        place_copy(k).start()
    send_weights(group)
    send_weights(group + 1)

    for load in loads[4:]:
        load.wait()
    for j in range(n):
        mgl[j] = lax.dot_general(
            up[...], wo[pl.ds(j * gq, gq), :], (((1,), (1,)), ((), ())), preferred_element_type=WIDE
        ).astype(SLIM)
    for j in range(n):
        @pl.when(here(j))
        def _():
            mg[me] = mgl[j]

        pl.when(jnp.logical_not(here(j)))(lambda: grad_copy(j).start())

    @pl.when(jnp.logical_not(lead))
    def _():
        for piece in range(group):
            send_weights(piece)

    def token_arrived(batch, block):
        dst = nx.at[batch, block]
        remote(dst, dst, nsend.at[0, 0], nrecv.at[batch, block], (section, me)).wait_recv()

    @pl.when(lead)
    def _():
        for batch in (0, 1):
            for block, outer in ((partner, False), (near, True), (far, True)):
                token_arrived(batch, block)
                if outer:
                    pl.when(at_edge)(lambda: to_partner(batch, block).start())
                to_mate(batch, block).start()
        for piece in range(group):
            send_weights(piece)

    taken(posg.at[pl.ds(0, n - 1)], precv.at[0])
    columns = []
    for j in range(n):
        column = jnp.transpose(jnp.broadcast_to(posg[j].astype(WIDE), (HEAD_DIM, rows)))
        angles = column * waves[0:1, :]
        at = pl.ds(j * rows, rows)
        cos[at, :] = jnp.cos(angles)
        sin[at, :] = jnp.sin(angles) * waves[1:2, :]
        columns.append(column)
    column = jnp.concatenate(columns, axis=0)
    bias[...] = jnp.where(jnp.transpose(column)[0:1, :] <= column[:, 0:1], 0.0, -1e30)

    @pl.when(jnp.logical_not(lead))
    def _():
        for batch in (0, 1):
            for block in range(n):
                token_arrived(batch, block)

    def turn(block, sign):
        return block * cos[...] + sign * (pltpu.roll(block, HEAD_DIM // 2, 1) * sin[...])

    def dot(a, b, dims):
        return lax.dot_general(a, b, (dims, ((), ())), preferred_element_type=WIDE)

    def projected(batch, at, sources=range(n)):
        result = None
        for j in sources:
            columns = pl.ds(pl.multiple_of(j * depth, HEAD_DIM), depth)
            term = dot(nx[batch, :, :, columns].reshape(total_rows, depth), wh[j, :, at], ((1,), (0,)))
            result = term if result is None else result + term
        return result

    weight_arrived(group)
    for batch in (0, 1):
        both = projected(batch, pl.ds(gq, 2 * HEAD_DIM))
        keys[batch] = turn(both[:, :HEAD_DIM], 1.0).astype(SLIM)
        values[batch] = both[:, HEAD_DIM:].astype(SLIM)

    def weigh(queries, key_block):
        masked = dot(queries, key_block, ((1,), (1,))) * scale + bias[...]
        numerators = jnp.exp(masked - jnp.max(masked, axis=-1, keepdims=True))
        return numerators, jnp.sum(numerators, axis=-1, keepdims=True)

    last = group - 1
    spans = ((0, last * HEAD_DIM), (last * HEAD_DIM, HEAD_DIM))

    def mixed_copy(block, i):
        at = pl.ds(*spans[i])
        return remote(
            mixed.at[block, :, at], mixed_in.at[group_at, :, at],
            asend.at[i], arecv.at[i], (served, block),
        )

    def elsewhere(block):
        return jnp.logical_not(jnp.logical_and(lead, me == block))

    def send_mixed(i, *blocks):
        for block in blocks:
            pl.when(elsewhere(block))(lambda: mixed_copy(block, i).start())

    def keep_mixed(i):
        @pl.when(lead)
        def _():
            at = pl.ds(*spans[i])
            mixed_in[group_at, :, at] = mixed[me, :, at]

    def forward_head(h):
        at = pl.ds(h * HEAD_DIM, HEAD_DIM)
        queries = turn(projected(0, at), 1.0).astype(SLIM)
        numerators, totals = weigh(queries, keys[0])
        result = dot(numerators.astype(SLIM), values[0], ((1,), (0,))) / totals
        mixed[:, :, at] = result.astype(SLIM).reshape(n, rows, HEAD_DIM)

    def backward_head(h):
        at = pl.ds(h * HEAD_DIM, HEAD_DIM)
        if h < last:
            weight_arrived(h)
            result = projected(1, at)
        else:
            taken(wh.at[pl.ds(0, n - 1), :, at], wrecv.at[h])
            result = projected(1, at, [lax.rem(near + i, n) for i in range(1, n)])
            taken(wh.at[0, :, at], wrecv.at[group + 1])
            result += projected(1, at, [near])
        queries = turn(result, 1.0).astype(SLIM)
        numerators, totals = weigh(queries, keys[1])
        rounded = numerators.astype(SLIM)
        summed = dot(rounded, values[1], ((1,), (0,)))
        summed_grad = mg[:, :, at].reshape(total_rows, HEAD_DIM).astype(WIDE) / totals
        totals_grad = -jnp.sum(summed_grad * (summed / totals), axis=-1, keepdims=True)
        narrow_grad = summed_grad.astype(SLIM)
        numer_grad = dot(narrow_grad, values[1], ((1,), (1,))) + totals_grad
        score_grad = (numerators * numer_grad * scale).astype(SLIM)
        query_grad = dot(score_grad, keys[1], ((1,), (0,))).astype(SLIM)
        dqkv[:, at] = turn(query_grad.astype(WIDE), -1.0).astype(SLIM)
        dkey[...] += dot(score_grad, queries, ((0,), (0,)))
        dval[...] += dot(rounded, narrow_grad, ((0,), (0,)))

    dkey[...] = jnp.zeros_like(dkey)
    dval[...] = jnp.zeros_like(dval)

    for h in range(group):
        if h == 0:
            pl.when(lead)(lambda: taken(mg.at[pl.ds(0, n - 1)], mrecv.at[0]))
            pl.when(jnp.logical_not(lead))(lambda: taken(mg, mrecv.at[0]))
        backward_head(h)
        if h < last:
            forward_head(h)
        if h == last - 1:
            send_mixed(0, partner, me)
            keep_mixed(0)

    dqkv[:, pl.ds(gq, HEAD_DIM)] = turn(dkey[...].astype(SLIM).astype(WIDE), -1.0).astype(SLIM)
    dqkv[:, pl.ds(gq + HEAD_DIM, HEAD_DIM)] = dval[...].astype(SLIM)
    send_mixed(0, far, near)

    def partial_grads(first):
        block_rows = dqkv[pl.ds(pl.multiple_of(first * rows, 16), half * rows), :]
        for j in range(n):
            part[pl.ds(first, half), :, pl.ds(j * depth, depth)] = (
                dot(block_rows, wh[j], ((1,), (1,))).astype(SLIM).reshape(half, rows, depth)
            )

    chunks = row_chunks(rows)

    def mate_sum(slot, block):
        return remote(part.at[block], from_mate.at[block], bsend.at[0], brecv.at[slot], (mate, me))

    def mate_sum_taken(slot, block):
        taken(from_mate.at[block], brecv.at[slot])

    def partner_sum(slot, block, c):
        at = pl.ds(*chunks[c])
        return remote(
            part.at[block, at], from_z.at[block, at], zsend.at[0], zrecv.at[slot, c], (section, partner)
        )

    def owner_sum(block, c):
        at = pl.ds(*chunks[c])
        return remote(part.at[block, at], dn.at[at], osend.at[0], orecv.at[c], (section, block))

    def summed_part(block, c, *others):
        at = pl.ds(*chunks[c])
        value = part[block, at].astype(WIDE)
        for other in others:
            value += other[block, at].astype(WIDE)
        return value.astype(SLIM)

    trailing = jnp.logical_not(lead)
    at_lead_edge = jnp.logical_and(lead, at_edge)
    at_lead_inner = jnp.logical_and(lead, jnp.logical_not(at_edge))

    def send_outer():
        mate_sum(0, near).start()
        mate_sum(1, far).start()

    def send_inner():
        mate_sum(2, partner).start()
        mate_sum(3, me).start()

    def pass_on(slot, block):
        mate_sum_taken(slot, block)
        for c in range(len(chunks)):
            part[block, pl.ds(*chunks[c])] = summed_part(block, c, from_mate)
            partner_sum(slot, block, c).start()

    own_first = jnp.where(at_edge, side, 1 - side)
    trail_edge = jnp.logical_and(trailing, at_edge)
    trail_inner = jnp.logical_and(trailing, jnp.logical_not(at_edge))
    partial_grads(own_first * half)
    pl.when(trail_edge)(send_inner)
    pl.when(trail_inner)(send_outer)
    pl.when(jnp.logical_and(at_lead_inner, core == 1))(lambda: pass_on(0, near))
    partial_grads((1 - own_first) * half)
    pl.when(trail_edge)(send_outer)
    pl.when(trail_inner)(send_inner)

    pl.when(jnp.logical_and(at_lead_inner, core == 0))(lambda: pass_on(0, near))

    forward_head(last)
    send_mixed(1, far, near, partner, me)
    keep_mixed(1)

    @pl.when(at_lead_inner)
    def _():
        pass_on(1, far)
        pass_on(2, partner)

    @pl.when(at_lead_edge)
    def _():
        pass_on(2, partner)


    def finish_block(slot, block):
        mate_sum_taken(slot, block)
        for c in range(len(chunks)):
            partner_sum(slot, block, c).wait_recv()
            part[block, pl.ds(*chunks[c])] = summed_part(block, c, from_mate, from_z)
            owner_sum(block, c).start()

    pl.when(at_lead_edge)(lambda: finish_block(0, near))

    def back_copy(c):
        at = pl.ds(*chunks[c])
        return remote(grads.at[at], back.at[at], csend.at[1], crecv.at[1], (preceding, me))

    def give_back():
        pl.when(lead)(lambda: mate_sum_taken(3, me))
        for c, chunk in enumerate(chunks):
            at = pl.ds(*chunk)

            @pl.when(lead)
            def _():
                partner_sum(2, me, c).wait_recv()
                dn[at] = summed_part(me, c, from_mate, from_z)

            pl.when(trailing)(lambda: owner_sum(me, c).wait_recv())
            widened = saved[at].astype(WIDE)
            inverse = lax.rsqrt(jnp.mean(widened * widened, axis=-1, keepdims=True) + norm_eps)
            scaled = dn[at].astype(WIDE) * gain[...]
            inner_mean = jnp.mean(scaled * widened, axis=-1, keepdims=True)
            project_grad = inverse * scaled - widened * (inverse * inverse * inverse * inner_mean)
            grads[at] = up[at] + project_grad.astype(SLIM)
            back_copy(c).start()

    early = jnp.logical_and(at_lead_inner, core == 0)
    pl.when(early)(give_back)

    total = tokens[...].astype(WIDE)
    for i, (start, size) in enumerate(spans):
        at = pl.ds(start, size)
        pl.when(lead)(lambda: taken(mixed_in.at[pl.ds(0, n - 1), :, at], arecv.at[i]))
        pl.when(trailing)(lambda: taken(mixed_in.at[:, :, at], arecv.at[i]))
        for j in range(n):
            total += jnp.dot(
                mixed_in[j, :, at], wo[pl.ds(j * gq + start, size), :], preferred_element_type=WIDE
            )
    produced[...] = total.astype(SLIM)
    ahead_copy = remote(produced, ahead, csend.at[0], crecv.at[0], (following, me))
    ahead_copy.start()
    pl.when(at_lead_edge)(lambda: finish_block(1, far))

    pl.when(jnp.logical_not(early))(give_back)

    @pl.when(lead)
    def _():
        for batch in (0, 1):
            given(nx.at[batch], nsend.at[batch, 0])
        given(mgl.at[pl.ds(0, n - 1)], msend.at[0])
        for i, span in enumerate(spans):
            given(mixed.at[pl.ds(0, n - 1), :, pl.ds(*span)], asend.at[i])

    @pl.when(at_lead_edge)
    def _():
        for batch in (0, 1):
            given(nx.at[batch, pl.ds(0, half + 1)], nsend.at[batch, 1])
        given(part.at[0], zsend.at[0])
        given(part.at[pl.ds(0, half)], osend.at[0])

    @pl.when(at_lead_inner)
    def _():
        for batch in (0, 1):
            given(nx.at[batch, 0], nsend.at[batch, 1])
        given(part.at[pl.ds(0, half + 1)], zsend.at[0])

    @pl.when(trailing)
    def _():
        for batch in (0, 1):
            given(mine.at[batch], nsend.at[batch, 0])
        given(mgl, msend.at[0])
        for i, span in enumerate(spans):
            given(mixed.at[:, :, pl.ds(*span)], asend.at[i])
        given(part, bsend.at[0])

    given(posg.at[pl.ds(0, n - 1)], psend.at[0])
    for j in range(n):
        pl.when(jnp.logical_not(here(j)))(lambda: given(wh.at[0], wsend.at[j]))

    ahead_copy.wait_send()
    given(grads, csend.at[1])
    ahead_copy.wait_recv()
    taken(back, crecv.at[1])


def hand_kernel(first, second, first_out, second_out, sems):
    gives = [
        pltpu.make_async_copy(src, dst, sems.at[i])
        for i, (src, dst) in enumerate(((first, first_out), (second, second_out)))
    ]
    for give in gives:
        give.start()
    for give in gives:
        give.wait()


def by_pairs(n, sections):
    def step(
        section_inputs, saved_inputs, output_grads, token_positions, norm_gain,
        query_weight, keyval_weight, output_weight,
    ):
        _, rows, width = section_inputs.shape
        _, depth, query_width = query_weight.shape
        gq = query_width // n
        group = gq // HEAD_DIM
        wide = gq + keyval_weight.shape[2] // n

        chunks = len(row_chunks(rows))

        half_dim = HEAD_DIM // 2
        frequency = rope_base ** (-2.0 * np.arange(half_dim) / HEAD_DIM)
        signs = np.ones(half_dim)
        waves = jnp.asarray(
            np.stack([np.concatenate([frequency, frequency]), np.concatenate([-signs, signs])]), WIDE
        )

        def shaped(shape, kind=SLIM):
            return jax.ShapeDtypeStruct(shape, kind)

        def held(*shape, kind=SLIM):
            return pltpu.VMEM(shape, kind)

        pair = (shaped((rows, width)), shaped((rows, width)))
        dma = pltpu.SemaphoreType.DMA
        ahead, back = pl.pallas_call(
            functools.partial(layer_kernel, n, sections),
            out_shape=(pltpu.VMEM((rows, width), SLIM),) * 2,
            in_specs=[HBM] * 9,
            out_specs=(VMEM,) * 2,
            scratch_shapes=[
                *[held(rows, width)] * 3, held(1, width, kind=WIDE), held(1, rows, kind=jnp.int32),
                held(2, HEAD_DIM, kind=WIDE), held(2, n, rows, width), held(2, rows, width),
                held(n, rows, gq), held(n, rows, gq), held(query_width, width), held(n, depth, wide),
                held(n, 1, rows, kind=jnp.int32), held(n * rows, n * rows, kind=WIDE),
                held(n * rows, HEAD_DIM, kind=WIDE), held(n * rows, HEAD_DIM, kind=WIDE),
                held(2, n * rows, HEAD_DIM), held(2, n * rows, HEAD_DIM),
                held(n * rows, HEAD_DIM, kind=WIDE), held(n * rows, HEAD_DIM, kind=WIDE),
                held(n, rows, gq), held(n, rows, gq), held(n * rows, wide),
                held(n, rows, width), held(n, rows, width), held(n, rows, width), held(rows, width),
                held(rows, width), held(rows, width),
                dma((2, 2)), dma((2, n)), dma((n,)), dma((group + 2,)), *[dma((1,))] * 4, *[dma((2,))] * 2,
                dma((1,)), dma((n,)), dma((1,)), dma((3, chunks)), dma((1,)), dma((chunks,)),
                *[dma((2,))] * 2, dma((7,)),
            ],
            compiler_params=pltpu.CompilerParams(
                collective_id=0, has_side_effects=True, vmem_limit_bytes=67043328 - 4 * rows * width - 2**16
            ),
            name="layer",
        )(
            section_inputs[0], saved_inputs[0], output_grads[0], norm_gain, output_weight[0],
            query_weight[0], keyval_weight[0], token_positions[None], waves,
        )
        ahead, back = (pltpu.with_memory_space_constraint(block, pltpu.VMEM) for block in (ahead, back))
        ahead, back = pl.pallas_call(
            hand_kernel, out_shape=pair, in_specs=[VMEM] * 2, out_specs=(HBM,) * 2,
            scratch_shapes=[dma((2,))], name="hand",
        )(ahead, back)
        return (ahead[None], back[None])

    return step


def solution(mesh):
    placed = (
        P("section", "ctx", None),
        P("section", "ctx", None),
        P("section", "ctx", None),
        P("ctx"),
        P("section", None),
        P("section", "ctx", None),
        P("section", "ctx", None),
        P("section", None, None),
    )
    n, sections = mesh.shape["ctx"], mesh.shape["section"]

    def chosen(*blocks):
        kv_heads = blocks[6].shape[2] // (2 * HEAD_DIM)
        rows, query_heads = blocks[0].shape[1], blocks[5].shape[2] // HEAD_DIM
        paired = n == 4 and sections > 2 and sections % 2 == 0
        if paired and kv_heads == n and query_heads > n and rows % 16 == 0:
            return by_pairs(n, sections)(*blocks)
        return shards(*blocks)

    return jax.shard_map(
        chosen,
        mesh=mesh,
        in_specs=placed,
        out_specs=(P("section", "ctx", None), P("section", "ctx", None)),
        check_vma=False,
    )
```

```python
import functools

import jax
import jax.numpy as jnp
import numpy as np
from jax import lax
from jax.experimental import pallas as pl
from jax.experimental.pallas import tpu as pltpu
from jax.sharding import PartitionSpec as P

HEAD_DIM = 128


norm_eps = 1e-05
rope_base = 500000.0


def from_behind(block, axis, distance):
    devices = range(lax.axis_size(axis))
    route = [((i - distance) % len(devices), i) for i in devices]
    return lax.ppermute(block, axis, route)


def rotate(matrix, positions):
    half_dim = matrix.shape[-1] // 2
    frequency = rope_base ** (-2.0 * jnp.arange(half_dim, dtype=jnp.float32) / matrix.shape[-1])
    angles = positions.astype(jnp.float32)[:, None] * frequency[None, :]
    cos_table = jnp.cos(angles)[:, None, :]
    sin_table = jnp.sin(angles)[:, None, :]
    leading = matrix[..., :half_dim]
    trailing = matrix[..., half_dim:]
    return jnp.concatenate(
        [leading * cos_table - trailing * sin_table, trailing * cos_table + leading * sin_table],
        axis=-1,
    )


def project(tokens, gain, query_matrix, keyval_matrix, positions):
    widened = tokens.astype(jnp.float32)
    inverse = lax.rsqrt(jnp.mean(widened * widened, axis=-1, keepdims=True) + norm_eps)
    normed = (widened * inverse * gain[None, :]).astype(jnp.bfloat16)
    row_count = tokens.shape[0]
    query_full = jnp.dot(normed, query_matrix, preferred_element_type=jnp.float32)
    keyval_full = jnp.dot(normed, keyval_matrix, preferred_element_type=jnp.float32)
    queries = rotate(query_full.reshape(row_count, -1, HEAD_DIM), positions).astype(jnp.bfloat16)
    paired = keyval_full.reshape(row_count, 2, -1, HEAD_DIM)
    key_rows = rotate(paired[:, 0], positions).astype(jnp.bfloat16)
    value_rows = paired[:, 1].astype(jnp.bfloat16)
    return (queries, key_rows, value_rows)


def attend(queries, key_wide, value_wide, query_pos, key_pos, narrow):
    row_count = queries.shape[0]
    kv_count = key_wide.shape[1]
    head_size = queries.shape[2]
    group_size = queries.shape[1] // kv_count
    grouped = jnp.moveaxis(queries.reshape(row_count, kv_count, group_size, head_size), 1, 0)
    key_heads = jnp.moveaxis(key_wide, 1, 0)
    value_heads = jnp.moveaxis(value_wide, 1, 0)
    visible = (key_pos[None, :] <= query_pos[:, None])[None]

    def one_head(block):
        query_block, key_block, value_block = block
        scores = jnp.einsum(
            "rgd,sd->grs", query_block, key_block, preferred_element_type=jnp.float32
        ) * head_size ** (-0.5)
        masked = jnp.where(visible, scores, -1e30)
        row_max = lax.stop_gradient(jnp.max(masked, axis=-1, keepdims=True))
        numerators = jnp.where(visible, jnp.exp(masked - row_max), 0.0)
        totals = jnp.sum(numerators, axis=-1)
        if narrow:
            rounded = numerators.astype(jnp.bfloat16)
        else:
            rounded = lax.optimization_barrier(numerators.astype(jnp.bfloat16)).astype(jnp.float32)
        summed = jnp.einsum("grs,sd->rgd", rounded, value_block, preferred_element_type=jnp.float32)
        return summed / jnp.transpose(totals, (1, 0))[..., None]

    averaged = lax.map(one_head, (grouped, key_heads, value_heads))
    return jnp.moveaxis(averaged, 0, 1).reshape(row_count, -1).astype(jnp.bfloat16)


def finish(tokens, mixed, output_matrix):
    return (
        tokens.astype(jnp.float32)
        + jnp.dot(mixed, output_matrix, preferred_element_type=jnp.float32)
    ).astype(jnp.bfloat16)


def shards(
    section_inputs,
    saved_inputs,
    output_grads,
    token_positions,
    norm_gain,
    query_weight,
    keyval_weight,
    output_weight,
):
    key_positions = lax.all_gather(token_positions, "ctx", axis=0, tiled=True)
    full_query, full_keyval = (
        lax.all_gather(query_weight[0], "ctx", axis=0, tiled=True),
        lax.all_gather(keyval_weight[0], "ctx", axis=0, tiled=True),
    )
    full_output = output_weight[0]
    gain = norm_gain[0]
    forward_tokens = section_inputs[0]
    saved_tokens = saved_inputs[0]
    upstream = output_grads[0]

    def projector(tokens):
        return project(tokens, gain, full_query, full_keyval, token_positions)

    def attention_wide(queries, key_wide, value_wide):
        return attend(queries, key_wide, value_wide, token_positions, key_positions, False)

    def finishing(tokens, mixed):
        return finish(tokens, mixed, full_output)

    forward_queries, forward_keys, forward_values = projector(forward_tokens)
    (backward_queries, backward_keys, backward_values), back_project = jax.vjp(
        projector, saved_tokens
    )
    forward_keyset, forward_valueset = (
        lax.all_gather(forward_keys, "ctx", axis=0, tiled=True),
        lax.all_gather(forward_values, "ctx", axis=0, tiled=True),
    )
    mixed = attend(
        forward_queries, forward_keyset, forward_valueset, token_positions, key_positions, True
    )
    produced = finishing(forward_tokens, mixed)
    sent_on = from_behind(produced[None], "section", 1)
    backward_keyset, backward_valueset = (
        lax.all_gather(backward_keys, "ctx", axis=0, tiled=True),
        lax.all_gather(backward_values, "ctx", axis=0, tiled=True),
    )
    mixed, back_attend = jax.vjp(
        attention_wide,
        backward_queries.astype(jnp.float32),
        backward_keyset.astype(jnp.float32),
        backward_valueset.astype(jnp.float32),
    )
    produced, back_finish = jax.vjp(finishing, saved_tokens, mixed)
    residual_grad, mixed_grad = back_finish(upstream)
    query_grad, key_partial, value_partial = back_attend(mixed_grad)
    key_grads = lax.psum_scatter(
        key_partial.astype(jnp.bfloat16), "ctx", scatter_dimension=0, tiled=True
    )
    value_grads = lax.psum_scatter(
        value_partial.astype(jnp.bfloat16), "ctx", scatter_dimension=0, tiled=True
    )
    (project_grad,) = back_project((query_grad.astype(jnp.bfloat16), key_grads, value_grads))
    sent_back = from_behind((residual_grad + project_grad)[None], "section", -1)
    return (sent_on, sent_back)


MESH = pl.DeviceIdType.MESH
VMEM = pl.BlockSpec(memory_space=pltpu.VMEM)
ANY = pl.BlockSpec(memory_space=pl.ANY)
WIDE = jnp.float32
SLIM = jnp.bfloat16


def remote(src, dst, send, recv, device):
    return pltpu.make_async_remote_copy(
        src_ref=src, dst_ref=dst, send_sem=send, recv_sem=recv, device_id=device, device_id_type=MESH
    )


HBM = pl.BlockSpec(memory_space=pltpu.HBM)


def row_chunks(rows):
    return [(start, 16) for start in range(0, rows, 16)]


def layer_kernel(
    n, sections, tokens_hbm, saved_hbm, up_hbm, gain_hbm, wo_hbm, wq, wkv, pos_hbm, waves_hbm, ahead, back,
    tokens, saved, up, gain, pos, waves, nx, mine, mgl, mg, wo, wh, posg, bias, cos, sin, keys, values, dkey, dval, mixed, mixed_in, dqkv,
    part, from_mate, from_z, dn, produced, grads,
    nsend, nrecv, wsend, wrecv, msend, mrecv, psend, precv, asend, arecv, bsend, brecv, zsend, zrecv,
    osend, orecv, csend, crecv, own,
):
    section = lax.axis_index("section")
    me = lax.axis_index("ctx")
    half = n // 2
    core = lax.rem(section, 2)
    base = section - core
    mate = base + 1 - core
    side = me // half
    served = base + side
    lead = core == side
    partner = 2 * side * half + half - 1 - me
    edge = half - 1 + side
    at_edge = me == edge
    group_at = lax.rem(me, half) * 2 + core
    near, far = half - side, (n - 1) * (1 - side)
    depth, _ = wq.shape
    rows, width = tokens.shape
    gq = mg.shape[2]
    group = gq // HEAD_DIM
    kv_half = wkv.shape[1] // 2
    total_rows = n * rows
    scale = HEAD_DIM ** (-0.5)
    following, preceding = lax.rem(section + 1, sections), lax.rem(section + sections - 1, sections)

    barrier = pltpu.get_barrier_semaphore()
    for k in range(1, n):
        for other in (section, mate):
            pl.semaphore_signal(barrier, inc=1, device_id=(other, lax.rem(me + k, n)), device_id_type=MESH)
    for other in (mate, following, preceding):
        pl.semaphore_signal(barrier, inc=1, device_id=(other, me), device_id_type=MESH)

    loads = [
        pltpu.make_async_copy(src, dst, own.at[i])
        for i, (src, dst) in enumerate(
            (
                (gain_hbm, gain), (tokens_hbm, tokens), (saved_hbm, saved), (pos_hbm, pos), (up_hbm, up),
                (waves_hbm, waves), (wo_hbm, wo),
            )
        )
    ]
    for load in loads:
        load.start()

    def normed(block):
        widened = block[...].astype(WIDE)
        inverse = lax.rsqrt(jnp.mean(widened * widened, axis=-1, keepdims=True) + norm_eps)
        return (widened * inverse * gain[...]).astype(SLIM)

    for load in loads[:4]:
        load.wait()
    for batch, block in enumerate((tokens, saved)):
        mine[batch] = normed(block)

    @pl.when(lead)
    def _():
        for batch in (0, 1):
            nx[batch, me] = mine[batch]

    posg[me] = pos[...]
    pl.semaphore_wait(barrier, 2 * n + 1)

    def seat(owner_core, j):
        return (base + lax.rem(j, 2), owner_core * half + j // 2)

    def token_copy(batch, lane, src, block, device):
        return remote(src, nx.at[batch, block], nsend.at[batch, lane], nrecv.at[batch, block], device)

    def to_mate(batch, block):
        return token_copy(batch, 0, nx.at[batch, block], block, (mate, me))

    def to_partner(batch, block):
        return token_copy(batch, 1, nx.at[batch, block], block, (section, partner))

    def to_edge(batch):
        return token_copy(batch, 0, mine.at[batch], me, (section, half - 1 + core))

    def piece_source(j, piece):
        if piece < group:
            start = j * gq + piece * HEAD_DIM
            return wq.at[:, pl.ds(pl.multiple_of(start, HEAD_DIM), HEAD_DIM)], piece * HEAD_DIM
        start = (piece - group) * kv_half + j * HEAD_DIM
        return wkv.at[:, pl.ds(pl.multiple_of(start, HEAD_DIM), HEAD_DIM)], piece * HEAD_DIM

    def piece_slot(piece):
        if piece != group - 1:
            return min(piece, group)
        return jnp.where(me == half - core, group + 1, piece)

    def weight_copy(j, piece):
        src, to = piece_source(j, piece)
        return remote(
            src, wh.at[me, :, pl.ds(to, HEAD_DIM)], wsend.at[j], wrecv.at[piece_slot(piece)], seat(core, j)
        )

    def weight_here(j, piece):
        src, to = piece_source(j, piece)
        return pltpu.make_async_copy(src, wh.at[me, :, pl.ds(to, HEAD_DIM)], wrecv.at[piece_slot(piece)])

    def taken(dst, recv):
        remote(dst, dst, osend.at[0], recv, (section, me)).wait_recv()

    def given(src, send):
        remote(src, src, send, orecv.at[0], (section, me)).wait_send()

    def weight_arrived(piece):
        size = HEAD_DIM if piece < group else 2 * HEAD_DIM
        taken(wh.at[:, :, pl.ds(piece * HEAD_DIM, size)], wrecv.at[piece])

    def here(j):
        return jnp.logical_and(lead, group_at == j)

    def send_weights(piece):
        for i in range(n):
            j = lax.rem(i + core * half, n)
            pl.when(here(j))(lambda: weight_here(j, piece).start())
            pl.when(jnp.logical_not(here(j)))(lambda: weight_copy(j, piece).start())

    def grad_copy(j):
        return remote(mgl.at[j], mg.at[me], msend.at[0], mrecv.at[0], seat(core, j))

    def place_copy(k):
        return remote(pos, posg.at[me], psend.at[0], precv.at[0], (section, lax.rem(me + k, n)))

    @pl.when(lead)
    def _():
        for batch in (0, 1):
            to_partner(batch, me).start()
        for batch in (0, 1):
            to_mate(batch, me).start()

    @pl.when(jnp.logical_not(lead))
    def _():
        for batch in (0, 1):
            to_edge(batch).start()

    for k in range(1, n):
        place_copy(k).start()
    send_weights(group)
    send_weights(group + 1)

    for load in loads[4:]:
        load.wait()
    for j in range(n):
        mgl[j] = lax.dot_general(
            up[...], wo[pl.ds(j * gq, gq), :], (((1,), (1,)), ((), ())), preferred_element_type=WIDE
        ).astype(SLIM)
    for j in range(n):
        @pl.when(here(j))
        def _():
            mg[me] = mgl[j]

        pl.when(jnp.logical_not(here(j)))(lambda: grad_copy(j).start())

    @pl.when(jnp.logical_not(lead))
    def _():
        for piece in range(group):
            send_weights(piece)

    def token_arrived(batch, block):
        dst = nx.at[batch, block]
        remote(dst, dst, nsend.at[0, 0], nrecv.at[batch, block], (section, me)).wait_recv()

    @pl.when(lead)
    def _():
        for batch in (0, 1):
            for block, outer in ((partner, False), (near, True), (far, True)):
                token_arrived(batch, block)
                if outer:
                    pl.when(at_edge)(lambda: to_partner(batch, block).start())
                to_mate(batch, block).start()
        for piece in range(group):
            send_weights(piece)

    taken(posg.at[pl.ds(0, n - 1)], precv.at[0])
    columns = []
    for j in range(n):
        column = jnp.transpose(jnp.broadcast_to(posg[j].astype(WIDE), (HEAD_DIM, rows)))
        angles = column * waves[0:1, :]
        at = pl.ds(j * rows, rows)
        cos[at, :] = jnp.cos(angles)
        sin[at, :] = jnp.sin(angles) * waves[1:2, :]
        columns.append(column)
    column = jnp.concatenate(columns, axis=0)
    bias[...] = jnp.where(jnp.transpose(column)[0:1, :] <= column[:, 0:1], 0.0, -1e30)

    @pl.when(jnp.logical_not(lead))
    def _():
        for batch in (0, 1):
            for block in range(n):
                token_arrived(batch, block)

    def turn(block, sign):
        return block * cos[...] + sign * (pltpu.roll(block, HEAD_DIM // 2, 1) * sin[...])

    def dot(a, b, dims):
        return lax.dot_general(a, b, (dims, ((), ())), preferred_element_type=WIDE)

    def projected(batch, at, sources=range(n)):
        result = None
        for j in sources:
            columns = pl.ds(pl.multiple_of(j * depth, HEAD_DIM), depth)
            term = dot(nx[batch, :, :, columns].reshape(total_rows, depth), wh[j, :, at], ((1,), (0,)))
            result = term if result is None else result + term
        return result

    weight_arrived(group)
    for batch in (0, 1):
        both = projected(batch, pl.ds(gq, 2 * HEAD_DIM))
        keys[batch] = turn(both[:, :HEAD_DIM], 1.0).astype(SLIM)
        values[batch] = both[:, HEAD_DIM:].astype(SLIM)

    def weigh(queries, key_block):
        masked = dot(queries, key_block, ((1,), (1,))) * scale + bias[...]
        numerators = jnp.exp(masked - jnp.max(masked, axis=-1, keepdims=True))
        return numerators, jnp.sum(numerators, axis=-1, keepdims=True)

    last = group - 1
    spans = ((0, last * HEAD_DIM), (last * HEAD_DIM, HEAD_DIM))

    def mixed_copy(block, i):
        at = pl.ds(*spans[i])
        return remote(
            mixed.at[block, :, at], mixed_in.at[group_at, :, at],
            asend.at[i], arecv.at[i], (served, block),
        )

    def elsewhere(block):
        return jnp.logical_not(jnp.logical_and(lead, me == block))

    def send_mixed(i, *blocks):
        for block in blocks:
            pl.when(elsewhere(block))(lambda: mixed_copy(block, i).start())

    def keep_mixed(i):
        @pl.when(lead)
        def _():
            at = pl.ds(*spans[i])
            mixed_in[group_at, :, at] = mixed[me, :, at]

    def forward_head(h):
        at = pl.ds(h * HEAD_DIM, HEAD_DIM)
        queries = turn(projected(0, at), 1.0).astype(SLIM)
        numerators, totals = weigh(queries, keys[0])
        result = dot(numerators.astype(SLIM), values[0], ((1,), (0,))) / totals
        mixed[:, :, at] = result.astype(SLIM).reshape(n, rows, HEAD_DIM)

    def backward_head(h):
        at = pl.ds(h * HEAD_DIM, HEAD_DIM)
        if h < last:
            weight_arrived(h)
            result = projected(1, at)
        else:
            taken(wh.at[pl.ds(0, n - 1), :, at], wrecv.at[h])
            result = projected(1, at, [lax.rem(near + i, n) for i in range(1, n)])
            taken(wh.at[0, :, at], wrecv.at[group + 1])
            result += projected(1, at, [near])
        queries = turn(result, 1.0).astype(SLIM)
        numerators, totals = weigh(queries, keys[1])
        rounded = numerators.astype(SLIM)
        summed = dot(rounded, values[1], ((1,), (0,)))
        summed_grad = mg[:, :, at].reshape(total_rows, HEAD_DIM).astype(WIDE) / totals
        totals_grad = -jnp.sum(summed_grad * (summed / totals), axis=-1, keepdims=True)
        narrow_grad = summed_grad.astype(SLIM)
        numer_grad = dot(narrow_grad, values[1], ((1,), (1,))) + totals_grad
        score_grad = (numerators * numer_grad * scale).astype(SLIM)
        query_grad = dot(score_grad, keys[1], ((1,), (0,))).astype(SLIM)
        dqkv[:, at] = turn(query_grad.astype(WIDE), -1.0).astype(SLIM)
        dkey[...] += dot(score_grad, queries, ((0,), (0,)))
        dval[...] += dot(rounded, narrow_grad, ((0,), (0,)))

    dkey[...] = jnp.zeros_like(dkey)
    dval[...] = jnp.zeros_like(dval)

    for h in range(group):
        if h == 0:
            pl.when(lead)(lambda: taken(mg.at[pl.ds(0, n - 1)], mrecv.at[0]))
            pl.when(jnp.logical_not(lead))(lambda: taken(mg, mrecv.at[0]))
        backward_head(h)
        if h < last:
            forward_head(h)
        if h == last - 1:
            send_mixed(0, partner, me)
            keep_mixed(0)

    dqkv[:, pl.ds(gq, HEAD_DIM)] = turn(dkey[...].astype(SLIM).astype(WIDE), -1.0).astype(SLIM)
    dqkv[:, pl.ds(gq + HEAD_DIM, HEAD_DIM)] = dval[...].astype(SLIM)
    holds = jnp.logical_and(jnp.logical_and(lead, core == 0), jnp.logical_not(at_edge))
    pl.when(jnp.logical_not(holds))(lambda: send_mixed(0, far, near))

    def partial_grads(first):
        block_rows = dqkv[pl.ds(pl.multiple_of(first * rows, 16), half * rows), :]
        for j in range(n):
            part[pl.ds(first, half), :, pl.ds(j * depth, depth)] = (
                dot(block_rows, wh[j], ((1,), (1,))).astype(SLIM).reshape(half, rows, depth)
            )

    chunks = row_chunks(rows)

    def mate_sum(slot, block):
        return remote(part.at[block], from_mate.at[block], bsend.at[0], brecv.at[slot], (mate, me))

    def mate_sum_taken(slot, block):
        taken(from_mate.at[block], brecv.at[slot])

    def partner_sum(slot, block, c):
        at = pl.ds(*chunks[c])
        return remote(
            part.at[block, at], from_z.at[block, at], zsend.at[0], zrecv.at[slot, c], (section, partner)
        )

    def owner_sum(block, c):
        at = pl.ds(*chunks[c])
        return remote(part.at[block, at], dn.at[at], osend.at[0], orecv.at[c], (section, block))

    def summed_part(block, c, *others):
        at = pl.ds(*chunks[c])
        value = part[block, at].astype(WIDE)
        for other in others:
            value += other[block, at].astype(WIDE)
        return value.astype(SLIM)

    trailing = jnp.logical_not(lead)
    at_lead_edge = jnp.logical_and(lead, at_edge)
    at_lead_inner = jnp.logical_and(lead, jnp.logical_not(at_edge))

    def send_outer():
        mate_sum(0, near).start()
        mate_sum(1, far).start()

    def send_inner():
        mate_sum(2, partner).start()
        mate_sum(3, me).start()

    def pass_on(slot, block):
        mate_sum_taken(slot, block)
        for c in range(len(chunks)):
            part[block, pl.ds(*chunks[c])] = summed_part(block, c, from_mate)
            partner_sum(slot, block, c).start()

    own_first = jnp.where(at_edge, side, 1 - side)
    trail_edge = jnp.logical_and(trailing, at_edge)
    trail_inner = jnp.logical_and(trailing, jnp.logical_not(at_edge))
    partial_grads(own_first * half)
    pl.when(trail_edge)(send_inner)
    pl.when(trail_inner)(send_outer)
    pl.when(jnp.logical_and(at_lead_inner, core == 1))(lambda: pass_on(0, near))
    partial_grads((1 - own_first) * half)
    pl.when(trail_edge)(send_outer)
    pl.when(trail_inner)(send_inner)

    @pl.when(holds)
    def _():
        pass_on(0, near)
        send_mixed(0, far, near)

    forward_head(last)
    send_mixed(1, far, near, partner, me)
    keep_mixed(1)

    @pl.when(at_lead_inner)
    def _():
        pass_on(1, far)
        pass_on(2, partner)

    @pl.when(at_lead_edge)
    def _():
        pass_on(2, partner)


    def finish_block(slot, block):
        mate_sum_taken(slot, block)
        for c in range(len(chunks)):
            partner_sum(slot, block, c).wait_recv()
            part[block, pl.ds(*chunks[c])] = summed_part(block, c, from_mate, from_z)
            owner_sum(block, c).start()

    pl.when(at_lead_edge)(lambda: finish_block(0, near))

    def back_copy(c):
        at = pl.ds(*chunks[c])
        return remote(grads.at[at], back.at[at], csend.at[1], crecv.at[1], (preceding, me))

    def give_back():
        pl.when(lead)(lambda: mate_sum_taken(3, me))
        for c, chunk in enumerate(chunks):
            at = pl.ds(*chunk)

            @pl.when(lead)
            def _():
                partner_sum(2, me, c).wait_recv()
                dn[at] = summed_part(me, c, from_mate, from_z)

            pl.when(trailing)(lambda: owner_sum(me, c).wait_recv())
            widened = saved[at].astype(WIDE)
            inverse = lax.rsqrt(jnp.mean(widened * widened, axis=-1, keepdims=True) + norm_eps)
            scaled = dn[at].astype(WIDE) * gain[...]
            inner_mean = jnp.mean(scaled * widened, axis=-1, keepdims=True)
            project_grad = inverse * scaled - widened * (inverse * inverse * inverse * inner_mean)
            grads[at] = up[at] + project_grad.astype(SLIM)
            back_copy(c).start()

    early = jnp.logical_and(at_lead_inner, core == 0)
    pl.when(early)(give_back)

    total = tokens[...].astype(WIDE)
    for i, (start, size) in enumerate(spans):
        at = pl.ds(start, size)
        pl.when(lead)(lambda: taken(mixed_in.at[pl.ds(0, n - 1), :, at], arecv.at[i]))
        pl.when(trailing)(lambda: taken(mixed_in.at[:, :, at], arecv.at[i]))
        for j in range(n):
            total += jnp.dot(
                mixed_in[j, :, at], wo[pl.ds(j * gq + start, size), :], preferred_element_type=WIDE
            )
    produced[...] = total.astype(SLIM)
    ahead_copy = remote(produced, ahead, csend.at[0], crecv.at[0], (following, me))
    ahead_copy.start()
    pl.when(at_lead_edge)(lambda: finish_block(1, far))

    pl.when(jnp.logical_not(early))(give_back)

    @pl.when(lead)
    def _():
        for batch in (0, 1):
            given(nx.at[batch], nsend.at[batch, 0])
        given(mgl.at[pl.ds(0, n - 1)], msend.at[0])
        for i, span in enumerate(spans):
            given(mixed.at[pl.ds(0, n - 1), :, pl.ds(*span)], asend.at[i])

    @pl.when(at_lead_edge)
    def _():
        for batch in (0, 1):
            given(nx.at[batch, pl.ds(0, half + 1)], nsend.at[batch, 1])
        given(part.at[0], zsend.at[0])
        given(part.at[pl.ds(0, half)], osend.at[0])

    @pl.when(at_lead_inner)
    def _():
        for batch in (0, 1):
            given(nx.at[batch, 0], nsend.at[batch, 1])
        given(part.at[pl.ds(0, half + 1)], zsend.at[0])

    @pl.when(trailing)
    def _():
        for batch in (0, 1):
            given(mine.at[batch], nsend.at[batch, 0])
        given(mgl, msend.at[0])
        for i, span in enumerate(spans):
            given(mixed.at[:, :, pl.ds(*span)], asend.at[i])
        given(part, bsend.at[0])

    given(posg.at[pl.ds(0, n - 1)], psend.at[0])
    for j in range(n):
        pl.when(jnp.logical_not(here(j)))(lambda: given(wh.at[0], wsend.at[j]))

    ahead_copy.wait_send()
    given(grads, csend.at[1])
    ahead_copy.wait_recv()
    taken(back, crecv.at[1])


def hand_kernel(first, second, first_out, second_out, sems):
    gives = [
        pltpu.make_async_copy(src, dst, sems.at[i])
        for i, (src, dst) in enumerate(((first, first_out), (second, second_out)))
    ]
    for give in gives:
        give.start()
    for give in gives:
        give.wait()


def by_pairs(n, sections):
    def step(
        section_inputs, saved_inputs, output_grads, token_positions, norm_gain,
        query_weight, keyval_weight, output_weight,
    ):
        _, rows, width = section_inputs.shape
        _, depth, query_width = query_weight.shape
        gq = query_width // n
        group = gq // HEAD_DIM
        wide = gq + keyval_weight.shape[2] // n

        chunks = len(row_chunks(rows))

        half_dim = HEAD_DIM // 2
        frequency = rope_base ** (-2.0 * np.arange(half_dim) / HEAD_DIM)
        signs = np.ones(half_dim)
        waves = jnp.asarray(
            np.stack([np.concatenate([frequency, frequency]), np.concatenate([-signs, signs])]), WIDE
        )

        def shaped(shape, kind=SLIM):
            return jax.ShapeDtypeStruct(shape, kind)

        def held(*shape, kind=SLIM):
            return pltpu.VMEM(shape, kind)

        pair = (shaped((rows, width)), shaped((rows, width)))
        dma = pltpu.SemaphoreType.DMA
        ahead, back = pl.pallas_call(
            functools.partial(layer_kernel, n, sections),
            out_shape=(pltpu.VMEM((rows, width), SLIM),) * 2,
            in_specs=[HBM] * 9,
            out_specs=(VMEM,) * 2,
            scratch_shapes=[
                *[held(rows, width)] * 3, held(1, width, kind=WIDE), held(1, rows, kind=jnp.int32),
                held(2, HEAD_DIM, kind=WIDE), held(2, n, rows, width), held(2, rows, width),
                held(n, rows, gq), held(n, rows, gq), held(query_width, width), held(n, depth, wide),
                held(n, 1, rows, kind=jnp.int32), held(n * rows, n * rows, kind=WIDE),
                held(n * rows, HEAD_DIM, kind=WIDE), held(n * rows, HEAD_DIM, kind=WIDE),
                held(2, n * rows, HEAD_DIM), held(2, n * rows, HEAD_DIM),
                held(n * rows, HEAD_DIM, kind=WIDE), held(n * rows, HEAD_DIM, kind=WIDE),
                held(n, rows, gq), held(n, rows, gq), held(n * rows, wide),
                held(n, rows, width), held(n, rows, width), held(n, rows, width), held(rows, width),
                held(rows, width), held(rows, width),
                dma((2, 2)), dma((2, n)), dma((n,)), dma((group + 2,)), *[dma((1,))] * 4, *[dma((2,))] * 2,
                dma((1,)), dma((n,)), dma((1,)), dma((3, chunks)), dma((1,)), dma((chunks,)),
                *[dma((2,))] * 2, dma((7,)),
            ],
            compiler_params=pltpu.CompilerParams(
                collective_id=0, has_side_effects=True, vmem_limit_bytes=67043328 - 4 * rows * width - 2**16
            ),
            name="layer",
        )(
            section_inputs[0], saved_inputs[0], output_grads[0], norm_gain, output_weight[0],
            query_weight[0], keyval_weight[0], token_positions[None], waves,
        )
        ahead, back = (pltpu.with_memory_space_constraint(block, pltpu.VMEM) for block in (ahead, back))
        ahead, back = pl.pallas_call(
            hand_kernel, out_shape=pair, in_specs=[VMEM] * 2, out_specs=(HBM,) * 2,
            scratch_shapes=[dma((2,))], name="hand",
        )(ahead, back)
        return (ahead[None], back[None])

    return step


def solution(mesh):
    placed = (
        P("section", "ctx", None),
        P("section", "ctx", None),
        P("section", "ctx", None),
        P("ctx"),
        P("section", None),
        P("section", "ctx", None),
        P("section", "ctx", None),
        P("section", None, None),
    )
    n, sections = mesh.shape["ctx"], mesh.shape["section"]

    def chosen(*blocks):
        kv_heads = blocks[6].shape[2] // (2 * HEAD_DIM)
        rows, query_heads = blocks[0].shape[1], blocks[5].shape[2] // HEAD_DIM
        paired = n == 4 and sections > 2 and sections % 2 == 0
        if paired and kv_heads == n and query_heads > n and rows % 16 == 0:
            return by_pairs(n, sections)(*blocks)
        return shards(*blocks)

    return jax.shard_map(
        chosen,
        mesh=mesh,
        in_specs=placed,
        out_specs=(P("section", "ctx", None), P("section", "ctx", None)),
        check_vma=False,
    )
```
